32 devices in a mesh: gz: 2 (over x), gy: 4 (over y, core), gx: 4 (over z).
Axes of the slice: x: 2, y: 2, z: 4, core: 2. Of those that a mesh axis runs over, the one named last changes fastest.
Arguments:
- density: float32 [32, 64, 256], P('gx', 'gy', 'gz'), may hold values from 0.05 to 0.95
- spread: float32 [32, 64, 256], P('gx', 'gy', 'gz'), may hold values from 0.05 to 0.3
- sensitivities: float32 [9, 32, 64, 256], P(None, 'gx', 'gy', 'gz'), may hold values from -180 to 180, as said below
- violation: float32 [9], replicated, may hold values from -0.05 to 0.15
- multipliers_start: float32 [9], replicated, may hold values from 0.1 to 10
Outputs:
- new_density: float32 [32, 64, 256], P('gx', 'gy', 'gz')
- multipliers: float32 [9], replicated
The draws below stay inside these ranges and needn't reach their ends.
Inputs may be any that keep to these rules, and one draw needn't show every extreme that they name: `sensitivities`: Real-valued, independent from voxel to voxel.
All inputs are finite; a program needn't handle non-finite values.
Results may differ from the reference program's by a relative error of at most 0.0003.
Values sent between devices are 32-bit elements; how exact they have to be, the bound alone decides.
A program may use at most 64 MiB of HBM per device.

```python
import math
import jax
import jax.numpy as jnp
from jax import lax

FIELDS = 9
ITERS = 3
NX = 32
NY = 64
NZ = 256


def draw_sensitivities(key, part):
    key_rough = jax.random.fold_in(key, 11)
    key_scale = jax.random.fold_in(key, 12)
    ramp = 1.0 + 2.0 * jnp.arange(NX, dtype=jnp.float32) / max(NX - 1, 1)
    scales = jnp.exp(jax.random.uniform(key_scale, (FIELDS,), jnp.float32, 0.0, math.log(10.0)))
    values = jnp.clip(jax.random.normal(key_rough, (FIELDS, NX, NY, NZ), jnp.float32), -6.0, 6.0)
    return values * scales[:, None, None, None] * ramp[None, :, None, None]


def levels(rng, extent, cuts, smallest, largest):
    def one(axis_at, blocks):
        steps = jax.random.uniform(jax.random.fold_in(jax.random.fold_in(rng, 6), axis_at), (blocks,), jnp.float32, smallest / len(cuts), largest / len(cuts))
        return jnp.repeat(jnp.exp(steps), extent[axis_at] // blocks).reshape((-1,) + (1,) * (len(extent) - axis_at - 1))

    factor_of = one(*cuts[0])
    for cut in cuts[1:]:
        factor_of = factor_of * one(*cut)
    return factor_of


def setup_inputs(seed: int = 0) -> dict:
    keys = jax.random.split(jax.random.key(seed), 6)
    return {
        "density": jnp.clip(0.05 + 0.9 * jax.random.uniform(keys[0], (NX, NY, NZ), jnp.float32) ** levels(keys[0], (NX, NY, NZ), ((0, 4), (1, 4), (2, 2)), -0.2, 0.2), 0.05, 0.95),
        "spread": jnp.clip(jnp.exp(math.log(0.3) - 1.7917595 * jax.random.uniform(keys[1], (NX, NY, NZ), jnp.float32) ** levels(keys[1], (NX, NY, NZ), ((0, 4), (1, 4), (2, 2)), -0.2, 0.2)), 0.05, 0.3),
        "sensitivities": draw_sensitivities(jax.random.fold_in(keys[5], 71), 0),
        "violation": jnp.clip(jax.random.uniform(keys[3], (FIELDS,), jnp.float32, -0.05, 0.15), -0.05, 0.15),
        "multipliers_start": jnp.clip(jnp.exp(jax.random.uniform(keys[4], (FIELDS,), jnp.float32, math.log(0.1), math.log(10.0))), 0.1, 10.0),
    }


RADIUS = 3.0
RAA = 1e-05
MOVE = 0.9
REG = 0.001
FLOOR = 0.2

def smooth(padded, nx, ny, nz):
    total = None
    for a in (-1, 0, 1):
        for b in (-1, 0, 1):
            for c in (-1, 0, 1):
                weight = RADIUS - math.sqrt(a * a + b * b + c * c)
                piece = padded[..., 1 + a:1 + a + nx, 1 + b:1 + b + ny, 1 + c:1 + c + nz]
                total = weight * piece if total is None else total + weight * piece
    return total

def reference(density, spread, sensitivities, violation, multipliers_start):
    nx, ny, nz = density.shape
    denom = smooth(jnp.pad(jnp.ones_like(density), 1), nx, ny, nz)

    def one_field(field):
        return smooth(jnp.pad(field, 1), nx, ny, nz) / denom
    filtered = lax.map(one_field, sensitivities)
    cells = nx * ny * nz
    dens = density.reshape(-1)
    span = spread.reshape(-1)
    rows = jnp.concatenate([filtered.reshape(FIELDS, cells), jnp.ones((1, cells), density.dtype)], axis=0)
    grow = jnp.maximum(rows, 0.0)
    fall = jnp.maximum(-rows, 0.0)
    square = span * span
    pp = square * (1.001 * grow + 0.001 * fall + RAA)
    qq = square * (0.001 * grow + 1.001 * fall + RAA)
    lower = dens - span
    upper = dens + span
    floor_x = jnp.maximum(0.0, dens - MOVE * span)
    ceil_x = jnp.minimum(1.0, dens + MOVE * span)
    base = (pp[1:] + qq[1:]) / span
    bound = (1.0 - violation) * lax.optimization_barrier(jnp.sum(base, axis=1))

    def respond(lam):
        weights = jnp.concatenate([jnp.ones((1,), lam.dtype), lam])
        big_p = jnp.dot(weights, pp, precision=lax.Precision.HIGHEST)
        big_q = jnp.dot(weights, qq, precision=lax.Precision.HIGHEST)
        root_p = jnp.sqrt(big_p)
        root_q = jnp.sqrt(big_q)
        moved = (root_p * lower + root_q * upper) / (root_p + root_q)
        return (jnp.clip(moved, floor_x, ceil_x), big_p, big_q)
    lam = multipliers_start
    for step in range(ITERS):
        moved, big_p, big_q = respond(lam)
        above = upper - moved
        below = moved - lower
        gradient = lax.optimization_barrier(jnp.sum(pp[1:] / above + qq[1:] / below, axis=1)) - bound
        slopes = pp[1:] / (above * above) - qq[1:] / (below * below)
        curv = 2.0 * big_p / (above * above * above) + 2.0 * big_q / (below * below * below)
        schur = jnp.dot(slopes / curv, slopes.T, precision=lax.Precision.HIGHEST)
        shift = REG * jnp.trace(schur) / FIELDS
        system = schur + shift * jnp.eye(FIELDS, dtype=schur.dtype)
        factor = jnp.linalg.cholesky(system)
        delta = jax.scipy.linalg.cho_solve((factor, True), gradient)
        lam = jnp.maximum(lam + delta, FLOOR * lam)
    moved, big_p, big_q = respond(lam)
    return (moved.reshape(nx, ny, nz), lam)
```

```python
import functools
import math

import jax
import jax.numpy as jnp
from jax import lax
from jax.experimental import pallas as pl
from jax.experimental.pallas import tpu as pltpu
from jax.sharding import PartitionSpec as P

FIELDS = 9
ITERS = 3

RADIUS = 3.0
RAA = 1e-05
MOVE = 0.9
REG = 0.001
FLOOR = 0.2

W0 = RADIUS
W1 = RADIUS - 1.0
W2 = RADIUS - math.sqrt(2.0)
W3 = RADIUS - math.sqrt(3.0)

SUB, LANE = 8, 128
AXES = ("gz", "gy", "gx")
SUMS = FIELDS + FIELDS * (FIELDS + 1) // 2
ROWS = SUMS + FIELDS
MESH = pl.DeviceIdType.MESH
GROUP = 3


def plan(shape):
    total = math.prod(shape[a] for a in AXES)
    if total <= 32:
        return (AXES,)
    return tuple((a,) for a in AXES)


def offsets(axes, shape):
    out = [()]
    for a in axes:
        out = [o + (d,) for o in out for d in range(shape[a])]
    return [o for o in out if any(o)]


def steps():
    return [range(f, min(f + GROUP, FIELDS)) for f in range(0, FIELDS, GROUP)]


def body(shape, dims, dens_hbm, span_hbm, sens_ref, viol_hbm, lam0_hbm, out_ref, lam_out,
         dens_ref, span_ref, viol_ref, lam0_ref, pad, ypack, yrecv, cpack, crecv, zpack, zrecv, mid, invden, pp, qq, slope, scaled,
         acc, wide, lam, part, *rest):
    stages = plan(shape)
    recvs = rest[: len(stages)]
    load_sem, send_sem, recv_sem, sum_send, sum_recv, known = rest[len(stages):]
    nx, ny, nz = dims
    tiles = ny // SUB
    chunks = nx * tiles
    me = {a: lax.axis_index(a) for a in AXES}

    has = {}
    for a in AXES:
        has[a, -1] = me[a] > 0
        has[a, 0] = jnp.bool_(True)
        has[a, 1] = me[a] < shape[a] - 1

    def both(o):
        moved = [has[a, d] for a, d in zip(AXES, o) if d]
        return functools.reduce(jnp.logical_and, moved)

    def at(**moves):
        return {a: me[a] + d for a, d in moves.items()}

    plane = [(0, dy, dx) for dy in (-1, 0, 1) for dx in (-1, 0, 1) if dy or dx]
    barrier = pltpu.get_barrier_semaphore()
    near = shape["gz"] == 2 and shape["gy"] <= 4 and shape["gx"] <= 4
    if near:
        greeted = [(-1, 0, 0), (1, 0, 0)] + plane
        for o in greeted:
            @pl.when(both(o))
            def _(o=o):
                pl.semaphore_signal(barrier, inc=1, device_id=at(gz=o[0], gy=o[1], gx=o[2]),
                                    device_id_type=MESH)
        arrivals = sum(both(o).astype(jnp.int32) for o in greeted)
    else:
        partners = set()
        for axes in stages:
            for o in offsets(axes, shape):
                partners.add(tuple(dict(zip(axes, o)).get(a, 0) for a in AXES))
        for d in [(-1, 0, 0), (1, 0, 0)] + plane:
            o = tuple(d % shape[a] for a, d in zip(AXES, d))
            if any(o):
                partners.add(o)
        partners = sorted(partners)
        for o in partners:
            target = {a: lax.rem(me[a] + d, shape[a]) for a, d in zip(AXES, o)}
            pl.semaphore_signal(barrier, inc=1, device_id=target, device_id_type=MESH)
        arrivals = len(partners)

    load = pltpu.make_async_copy(
        sens_ref, pad.at[:, 1 : nx + 1, SUB : SUB + ny, :], load_sem.at[0]
    )
    load.start()
    small = [
        pltpu.make_async_copy(src, dst, load_sem.at[1 + i])
        for i, (src, dst) in enumerate([
            (span_hbm, span_ref), (dens_hbm, dens_ref), (viol_hbm, viol_ref), (lam0_hbm, lam0_ref)])
    ]
    for copy in small:
        copy.start()

    lane = lax.broadcasted_iota(jnp.int32, (SUB, LANE), 1)
    row = lax.broadcasted_iota(jnp.int32, (SUB, LANE), 0)
    zero = jnp.zeros((SUB, LANE), jnp.float32)

    for i, sx in enumerate((1, -1)):
        @pl.when(jnp.logical_not(has["gx", -sx]))
        def _(i=i):
            pad[:, i * (nx + 1), SUB : SUB + ny, :] = jnp.zeros((FIELDS, ny, LANE), jnp.float32)
    for i, sy in enumerate((1, -1)):
        @pl.when(jnp.logical_not(has["gy", -sy]))
        def _(i=i):
            yrecv[i] = jnp.zeros((FIELDS, nx, LANE), jnp.float32)
    for i, sz in enumerate((1, -1)):
        @pl.when(jnp.logical_not(has["gz", -sz]))
        def _(i=i):
            zrecv[i] = jnp.zeros(zrecv.shape[1:], jnp.float32)
    corners = [(sx, sy) for sx in (1, -1) for sy in (1, -1)]
    for i, (sx, sy) in enumerate(corners):
        @pl.when(jnp.logical_not(jnp.logical_and(has["gx", -sx], has["gy", -sy])))
        def _(i=i):
            crecv[i] = jnp.zeros((FIELDS, 1, LANE), jnp.float32)

    def count(a, index, extent):
        low = jnp.where(jnp.logical_and(me[a] == 0, index == 0), 0.0, 1.0)
        high = jnp.where(jnp.logical_and(me[a] == shape[a] - 1, index == extent - 1), 0.0, 1.0)
        return low + high
    cz = count("gz", lane, nz)
    for x in range(nx):
        cx = count("gx", jnp.full((SUB, LANE), x, jnp.int32), nx)
        for t in range(tiles):
            cy = count("gy", row + t * SUB, ny)
            den = W0 + W1 * (cx + cy + cz) + W2 * (cx * cy + cy * cz + cx * cz) + W3 * (cx * cy * cz)
            k = x * tiles + t
            invden[k] = 1.0 / den

    load.wait()

    for f in range(FIELDS):
        for i, y in enumerate((SUB + ny - 1, SUB)):
            for x in range(nx):
                ypack[i, f, x : x + 1, :] = pad[f, x + 1, y : y + 1, :]
        for i, (sx, sy) in enumerate(corners):
            x = nx if sx > 0 else 1
            y = SUB + ny - 1 if sy > 0 else SUB
            cpack[i, f] = pad[f, x, y : y + 1, :]

    pl.semaphore_wait(barrier, arrivals)

    groups = steps()
    count_of = len(groups)

    def moves_x(g):
        fields = pl.ds(groups[g][0], len(groups[g]))
        out = []
        for i, sx in enumerate((1, -1)):
            copy = pltpu.make_async_remote_copy(
                src_ref=pad.at[fields, nx if sx > 0 else 1, SUB : SUB + ny, :],
                dst_ref=pad.at[fields, 0 if sx > 0 else nx + 1, SUB : SUB + ny, :],
                send_sem=send_sem.at[6 + 4 * g + i], recv_sem=recv_sem.at[6 + 4 * g + i],
                device_id=at(gx=sx), device_id_type=MESH)
            out.append((has["gx", sx], has["gx", -sx], copy))
        return out

    moves_c, moves_y, moves_z = [], [], []
    for i, (sx, sy) in enumerate(corners):
        copy = pltpu.make_async_remote_copy(
            src_ref=cpack.at[i], dst_ref=crecv.at[i],
            send_sem=send_sem.at[2 + i], recv_sem=recv_sem.at[2 + i],
            device_id=at(gx=sx, gy=sy), device_id_type=MESH)
        moves_c.append((jnp.logical_and(has["gx", sx], has["gy", sy]),
                        jnp.logical_and(has["gx", -sx], has["gy", -sy]), copy))
    for i, sy in enumerate((1, -1)):
        copy = pltpu.make_async_remote_copy(
            src_ref=ypack.at[i], dst_ref=yrecv.at[i],
            send_sem=send_sem.at[i], recv_sem=recv_sem.at[i],
            device_id=at(gy=sy), device_id_type=MESH)
        moves_y.append((has["gy", sy], has["gy", -sy], copy))

    def start(moves):
        for send, _, copy in moves:
            pl.when(send)(copy.start)

    def receive(moves):
        for _, expected, copy in moves:
            pl.when(expected)(copy.wait_recv)

    xs = [moves_x(g) for g in range(count_of)]
    start(moves_c)
    start(xs[0])
    start(moves_y)
    for g in range(1, count_of):
        start(xs[g])
    receive(moves_c)
    receive(moves_y)

    ends = jnp.logical_or(lane == 0, lane == LANE - 1)

    def smooth(f, g):
        for i, y in enumerate((SUB - 1, SUB + ny)):
            for x in range(nx):
                pad[f, x + 1, y : y + 1, :] = yrecv[i, f, x : x + 1, :]
        for i, (sx, sy) in enumerate(corners):
            pad[f, 0 if sx > 0 else nx + 1, (SUB - 1 if sy > 0 else SUB + ny) : (SUB if sy > 0 else SUB + ny + 1), :] = crecv[i, f]
        packed = zero
        for t in range(tiles):
            y = SUB + t * SUB
            mids, sides = [], []
            for p in range(nx + 2):
                mids.append(pad[f, p, y : y + SUB, :])
                sides.append(pad[f, p, y - 1 : y - 1 + SUB, :] + pad[f, p, y + 1 : y + 1 + SUB, :])
            for x in range(nx):
                k = x * tiles + t
                near = sides[x + 1] + (mids[x] + mids[x + 2])
                far = sides[x] + sides[x + 2]
                s0 = W0 * mids[x + 1] + W1 * near + W2 * far
                s1 = W1 * mids[x + 1] + W2 * near + W3 * far
                up = pltpu.roll(s1, 1, 1)
                down = pltpu.roll(s1, LANE - 1, 1)
                mid[f, k] = s0 + jnp.where(lane == 0, 0.0, up) + jnp.where(lane == LANE - 1, 0.0, down)
                edge = jnp.where(lane == 0, up, down)
                if k:
                    edge = pltpu.roll(edge, 2 * k, 1)
                here = jnp.logical_or(lane == 2 * k, lane == (2 * k - 1) % LANE)
                packed = jnp.where(here, edge, packed)
        shift = (f - groups[g][0]) * (2 * chunks)
        return pltpu.roll(packed, shift, 1) if shift else packed

    even = (lane % 2) == 0
    for g in range(count_of):
        receive(xs[g])
        v = zero
        for f in groups[g]:
            v += smooth(f, g)
        zpack[0, g] = jnp.where(even, v, 0.0)
        zpack[1, g] = jnp.where(even, 0.0, v)
        zs = []
        for i, sz in enumerate((1, -1)):
            copy = pltpu.make_async_remote_copy(
                src_ref=zpack.at[i, g], dst_ref=zrecv.at[i, g],
                send_sem=send_sem.at[8 + 4 * g + i], recv_sem=recv_sem.at[8 + 4 * g + i],
                device_id=at(gz=sz), device_id_type=MESH)
            zs.append((has["gz", sz], has["gz", -sz], copy))
        start(zs)
        moves_z.append(zs)

    def piece(ref, k):
        x, t = divmod(k, tiles)
        return ref[x, t * SUB : (t + 1) * SUB, :]

    def rows(f, g):
        outer = zrecv[0, g] + zrecv[1, g]
        shift = (f - groups[g][0]) * (2 * chunks)
        total = zero
        for k in range(chunks):
            turn = (LANE - shift - 2 * k) % LANE
            edge = pltpu.roll(outer, turn, 1) if turn else outer
            r = (mid[f, k] + jnp.where(ends, edge, 0.0)) * invden[k]
            s = piece(span_ref, k)
            square = s * s
            gp = jnp.maximum(r, 0.0)
            gm = jnp.maximum(-r, 0.0)
            pp[f, k] = square * (1.001 * gp + 0.001 * gm + RAA)
            qq[f, k] = square * (0.001 * gp + 1.001 * gm + RAA)
            total += s * (1.002 * (gp + gm) + 2 * RAA)
        if f:
            acc[SUMS - 1 + f] = total

    for copy in small:
        copy.wait()
    for g in range(count_of):
        receive(moves_z[g])
        if near and g == 0:
            for o in plane:
                @pl.when(both(o))
                def _(o=o):
                    pl.semaphore_signal(known, inc=1, device_id=at(gy=o[1], gx=o[2]),
                                        device_id_type=MESH)
        for f in groups[g]:
            rows(f, g)
    total = zero
    for k in range(chunks):
        s = piece(span_ref, k)
        square = s * s
        pp[FIELDS, k] = square * (1.001 + RAA)
        qq[FIELDS, k] = square * (0.001 + RAA)
        total += s * (1.002 + 2 * RAA)
    acc[ROWS - 1] = total
    for k in range(FIELDS):
        lam[k] = jnp.full((SUB, LANE), lam0_ref[k], jnp.float32)

    def respond(k, weights):
        big_p, big_q = pp[0, k], qq[0, k]
        for j in range(FIELDS):
            big_p += weights[j] * pp[j + 1, k]
            big_q += weights[j] * qq[j + 1, k]
        s = piece(span_ref, k)
        d = piece(dens_ref, k)
        root_p = jnp.sqrt(big_p)
        root_q = jnp.sqrt(big_q)
        lower, upper = d - s, d + s
        moved = (root_p * lower + root_q * upper) / (root_p + root_q)
        low = jnp.maximum(0.0, d - MOVE * s)
        high = jnp.minimum(1.0, d + MOVE * s)
        return jnp.minimum(jnp.maximum(moved, low), high), big_p, big_q, lower, upper

    def flat(axes):
        index = 0
        for a in axes:
            index = index * shape[a] + me[a]
        return index

    def newton(it, carry):
        weights = [lam[j] for j in range(FIELDS)]
        grads = [zero] * FIELDS
        for k in range(chunks):
            moved, big_p, big_q, lower, upper = respond(k, weights)
            ia = 1.0 / (upper - moved)
            ib = 1.0 / (moved - lower)
            ia2, ib2 = ia * ia, ib * ib
            inv = 1.0 / (2.0 * big_p * (ia2 * ia) + 2.0 * big_q * (ib2 * ib))
            for j in range(FIELDS):
                p, q = pp[j + 1, k], qq[j + 1, k]
                grads[j] += p * ia + q * ib
                a = p * ia2 - q * ib2
                slope[j, k] = a
                scaled[j, k] = a * inv
        for j in range(FIELDS):
            acc[j] = grads[j]
        at_row = FIELDS
        for group in ((0, 1), (2, 3), (4, 5, 6, 7, 8)):
            sums = {(i, j): zero for i in group for j in range(i, FIELDS)}
            for k in range(chunks):
                right = {j: slope[j, k] for j in range(group[0], FIELDS)}
                for i in group:
                    left = scaled[i, k]
                    for j in range(i, FIELDS):
                        sums[i, j] += left * right[j]
            for key in sums:
                acc[at_row] = sums[key]
                at_row += 1

        packed = zero
        for r in range(ROWS):
            packed = jnp.where(lane == r, jnp.sum(acc[r], axis=1, keepdims=True), packed)
        value = jnp.sum(packed, axis=0, keepdims=True)
        for n, axes in enumerate(stages):
            size = math.prod(shape[a] for a in axes)
            part[it, n] = value
            recvs[n][it, flat(axes)] = value
            for o in sorted(offsets(axes, shape), key=lambda o: (-abs(o[-1] - 2), o), reverse=True):
                target = {a: lax.rem(me[a] + d, shape[a]) for a, d in zip(axes, o)}
                pltpu.make_async_remote_copy(
                    src_ref=part.at[it, n], dst_ref=recvs[n].at[it, flat(axes)],
                    send_sem=sum_send.at[it, n], recv_sem=sum_recv.at[it, n],
                    device_id=target, device_id_type=MESH).start()
            whole = recvs[n].at[it, pl.ds(0, size - 1)]
            pltpu.make_async_copy(whole, whole, sum_recv.at[it, n]).wait()
            values = [recvs[n][it, i] for i in range(size)]
            while len(values) > 1:
                values = [sum(values[i + 1 : i + 2], values[i]) for i in range(0, len(values), 2)]
            value = values[0]
        every = jnp.broadcast_to(value, (SUB, LANE))
        for g in range(wide.shape[0]):
            one = jnp.sum(jnp.where(lane == g * SUB + row, every, 0.0), axis=1, keepdims=True)
            wide[g] = jnp.broadcast_to(one, (SUB, LANE))

        def read(r):
            return jnp.broadcast_to(wide[r // SUB, r % SUB : r % SUB + 1, :], (SUB, LANE))
        b = [read(j) - (1.0 - viol_ref[j]) * read(SUMS + j) for j in range(FIELDS)]
        m = {}
        at_row = FIELDS
        for i in range(FIELDS):
            for j in range(i, FIELDS):
                m[i, j] = read(at_row)
                at_row += 1
        trace = m[0, 0]
        for i in range(1, FIELDS):
            trace += m[i, i]
        shift = REG * trace / FIELDS
        for i in range(FIELDS):
            m[i, i] += shift
        inverse = []
        for k in range(FIELDS):
            inverse.append(1.0 / m[k, k])
            for i in range(k + 1, FIELDS):
                factor = m[k, i] * inverse[k]
                for j in range(i, FIELDS):
                    m[i, j] -= factor * m[k, j]
                b[i] -= factor * b[k]
        delta = [None] * FIELDS
        for k in reversed(range(FIELDS)):
            v = b[k]
            for j in range(k + 1, FIELDS):
                v -= m[k, j] * delta[j]
            delta[k] = v * inverse[k]
        for k in range(FIELDS):
            lam[k] = jnp.maximum(weights[k] + delta[k], FLOOR * weights[k])
        return carry
    if near:
        pl.semaphore_wait(known, sum(both(o).astype(jnp.int32) for o in plane))
    lax.fori_loop(0, ITERS, newton, 0)

    weights = [lam[j] for j in range(FIELDS)]
    for k in range(chunks):
        x, t = divmod(k, tiles)
        out_ref[x, t * SUB : (t + 1) * SUB, :] = respond(k, weights)[0]
    final = zero
    for j in range(FIELDS):
        final = jnp.where(lane == j, weights[j], final)
    lam_out[...] = final

    for moves in [moves_c, moves_y] + xs + moves_z:
        for send, _, copy in moves:
            pl.when(send)(copy.wait_send)
    for it in range(ITERS):
        for n, axes in enumerate(stages):
            size = math.prod(shape[a] for a in axes)
            whole = recvs[n].at[it, pl.ds(0, size - 1)]
            pltpu.make_async_copy(whole, whole, sum_send.at[it, n]).wait()


def finish(field_ref, lam_ref, field_out, lam_out, row, sem):
    whole = pltpu.make_async_copy(field_ref, field_out, sem.at[0])
    whole.start()
    row[...] = lam_ref[0, :FIELDS]
    short = pltpu.make_async_copy(row, lam_out, sem.at[1])
    short.start()
    whole.wait()
    short.wait()


def shards(shape, density, spread, sensitivities, violation, multipliers_start):
    nx, ny, nz = density.shape
    chunks = nx * ny // SUB
    groups = len(steps())
    stages = plan(shape)
    f32 = jnp.float32
    vmem = pl.BlockSpec(memory_space=pltpu.VMEM)
    dma = pltpu.SemaphoreType.DMA
    hbm = pl.BlockSpec(memory_space=pltpu.HBM)
    field, lam = pl.pallas_call(
        functools.partial(body, shape, (nx, ny, nz)),
        out_shape=(
            pltpu.VMEM((nx, ny, nz), f32),
            pltpu.VMEM((SUB, LANE), f32),
        ),
        in_specs=[hbm] * 5,
        out_specs=(vmem, vmem),
        scratch_shapes=[
            pltpu.VMEM((nx, ny, nz), f32),
            pltpu.VMEM((nx, ny, nz), f32),
            pltpu.SMEM((FIELDS,), f32),
            pltpu.SMEM((FIELDS,), f32),
            pltpu.VMEM((FIELDS, nx + 2, ny + 2 * SUB, nz), f32),
            pltpu.VMEM((2, FIELDS, nx, nz), f32),
            pltpu.VMEM((2, FIELDS, nx, nz), f32),
            pltpu.VMEM((4, FIELDS, 1, nz), f32),
            pltpu.VMEM((4, FIELDS, 1, nz), f32),
            pltpu.VMEM((2, groups, SUB, LANE), f32),
            pltpu.VMEM((2, groups, SUB, LANE), f32),
            pltpu.VMEM((FIELDS, chunks, SUB, LANE), f32),
            pltpu.VMEM((chunks, SUB, LANE), f32),
            pltpu.VMEM((FIELDS + 1, chunks, SUB, LANE), f32),
            pltpu.VMEM((FIELDS + 1, chunks, SUB, LANE), f32),
            pltpu.VMEM((FIELDS, chunks, SUB, LANE), f32),
            pltpu.VMEM((FIELDS, chunks, SUB, LANE), f32),
            pltpu.VMEM((ROWS, SUB, LANE), f32),
            pltpu.VMEM((-(-ROWS // SUB), SUB, LANE), f32),
            pltpu.VMEM((FIELDS, SUB, LANE), f32),
            pltpu.VMEM((ITERS, len(stages), 1, LANE), f32),
        ] + [
            pltpu.VMEM((ITERS, math.prod(shape[a] for a in axes), 1, LANE), f32) for axes in stages
        ] + [
            dma((5,)), dma((6 + 4 * groups,)), dma((6 + 4 * groups,)),
            dma((ITERS, len(stages))), dma((ITERS, len(stages))), pltpu.SemaphoreType.REGULAR,
        ],
        compiler_params=pltpu.CompilerParams(
            collective_id=0, has_side_effects=True, vmem_limit_bytes=24 << 20),
        name="design_step",
    )(*[pltpu.with_memory_space_constraint(v, pltpu.HBM) for v in (density, spread, sensitivities, violation, multipliers_start)])
    return pl.pallas_call(
        finish,
        out_shape=(
            jax.ShapeDtypeStruct((nx, ny, nz), f32),
            jax.ShapeDtypeStruct((FIELDS,), f32),
        ),
        in_specs=[vmem, vmem],
        out_specs=(hbm, hbm),
        scratch_shapes=[pltpu.VMEM((FIELDS,), f32), dma((2,))],
        compiler_params=pltpu.CompilerParams(vmem_limit_bytes=1 << 20),
        name="finish",
    )(field, lam)


def solution(mesh):
    shape = {a: int(mesh.shape[a]) for a in AXES}
    return jax.shard_map(
        functools.partial(shards, shape),
        mesh=mesh,
        in_specs=(P("gx", "gy", "gz"), P("gx", "gy", "gz"), P(None, "gx", "gy", "gz"), P(), P()),
        out_specs=(P("gx", "gy", "gz"), P()),
        check_vma=False,
    )
```

```python
import functools
import math

import jax
import jax.numpy as jnp
from jax import lax
from jax.experimental import pallas as pl
from jax.experimental.pallas import tpu as pltpu
from jax.sharding import PartitionSpec as P

FIELDS = 9
ITERS = 3

RADIUS = 3.0
RAA = 1e-05
MOVE = 0.9
REG = 0.001
FLOOR = 0.2

W0 = RADIUS
W1 = RADIUS - 1.0
W2 = RADIUS - math.sqrt(2.0)
W3 = RADIUS - math.sqrt(3.0)

SUB, LANE = 8, 128
AXES = ("gz", "gy", "gx")
SUMS = FIELDS + FIELDS * (FIELDS + 1) // 2
ROWS = SUMS + FIELDS
MESH = pl.DeviceIdType.MESH
GROUP = 3


def plan(shape):
    total = math.prod(shape[a] for a in AXES)
    if total <= 32:
        return (AXES,)
    return tuple((a,) for a in AXES)


def offsets(axes, shape):
    out = [()]
    for a in axes:
        out = [o + (d,) for o in out for d in range(shape[a])]
    return [o for o in out if any(o)]


def steps():
    return [range(f, min(f + GROUP, FIELDS)) for f in range(0, FIELDS, GROUP)]


def body(shape, dims, dens_hbm, span_hbm, sens_ref, viol_hbm, lam0_hbm, out_ref, lam_out,
         dens_ref, span_ref, viol_ref, lam0_ref, pad, xpad, ypack, yrecv, cpack, crecv, ycorr,
         zpack, zrecv, xzpack, xzrecv, yzpack, yzrecv, czrecv, around, mid, invden, pp, qq, slope, scaled,
         acc, wide, lam, part, *rest):
    stages = plan(shape)
    recvs = rest[: len(stages)]
    load_sem, send_sem, recv_sem, zsend_sem, zrecv_sem, sum_send, sum_recv, known = rest[len(stages):]
    nx, ny, nz = dims
    tiles = ny // SUB
    chunks = nx * tiles
    slots = 2 * chunks
    wide_x = 2 * tiles
    groups = steps()
    count_of = len(groups)
    me = {a: lax.axis_index(a) for a in AXES}

    has = {}
    for a in AXES:
        has[a, -1] = me[a] > 0
        has[a, 0] = jnp.bool_(True)
        has[a, 1] = me[a] < shape[a] - 1

    def both(o):
        moved = [has[a, d] for a, d in zip(AXES, o) if d]
        return functools.reduce(jnp.logical_and, moved)

    def at(**moves):
        return {a: me[a] + d for a, d in moves.items()}

    signs = (-1, 0, 1)
    plane = [(0, dy, dx) for dy in signs for dx in signs if dy or dx]
    ring = [(dz, dy, dx) for dz in signs for dy in signs for dx in signs if dz or dy or dx]
    barrier = pltpu.get_barrier_semaphore()
    near = shape["gz"] == 2 and shape["gy"] <= 4 and shape["gx"] <= 4
    if near:
        for o in ring:
            @pl.when(both(o))
            def _(o=o):
                pl.semaphore_signal(barrier, inc=1, device_id=at(gz=o[0], gy=o[1], gx=o[2]),
                                    device_id_type=MESH)
        arrivals = sum(both(o).astype(jnp.int32) for o in ring)
    else:
        partners = set()
        for axes in stages:
            for o in offsets(axes, shape):
                partners.add(tuple(dict(zip(axes, o)).get(a, 0) for a in AXES))
        for d in ring:
            o = tuple(d % shape[a] for a, d in zip(AXES, d))
            if any(o):
                partners.add(o)
        partners = sorted(partners)
        for o in partners:
            target = {a: lax.rem(me[a] + d, shape[a]) for a, d in zip(AXES, o)}
            pl.semaphore_signal(barrier, inc=1, device_id=target, device_id_type=MESH)
        arrivals = len(partners)

    load = pltpu.make_async_copy(
        sens_ref, pad.at[:, :, SUB : SUB + ny, :], load_sem.at[0]
    )
    load.start()
    small = [
        pltpu.make_async_copy(src, dst, load_sem.at[1 + i])
        for i, (src, dst) in enumerate([
            (span_hbm, span_ref), (dens_hbm, dens_ref), (viol_hbm, viol_ref), (lam0_hbm, lam0_ref)])
    ]
    for copy in small:
        copy.start()

    lane = lax.broadcasted_iota(jnp.int32, (SUB, LANE), 1)
    row = lax.broadcasted_iota(jnp.int32, (SUB, LANE), 0)
    zero = jnp.zeros((SUB, LANE), jnp.float32)
    slot = lane % slots
    x_of = slot // wide_x
    t_of = (slot % wide_x) // 2
    odd = (lane % 2) == 1
    ends = jnp.logical_or(lane == 0, lane == LANE - 1)

    corners = [(sx, sy) for sx in (1, -1) for sy in (1, -1)]
    line = jnp.zeros((1, LANE), jnp.float32)
    for f in range(FIELDS):
        for x in range(nx):
            pad[f, x, SUB - 1 : SUB, :] = line
            pad[f, x, SUB + ny : SUB + ny + 1, :] = line
        for i in range(2):
            xpad[i, f, SUB - 1 : SUB, :] = line
            xpad[i, f, SUB + ny : SUB + ny + 1, :] = line
    for i, sx in enumerate((1, -1)):
        @pl.when(jnp.logical_not(has["gx", -sx]))
        def _(i=i):
            xpad[i, :, SUB : SUB + ny, :] = jnp.zeros((FIELDS, ny, LANE), jnp.float32)
    for i, sy in enumerate((1, -1)):
        @pl.when(jnp.logical_not(has["gy", -sy]))
        def _(i=i):
            yrecv[i] = jnp.zeros((FIELDS, nx, LANE), jnp.float32)
    for i, (sx, sy) in enumerate(corners):
        @pl.when(jnp.logical_not(jnp.logical_and(has["gx", -sx], has["gy", -sy])))
        def _(i=i):
            crecv[i] = jnp.zeros((FIELDS, 1, LANE), jnp.float32)
    for i, sz in enumerate((1, -1)):
        @pl.when(jnp.logical_not(has["gz", -sz]))
        def _(i=i):
            zrecv[i] = jnp.zeros(zrecv.shape[1:], jnp.float32)
        for n, sx in enumerate((1, -1)):
            @pl.when(jnp.logical_not(jnp.logical_and(has["gz", -sz], has["gx", -sx])))
            def _(i=i, n=n):
                xzrecv[i, n] = zero
        for n, sy in enumerate((1, -1)):
            @pl.when(jnp.logical_not(jnp.logical_and(has["gz", -sz], has["gy", -sy])))
            def _(i=i, n=n):
                yzrecv[i, n] = zero
        for n, (sx, sy) in enumerate(corners):
            @pl.when(jnp.logical_not(both((-sz, -sy, -sx))))
            def _(i=i, n=n):
                czrecv[i, n] = zero

    def count(a, index, extent):
        low = jnp.where(jnp.logical_and(me[a] == 0, index == 0), 0.0, 1.0)
        high = jnp.where(jnp.logical_and(me[a] == shape[a] - 1, index == extent - 1), 0.0, 1.0)
        return low + high
    cz = count("gz", lane, nz)
    for x in range(nx):
        cx = count("gx", jnp.full((SUB, LANE), x, jnp.int32), nx)
        for t in range(tiles):
            cy = count("gy", row + t * SUB, ny)
            den = W0 + W1 * (cx + cy + cz) + W2 * (cx * cy + cy * cz + cx * cz) + W3 * (cx * cy * cz)
            k = x * tiles + t
            invden[k] = 1.0 / den

    load.wait()

    def turned(value, shift, axis=1):
        shift %= value.shape[axis]
        return pltpu.roll(value, shift, axis) if shift else value

    def place(packed, value, k, j):
        here = lane // 2 == k + j * chunks
        return jnp.where(here, turned(value, 2 * k + 1 + j * slots), packed)

    edges = []
    for g, fields in enumerate(groups):
        packed = zero
        for j, f in enumerate(fields):
            for k in range(chunks):
                x, t = divmod(k, tiles)
                packed = place(packed, pad[f, x, SUB + t * SUB : 2 * SUB + t * SUB, :], k, j)
        zpack[g] = packed
        edges.append(packed)
    for n, x in enumerate((nx - 1, 0)):
        packed = zero
        for g in range(count_of):
            packed = jnp.where(x_of == g, turned(edges[g], (g - x) * wide_x), packed)
        xzpack[n] = packed
    for n, y in enumerate((SUB - 1, 0)):
        packed = zero
        for g in range(count_of):
            packed = jnp.where(row == g, jnp.broadcast_to(edges[g][y : y + 1, :], (SUB, LANE)), packed)
        yzpack[n] = packed
    for f in range(FIELDS):
        for i, y in enumerate((SUB + ny - 1, SUB)):
            for x in range(nx):
                ypack[i, f, x : x + 1, :] = pad[f, x, y : y + 1, :]
        for i, (sx, sy) in enumerate(corners):
            x = nx - 1 if sx > 0 else 0
            y = SUB + ny - 1 if sy > 0 else SUB
            cpack[i, f] = pad[f, x, y : y + 1, :]

    pl.semaphore_wait(barrier, arrivals)

    def remote(src, dst, sends, recvs_, index, **moves):
        copy = pltpu.make_async_remote_copy(
            src_ref=src, dst_ref=dst, send_sem=sends.at[index], recv_sem=recvs_.at[index],
            device_id=at(**moves), device_id_type=MESH)
        there = functools.reduce(jnp.logical_and, [has[a, d] for a, d in moves.items()])
        back = functools.reduce(jnp.logical_and, [has[a, -d] for a, d in moves.items()])
        return there, back, copy

    def moves_x(g):
        fields = pl.ds(groups[g][0], len(groups[g]))
        return [
            remote(pad.at[fields, nx - 1 if sx > 0 else 0, SUB : SUB + ny, :],
                   xpad.at[i, fields, SUB : SUB + ny, :], send_sem, recv_sem, 6 + 2 * g + i, gx=sx)
            for i, sx in enumerate((1, -1))
        ]

    moves_c = [remote(cpack.at[i], crecv.at[i], send_sem, recv_sem, 2 + i, gx=sx, gy=sy)
               for i, (sx, sy) in enumerate(corners)]
    moves_y = [remote(ypack.at[i], yrecv.at[i], send_sem, recv_sem, i, gy=sy)
               for i, sy in enumerate((1, -1))]
    moves_z = []
    for i, sz in enumerate((1, -1)):
        first = 0 if shape["gz"] == 2 else 9 * i
        for n, (sx, sy) in enumerate(corners):
            moves_z.append(remote(yzpack.at[n % 2], czrecv.at[i, n], zsend_sem, zrecv_sem, first + 5 + n,
                                  gz=sz, gx=sx, gy=sy))
        for n, sx in enumerate((1, -1)):
            moves_z.append(remote(xzpack.at[n], xzrecv.at[i, n], zsend_sem, zrecv_sem, first + 1 + n,
                                  gz=sz, gx=sx))
        for n, sy in enumerate((1, -1)):
            moves_z.append(remote(yzpack.at[n], yzrecv.at[i, n], zsend_sem, zrecv_sem, first + 3 + n,
                                  gz=sz, gy=sy))
        moves_z.append(remote(zpack, zrecv.at[i], zsend_sem, zrecv_sem, first, gz=sz))

    def start(moves):
        for send, _, copy in moves:
            pl.when(send)(copy.start)

    def receive(moves):
        for _, expected, copy in moves:
            pl.when(expected)(copy.wait_recv)

    xs = [moves_x(g) for g in range(count_of)]
    start(moves_z)
    start(moves_c)
    start(xs[0])
    start(moves_y)
    for g in range(1, count_of):
        start(xs[g])

    def along(s0, s1):
        up = jnp.where(lane == 0, 0.0, pltpu.roll(s1, 1, 1))
        down = jnp.where(lane == LANE - 1, 0.0, pltpu.roll(s1, LANE - 1, 1))
        return s0 + up + down

    for f in range(FIELDS):
        for t in range(tiles):
            y = SUB + t * SUB
            mids, sides = [None], [None]
            for x in range(nx):
                mids.append(pad[f, x, y : y + SUB, :])
                sides.append(pad[f, x, y - 1 : y - 1 + SUB, :] + pad[f, x, y + 1 : y + 1 + SUB, :])
            mids.append(None)
            sides.append(None)
            for x in range(nx):
                next_to = [v for v in (mids[x], mids[x + 2]) if v is not None]
                beyond = [v for v in (sides[x], sides[x + 2]) if v is not None]
                close = sides[x + 1] + sum(next_to[1:], next_to[0])
                far = sum(beyond[1:], beyond[0])
                s0 = W0 * mids[x + 1] + W1 * close + W2 * far
                s1 = W1 * mids[x + 1] + W2 * close + W3 * far
                mid[f, x * tiles + t] = along(s0, s1)

    def piece(ref, k):
        x, t = divmod(k, tiles)
        return ref[x, t * SUB : (t + 1) * SUB, :]

    for copy in small:
        copy.wait()
    for n, ref in enumerate((span_ref, dens_ref, invden)):
        packed = zero
        for k in range(chunks):
            value = ref[k] if n == 2 else piece(ref, k)
            for j in range(LANE // slots):
                packed = place(packed, value, k, j)
        around[n] = packed
    for k in range(FIELDS):
        lam[k] = jnp.full((SUB, LANE), lam0_ref[k], jnp.float32)
    total = zero
    for k in range(chunks):
        s = piece(span_ref, k)
        square = s * s
        pp[FIELDS, k] = square * (1.001 + RAA)
        qq[FIELDS, k] = square * (0.001 + RAA)
        total += s * (1.002 + 2 * RAA)
    acc[ROWS - 1] = total

    receive(moves_c)
    receive(moves_y)
    x_row = lax.broadcasted_iota(jnp.int32, (nx, LANE), 0)
    x_lane = lax.broadcasted_iota(jnp.int32, (nx, LANE), 1)
    for i in range(2):
        for f in range(FIELDS):
            h = yrecv[i, f]
            low = jnp.broadcast_to(crecv[i, f], (nx, LANE))
            high = jnp.broadcast_to(crecv[2 + i, f], (nx, LANE))
            pair = jnp.where(x_row == 0, low, pltpu.roll(h, 1, 0)) + jnp.where(x_row == nx - 1, high, pltpu.roll(h, nx - 1, 0))
            s0 = W1 * h + W2 * pair
            s1 = W2 * h + W3 * pair
            up = jnp.where(x_lane == 0, 0.0, pltpu.roll(s1, 1, 1))
            down = jnp.where(x_lane == LANE - 1, 0.0, pltpu.roll(s1, LANE - 1, 1))
            ycorr[i, f] = s0 + up + down

    def grown(r, s):
        gp = jnp.maximum(r, 0.0)
        gm = jnp.maximum(-r, 0.0)
        square = s * s
        p = square * (1.001 * gp + 0.001 * gm + RAA)
        q = square * (0.001 * gp + 1.001 * gm + RAA)
        return p, q, s * (1.002 * (gp + gm) + 2 * RAA)

    def rows(f, j, packed):
        total = zero
        for k in range(chunks):
            x, t = divmod(k, tiles)
            value = mid[f, k]
            if t == 0:
                value += jnp.where(row == 0, jnp.broadcast_to(ycorr[0, f, x : x + 1, :], (SUB, LANE)), 0.0)
            if t == tiles - 1:
                value += jnp.where(row == SUB - 1, jnp.broadcast_to(ycorr[1, f, x : x + 1, :], (SUB, LANE)), 0.0)
            for i in range(2):
                if x == (0, nx - 1)[i]:
                    y = SUB + t * SUB
                    h = xpad[i, f, y : y + SUB, :]
                    pair = xpad[i, f, y - 1 : y - 1 + SUB, :] + xpad[i, f, y + 1 : y + 1 + SUB, :]
                    value += along(W1 * h + W2 * pair, W2 * h + W3 * pair)
            packed = place(packed, value, k, j)
            pp[f, k], qq[f, k], base = grown(value * invden[k], piece(span_ref, k))
            total += base
        if f:
            acc[SUMS - 1 + f] = total
        return packed

    inner = []
    for g, fields in enumerate(groups):
        receive(xs[g])
        if near and g == 0:
            for o in plane:
                @pl.when(both(o))
                def _(o=o):
                    pl.semaphore_signal(known, inc=1, device_id=at(gy=o[1], gx=o[2]),
                                        device_id_type=MESH)
        packed = zero
        for j, f in enumerate(fields):
            packed = rows(f, j, packed)
        inner.append(packed)

    def respond(k, weights):
        big_p, big_q = pp[0, k], qq[0, k]
        for j in range(FIELDS):
            big_p += weights[j] * pp[j + 1, k]
            big_q += weights[j] * qq[j + 1, k]
        s = around[0] if k == chunks else piece(span_ref, k)
        d = around[1] if k == chunks else piece(dens_ref, k)
        root_p = jnp.sqrt(big_p)
        root_q = jnp.sqrt(big_q)
        lower, upper = d - s, d + s
        moved = (root_p * lower + root_q * upper) / (root_p + root_q)
        low = jnp.maximum(0.0, d - MOVE * s)
        high = jnp.minimum(1.0, d + MOVE * s)
        return jnp.minimum(jnp.maximum(moved, low), high), big_p, big_q, lower, upper

    def terms(k, weights):
        moved, big_p, big_q, lower, upper = respond(k, weights)
        ia = 1.0 / (upper - moved)
        ib = 1.0 / (moved - lower)
        ia2, ib2 = ia * ia, ib * ib
        inv = 1.0 / (2.0 * big_p * (ia2 * ia) + 2.0 * big_q * (ib2 * ib))
        grads, slopes, ratios = [], [], []
        for j in range(FIELDS):
            p, q = pp[j + 1, k], qq[j + 1, k]
            grads.append(p * ia + q * ib)
            a = p * ia2 - q * ib2
            slopes.append(a)
            ratios.append(a * inv)
        return grads, slopes, ratios

    def main_sums(weights):
        grads = [zero] * FIELDS
        for k in range(chunks):
            more, slopes, ratios = terms(k, weights)
            for j in range(FIELDS):
                grads[j] += more[j]
                slope[j, k] = slopes[j]
                scaled[j, k] = ratios[j]
        for j in range(FIELDS):
            acc[j] = grads[j]
        at_row = FIELDS
        for group in ((0, 1), (2, 3), (4, 5, 6, 7, 8)):
            sums = {(i, j): zero for i in group for j in range(i, FIELDS)}
            for k in range(chunks):
                right = {j: slope[j, k] for j in range(group[0], FIELDS)}
                for i in group:
                    left = scaled[i, k]
                    for j in range(i, FIELDS):
                        sums[i, j] += left * right[j]
            for key in sums:
                acc[at_row] = sums[key]
                at_row += 1

    def combined(ref, *index):
        return jnp.where(odd, pltpu.roll(ref[(0,) + index], 1, 1), pltpu.roll(ref[(1,) + index], LANE - 1, 1))

    def outer_edges():
        last_x, last_t = wide_x * (nx - 1), 2 * (tiles - 1)
        yz = [combined(yzrecv, n) for n in range(2)]
        xz = [combined(xzrecv, n) for n in range(2)]
        cz_ = [combined(czrecv, n) for n in range(4)]

        def pick(value, g, shift):
            return turned(jnp.broadcast_to(value[g : g + 1, :], (SUB, LANE)), shift)

        def beside(c, first, final):
            down = pltpu.roll(c, 1, 0)
            up = pltpu.roll(c, SUB - 1, 0)
            before = jnp.where(row == 0, jnp.where(t_of == 0, first, turned(down, 2)), down)
            after = jnp.where(row == SUB - 1, jnp.where(t_of == tiles - 1, final, turned(up, LANE - 2)), up)
            return before + after

        out = []
        for g in range(count_of):
            c = combined(zrecv, g)
            s = beside(c, pick(yz[0], g, -last_t), pick(yz[1], g, last_t))
            c_low = turned(xz[0], -wide_x * g)
            c_high = turned(xz[1], last_x - wide_x * g)
            s_low = beside(c_low, pick(cz_[0], g, -last_x - last_t), pick(cz_[1], g, -last_x + last_t))
            s_high = beside(c_high, pick(cz_[2], g, last_x - last_t), pick(cz_[3], g, last_x + last_t))

            def pair(own, low, high):
                return (jnp.where(x_of == 0, low, turned(own, wide_x))
                        + jnp.where(x_of == nx - 1, high, turned(own, -wide_x)))
            out.append(W1 * c + W2 * (s + pair(c, c_low, c_high)) + W3 * pair(s, s_low, s_high))
        return out

    def edge_rows():
        outer = outer_edges()
        s = around[0]
        bases = []
        for g, fields in enumerate(groups):
            p, q, base = grown((inner[g] + outer[g]) * around[2], s)
            for j, f in enumerate(fields):
                pp[f, chunks] = turned(p, -j * slots)
                qq[f, chunks] = turned(q, -j * slots)
                bases.append(turned(base, -j * slots))
        pp[FIELDS, chunks] = s * s * (1.001 + RAA)
        qq[FIELDS, chunks] = s * s * (0.001 + RAA)
        return bases[1:] + [s * (1.002 + 2 * RAA)]

    def edge_sums(weights, bases):
        grads, slopes, ratios = terms(chunks, weights)
        more = grads + [ratios[i] * slopes[j] for i in range(FIELDS) for j in range(i, FIELDS)] + bases
        for r in range(ROWS):
            acc[r] = jnp.where(ends, 0.0, acc[r]) + jnp.where(lane < slots, more[r], 0.0)

    def repair():
        for f in range(FIELDS):
            p, q = pp[f, chunks], qq[f, chunks]
            for k in range(chunks):
                pp[f, k] = jnp.where(ends, turned(p, -2 * k - 1), pp[f, k])
                qq[f, k] = jnp.where(ends, turned(q, -2 * k - 1), qq[f, k])

    def flat(axes):
        index = 0
        for a in axes:
            index = index * shape[a] + me[a]
        return index

    def exchange(it, meanwhile):
        packed = zero
        for r in range(ROWS):
            packed = jnp.where(lane == r, jnp.sum(acc[r], axis=1, keepdims=True), packed)
        value = jnp.sum(packed, axis=0, keepdims=True)
        for n, axes in enumerate(stages):
            size = math.prod(shape[a] for a in axes)
            part[it, n] = value
            recvs[n][it, flat(axes)] = value
            for o in sorted(offsets(axes, shape), key=lambda o: (-abs(o[-1] - 2), o), reverse=True):
                target = {a: lax.rem(me[a] + d, shape[a]) for a, d in zip(axes, o)}
                pltpu.make_async_remote_copy(
                    src_ref=part.at[it, n], dst_ref=recvs[n].at[it, flat(axes)],
                    send_sem=sum_send.at[it, n], recv_sem=sum_recv.at[it, n],
                    device_id=target, device_id_type=MESH).start()
            if n == 0:
                meanwhile()
            whole = recvs[n].at[it, pl.ds(0, size - 1)]
            pltpu.make_async_copy(whole, whole, sum_recv.at[it, n]).wait()
            values = [recvs[n][it, i] for i in range(size)]
            while len(values) > 1:
                values = [sum(values[i + 1 : i + 2], values[i]) for i in range(0, len(values), 2)]
            value = values[0]
        every = jnp.broadcast_to(value, (SUB, LANE))
        for g in range(wide.shape[0]):
            one = jnp.sum(jnp.where(lane == g * SUB + row, every, 0.0), axis=1, keepdims=True)
            wide[g] = jnp.broadcast_to(one, (SUB, LANE))

    def solve(weights):
        def read(r):
            return jnp.broadcast_to(wide[r // SUB, r % SUB : r % SUB + 1, :], (SUB, LANE))
        b = [read(j) - (1.0 - viol_ref[j]) * read(SUMS + j) for j in range(FIELDS)]
        m = {}
        at_row = FIELDS
        for i in range(FIELDS):
            for j in range(i, FIELDS):
                m[i, j] = read(at_row)
                at_row += 1
        trace = m[0, 0]
        for i in range(1, FIELDS):
            trace += m[i, i]
        shift = REG * trace / FIELDS
        for i in range(FIELDS):
            m[i, i] += shift
        inverse = []
        for k in range(FIELDS):
            inverse.append(1.0 / m[k, k])
            for i in range(k + 1, FIELDS):
                factor = m[k, i] * inverse[k]
                for j in range(i, FIELDS):
                    m[i, j] -= factor * m[k, j]
                b[i] -= factor * b[k]
        delta = [None] * FIELDS
        for k in reversed(range(FIELDS)):
            v = b[k]
            for j in range(k + 1, FIELDS):
                v -= m[k, j] * delta[j]
            delta[k] = v * inverse[k]
        for k in range(FIELDS):
            lam[k] = jnp.maximum(weights[k] + delta[k], FLOOR * weights[k])

    def newton(it, carry):
        weights = [lam[j] for j in range(FIELDS)]
        main_sums(weights)
        exchange(it, lambda: None)
        solve(weights)
        return carry

    weights = [lam[j] for j in range(FIELDS)]
    main_sums(weights)
    receive(moves_z)
    edge_sums(weights, edge_rows())
    if near:
        pl.semaphore_wait(known, sum(both(o).astype(jnp.int32) for o in plane))
    exchange(0, repair)
    solve(weights)
    lax.fori_loop(1, ITERS, newton, 0)

    weights = [lam[j] for j in range(FIELDS)]
    for k in range(chunks):
        x, t = divmod(k, tiles)
        out_ref[x, t * SUB : (t + 1) * SUB, :] = respond(k, weights)[0]
    final = zero
    for j in range(FIELDS):
        final = jnp.where(lane == j, weights[j], final)
    lam_out[...] = final

    for moves in [moves_c, moves_y] + xs + [moves_z]:
        for send, _, copy in moves:
            pl.when(send)(copy.wait_send)
    for it in range(ITERS):
        for n, axes in enumerate(stages):
            size = math.prod(shape[a] for a in axes)
            whole = recvs[n].at[it, pl.ds(0, size - 1)]
            pltpu.make_async_copy(whole, whole, sum_send.at[it, n]).wait()


def finish(field_ref, lam_ref, field_out, lam_out, row, sem):
    whole = pltpu.make_async_copy(field_ref, field_out, sem.at[0])
    whole.start()
    row[...] = lam_ref[0, :FIELDS]
    short = pltpu.make_async_copy(row, lam_out, sem.at[1])
    short.start()
    whole.wait()
    short.wait()


def shards(shape, density, spread, sensitivities, violation, multipliers_start):
    nx, ny, nz = density.shape
    chunks = nx * ny // SUB
    groups = len(steps())
    stages = plan(shape)
    corners = 9 if shape["gz"] == 2 else 18
    f32 = jnp.float32
    vmem = pl.BlockSpec(memory_space=pltpu.VMEM)
    dma = pltpu.SemaphoreType.DMA
    hbm = pl.BlockSpec(memory_space=pltpu.HBM)
    field, lam = pl.pallas_call(
        functools.partial(body, shape, (nx, ny, nz)),
        out_shape=(
            pltpu.VMEM((nx, ny, nz), f32),
            pltpu.VMEM((SUB, LANE), f32),
        ),
        in_specs=[hbm] * 5,
        out_specs=(vmem, vmem),
        scratch_shapes=[
            pltpu.VMEM((nx, ny, nz), f32),
            pltpu.VMEM((nx, ny, nz), f32),
            pltpu.SMEM((FIELDS,), f32),
            pltpu.SMEM((FIELDS,), f32),
            pltpu.VMEM((FIELDS, nx, ny + 2 * SUB, nz), f32),
            pltpu.VMEM((2, FIELDS, ny + 2 * SUB, nz), f32),
            pltpu.VMEM((2, FIELDS, nx, nz), f32),
            pltpu.VMEM((2, FIELDS, nx, nz), f32),
            pltpu.VMEM((4, FIELDS, 1, nz), f32),
            pltpu.VMEM((4, FIELDS, 1, nz), f32),
            pltpu.VMEM((2, FIELDS, nx, nz), f32),
            pltpu.VMEM((groups, SUB, LANE), f32),
            pltpu.VMEM((2, groups, SUB, LANE), f32),
            pltpu.VMEM((2, SUB, LANE), f32),
            pltpu.VMEM((2, 2, SUB, LANE), f32),
            pltpu.VMEM((2, SUB, LANE), f32),
            pltpu.VMEM((2, 2, SUB, LANE), f32),
            pltpu.VMEM((2, 4, SUB, LANE), f32),
            pltpu.VMEM((3, SUB, LANE), f32),
            pltpu.VMEM((FIELDS, chunks, SUB, LANE), f32),
            pltpu.VMEM((chunks, SUB, LANE), f32),
            pltpu.VMEM((FIELDS + 1, chunks + 1, SUB, LANE), f32),
            pltpu.VMEM((FIELDS + 1, chunks + 1, SUB, LANE), f32),
            pltpu.VMEM((FIELDS, chunks, SUB, LANE), f32),
            pltpu.VMEM((FIELDS, chunks, SUB, LANE), f32),
            pltpu.VMEM((ROWS, SUB, LANE), f32),
            pltpu.VMEM((-(-ROWS // SUB), SUB, LANE), f32),
            pltpu.VMEM((FIELDS, SUB, LANE), f32),
            pltpu.VMEM((ITERS, len(stages), 1, LANE), f32),
        ] + [
            pltpu.VMEM((ITERS, math.prod(shape[a] for a in axes), 1, LANE), f32) for axes in stages
        ] + [
            dma((5,)), dma((6 + 2 * groups,)), dma((6 + 2 * groups,)), dma((corners,)), dma((corners,)),
            dma((ITERS, len(stages))), dma((ITERS, len(stages))), pltpu.SemaphoreType.REGULAR,
        ],
        compiler_params=pltpu.CompilerParams(
            collective_id=0, has_side_effects=True, vmem_limit_bytes=24 << 20),
        name="design_step",
    )(*[pltpu.with_memory_space_constraint(v, pltpu.HBM) for v in (density, spread, sensitivities, violation, multipliers_start)])
    return pl.pallas_call(
        finish,
        out_shape=(
            jax.ShapeDtypeStruct((nx, ny, nz), f32),
            jax.ShapeDtypeStruct((FIELDS,), f32),
        ),
        in_specs=[vmem, vmem],
        out_specs=(hbm, hbm),
        scratch_shapes=[pltpu.VMEM((FIELDS,), f32), dma((2,))],
        compiler_params=pltpu.CompilerParams(vmem_limit_bytes=1 << 20),
        name="finish",
    )(field, lam)


def solution(mesh):
    shape = {a: int(mesh.shape[a]) for a in AXES}
    return jax.shard_map(
        functools.partial(shards, shape),
        mesh=mesh,
        in_specs=(P("gx", "gy", "gz"), P("gx", "gy", "gz"), P(None, "gx", "gy", "gz"), P(), P()),
        out_specs=(P("gx", "gy", "gz"), P()),
        check_vma=False,
    )
```

```python
import functools
import math

import jax
import jax.numpy as jnp
from jax import lax
from jax.experimental import pallas as pl
from jax.experimental.pallas import tpu as pltpu
from jax.sharding import PartitionSpec as P

FIELDS = 9
ITERS = 3

RADIUS = 3.0
RAA = 1e-05
MOVE = 0.9
REG = 0.001
FLOOR = 0.2

W0 = RADIUS
W1 = RADIUS - 1.0
W2 = RADIUS - math.sqrt(2.0)
W3 = RADIUS - math.sqrt(3.0)

SUB, LANE = 8, 128
AXES = ("gz", "gy", "gx")
SUMS = FIELDS + FIELDS * (FIELDS + 1) // 2
ROWS = SUMS + FIELDS
MESH = pl.DeviceIdType.MESH
GROUP = 3


def plan(shape):
    total = math.prod(shape[a] for a in AXES)
    if total <= 32:
        return (AXES,)
    return tuple((a,) for a in AXES)


def offsets(axes, shape):
    out = [()]
    for a in axes:
        out = [o + (d,) for o in out for d in range(shape[a])]
    return [o for o in out if any(o)]


def steps():
    return [range(f, min(f + GROUP, FIELDS)) for f in range(0, FIELDS, GROUP)]


def body(shape, dims, dens_hbm, span_hbm, sens_ref, viol_hbm, lam0_hbm, out_ref, lam_out,
         dens_ref, span_ref, viol_ref, lam0_ref, pad, xpad, ypack, yrecv, cpack, crecv, ymid,
         zpack, zrecv, xzpack, xzrecv, yzpack, yzrecv, czrecv, around, mid, invden, pp, qq, slope, scaled,
         acc, wide, lam, part, *rest):
    stages = plan(shape)
    recvs = rest[: len(stages)]
    load_sem, send_sem, recv_sem, zsend_sem, zrecv_sem, sum_send, sum_recv, known = rest[len(stages):]
    nx, ny, nz = dims
    tiles = ny // SUB
    chunks = nx * tiles
    slots = 2 * chunks
    load = pltpu.make_async_copy(
        sens_ref, pad.at[:, :, SUB : SUB + ny, :], load_sem.at[0]
    )
    load.start()
    small = [
        pltpu.make_async_copy(src, dst, load_sem.at[1 + i])
        for i, (src, dst) in enumerate([
            (span_hbm, span_ref), (dens_hbm, dens_ref), (viol_hbm, viol_ref), (lam0_hbm, lam0_ref)])
    ]
    for copy in small:
        copy.start()
    wide_x = 2 * tiles
    groups = steps()
    count_of = len(groups)
    me = {a: lax.axis_index(a) for a in AXES}

    has = {}
    for a in AXES:
        has[a, -1] = me[a] > 0
        has[a, 0] = jnp.bool_(True)
        has[a, 1] = me[a] < shape[a] - 1

    def both(o):
        moved = [has[a, d] for a, d in zip(AXES, o) if d]
        return functools.reduce(jnp.logical_and, moved)

    def at(**moves):
        return {a: me[a] + d for a, d in moves.items()}

    signs = (-1, 0, 1)
    plane = [(0, dy, dx) for dy in signs for dx in signs if dy or dx]
    ring = [(dz, dy, dx) for dz in signs for dy in signs for dx in signs if dz or dy or dx]
    barrier = pltpu.get_barrier_semaphore()
    near = shape["gz"] == 2 and shape["gy"] <= 4 and shape["gx"] <= 4
    if near:
        for o in ring:
            @pl.when(both(o))
            def _(o=o):
                pl.semaphore_signal(barrier, inc=1, device_id=at(gz=o[0], gy=o[1], gx=o[2]),
                                    device_id_type=MESH)
        arrivals = sum(both(o).astype(jnp.int32) for o in ring)
    else:
        partners = set()
        for axes in stages:
            for o in offsets(axes, shape):
                partners.add(tuple(dict(zip(axes, o)).get(a, 0) for a in AXES))
        for d in ring:
            o = tuple(d % shape[a] for a, d in zip(AXES, d))
            if any(o):
                partners.add(o)
        partners = sorted(partners)
        for o in partners:
            target = {a: lax.rem(me[a] + d, shape[a]) for a, d in zip(AXES, o)}
            pl.semaphore_signal(barrier, inc=1, device_id=target, device_id_type=MESH)
        arrivals = len(partners)

    lane = lax.broadcasted_iota(jnp.int32, (SUB, LANE), 1)
    row = lax.broadcasted_iota(jnp.int32, (SUB, LANE), 0)
    zero = jnp.zeros((SUB, LANE), jnp.float32)
    slot = lane % slots
    x_of = slot // wide_x
    t_of = (slot % wide_x) // 2
    odd = (lane % 2) == 1
    ends = jnp.logical_or(lane == 0, lane == LANE - 1)

    corners = [(sx, sy) for sx in (1, -1) for sy in (1, -1)]
    line = jnp.zeros((1, LANE), jnp.float32)
    for f in range(FIELDS):
        for x in range(nx):
            pad[f, x, SUB - 1 : SUB, :] = line
            pad[f, x, SUB + ny : SUB + ny + 1, :] = line
        for i in range(2):
            xpad[i, f, SUB - 1 : SUB, :] = line
            xpad[i, f, SUB + ny : SUB + ny + 1, :] = line
    for i, sx in enumerate((1, -1)):
        @pl.when(jnp.logical_not(has["gx", -sx]))
        def _(i=i):
            xpad[i, :, SUB : SUB + ny, :] = jnp.zeros((FIELDS, ny, LANE), jnp.float32)
    for i, sy in enumerate((1, -1)):
        @pl.when(jnp.logical_not(has["gy", -sy]))
        def _(i=i):
            yrecv[i] = jnp.zeros((FIELDS, nx, LANE), jnp.float32)
    for i, (sx, sy) in enumerate(corners):
        @pl.when(jnp.logical_not(jnp.logical_and(has["gx", -sx], has["gy", -sy])))
        def _(i=i):
            crecv[i] = jnp.zeros((FIELDS, 1, LANE), jnp.float32)
    for i, sz in enumerate((1, -1)):
        @pl.when(jnp.logical_not(has["gz", -sz]))
        def _(i=i):
            zrecv[i] = jnp.zeros(zrecv.shape[1:], jnp.float32)
        for n, sx in enumerate((1, -1)):
            @pl.when(jnp.logical_not(jnp.logical_and(has["gz", -sz], has["gx", -sx])))
            def _(i=i, n=n):
                xzrecv[i, n] = zero
        for n, sy in enumerate((1, -1)):
            @pl.when(jnp.logical_not(jnp.logical_and(has["gz", -sz], has["gy", -sy])))
            def _(i=i, n=n):
                yzrecv[i, n] = zero
        for n, (sx, sy) in enumerate(corners):
            @pl.when(jnp.logical_not(both((-sz, -sy, -sx))))
            def _(i=i, n=n):
                czrecv[i, n] = zero

    def count(a, index, extent):
        low = jnp.where(jnp.logical_and(me[a] == 0, index == 0), 0.0, 1.0)
        high = jnp.where(jnp.logical_and(me[a] == shape[a] - 1, index == extent - 1), 0.0, 1.0)
        return low + high
    cz = count("gz", lane, nz)
    for x in range(nx):
        cx = count("gx", jnp.full((SUB, LANE), x, jnp.int32), nx)
        for t in range(tiles):
            cy = count("gy", row + t * SUB, ny)
            den = W0 + W1 * (cx + cy + cz) + W2 * (cx * cy + cy * cz + cx * cz) + W3 * (cx * cy * cz)
            k = x * tiles + t
            invden[k] = 1.0 / den

    load.wait()

    def turned(value, shift, axis=1):
        shift %= value.shape[axis]
        return pltpu.roll(value, shift, axis) if shift else value

    def place(packed, value, k, j):
        here = lane // 2 == k + j * chunks
        return jnp.where(here, turned(value, 2 * k + 1 + j * slots), packed)

    edges = []
    for g, fields in enumerate(groups):
        packed = zero
        for j, f in enumerate(fields):
            for k in range(chunks):
                x, t = divmod(k, tiles)
                packed = place(packed, pad[f, x, SUB + t * SUB : 2 * SUB + t * SUB, :], k, j)
        zpack[g] = packed
        edges.append(packed)
    for n, x in enumerate((nx - 1, 0)):
        packed = zero
        for g in range(count_of):
            packed = jnp.where(x_of == g, turned(edges[g], (g - x) * wide_x), packed)
        xzpack[n] = packed
    for n, y in enumerate((SUB - 1, 0)):
        packed = zero
        for g in range(count_of):
            packed = jnp.where(row == g, jnp.broadcast_to(edges[g][y : y + 1, :], (SUB, LANE)), packed)
        yzpack[n] = packed
    for f in range(FIELDS):
        for i, y in enumerate((SUB + ny - 1, SUB)):
            for x in range(nx):
                ypack[i, f, x : x + 1, :] = pad[f, x, y : y + 1, :]
        for i, (sx, sy) in enumerate(corners):
            x = nx - 1 if sx > 0 else 0
            y = SUB + ny - 1 if sy > 0 else SUB
            cpack[i, f] = pad[f, x, y : y + 1, :]

    pl.semaphore_wait(barrier, arrivals)

    def remote(src, dst, sends, recvs_, index, **moves):
        copy = pltpu.make_async_remote_copy(
            src_ref=src, dst_ref=dst, send_sem=sends.at[index], recv_sem=recvs_.at[index],
            device_id=at(**moves), device_id_type=MESH)
        there = functools.reduce(jnp.logical_and, [has[a, d] for a, d in moves.items()])
        back = functools.reduce(jnp.logical_and, [has[a, -d] for a, d in moves.items()])
        return there, back, copy

    def moves_x(g):
        fields = pl.ds(groups[g][0], len(groups[g]))
        return [
            remote(pad.at[fields, nx - 1 if sx > 0 else 0, SUB : SUB + ny, :],
                   xpad.at[i, fields, SUB : SUB + ny, :], send_sem, recv_sem, 6 + 2 * g + i, gx=sx)
            for i, sx in enumerate((1, -1))
        ]

    moves_c = [remote(cpack.at[i], crecv.at[i], send_sem, recv_sem, 2 + i, gx=sx, gy=sy)
               for i, (sx, sy) in enumerate(corners)]
    moves_y = [remote(ypack.at[i], yrecv.at[i], send_sem, recv_sem, i, gy=sy)
               for i, sy in enumerate((1, -1))]
    moves_z = []
    for i, sz in enumerate((1, -1)):
        first = 0 if shape["gz"] == 2 else 9 * i
        for n, (sx, sy) in enumerate(corners):
            moves_z.append(remote(yzpack.at[n % 2], czrecv.at[i, n], zsend_sem, zrecv_sem, first + 5 + n,
                                  gz=sz, gx=sx, gy=sy))
        for n, sx in enumerate((1, -1)):
            moves_z.append(remote(xzpack.at[n], xzrecv.at[i, n], zsend_sem, zrecv_sem, first + 1 + n,
                                  gz=sz, gx=sx))
        for n, sy in enumerate((1, -1)):
            moves_z.append(remote(yzpack.at[n], yzrecv.at[i, n], zsend_sem, zrecv_sem, first + 3 + n,
                                  gz=sz, gy=sy))
        moves_z.append(remote(zpack, zrecv.at[i], zsend_sem, zrecv_sem, first, gz=sz))

    def start(moves):
        for send, _, copy in moves:
            pl.when(send)(copy.start)

    def receive(moves):
        for _, expected, copy in moves:
            pl.when(expected)(copy.wait_recv)

    friends = sum(both(o).astype(jnp.int32) for o in plane)

    def tell(n):
        for o in plane:
            @pl.when(both(o))
            def _(o=o):
                pl.semaphore_signal(known.at[n], inc=1, device_id=at(gy=o[1], gx=o[2]),
                                    device_id_type=MESH)

    xs = [moves_x(g) for g in range(count_of)]
    start(moves_z)
    start(moves_c)
    start(xs[0])
    start(moves_y)
    for g in range(1, count_of):
        start(xs[g])
    if near:
        tell(0)

    def along(s0, s1):
        up = jnp.where(lane == 0, 0.0, pltpu.roll(s1, 1, 1))
        down = jnp.where(lane == LANE - 1, 0.0, pltpu.roll(s1, LANE - 1, 1))
        return s0 + up + down

    for f in range(FIELDS):
        for t in range(tiles):
            y = SUB + t * SUB
            mids, sides = [None], [None]
            for x in range(nx):
                mids.append(pad[f, x, y : y + SUB, :])
                sides.append(pad[f, x, y - 1 : y - 1 + SUB, :] + pad[f, x, y + 1 : y + 1 + SUB, :])
            mids.append(None)
            sides.append(None)
            for x in range(nx):
                next_to = [v for v in (mids[x], mids[x + 2]) if v is not None]
                beyond = [v for v in (sides[x], sides[x + 2]) if v is not None]
                close = sides[x + 1] + sum(next_to[1:], next_to[0])
                far = sum(beyond[1:], beyond[0])
                s0 = W0 * mids[x + 1] + W1 * close + W2 * far
                s1 = W1 * mids[x + 1] + W2 * close + W3 * far
                mid[f, x * tiles + t] = along(s0, s1)

    def piece(ref, k):
        x, t = divmod(k, tiles)
        return ref[x, t * SUB : (t + 1) * SUB, :]

    for copy in small:
        copy.wait()
    for n, ref in enumerate((span_ref, dens_ref, invden)):
        packed = zero
        for k in range(chunks):
            value = ref[k] if n == 2 else piece(ref, k)
            for j in range(LANE // slots):
                packed = place(packed, value, k, j)
        around[n, 0] = packed
        for i, y in enumerate((0, ny - 1)):
            for x in range(nx):
                k = x * tiles + y // SUB
                around[n, 1 + i, x : x + 1, :] = (
                    ref[k, y % SUB : y % SUB + 1, :] if n == 2 else ref[x, y : y + 1, :])
    for k in range(FIELDS):
        lam[k] = jnp.full((SUB, LANE), lam0_ref[k], jnp.float32)
    total = zero
    for k in range(chunks):
        s = piece(span_ref, k)
        square = s * s
        pp[FIELDS, k] = square * (1.001 + RAA)
        qq[FIELDS, k] = square * (0.001 + RAA)
        total += s * (1.002 + 2 * RAA)
    acc[ROWS - 1] = total
    weights = [lam[j] for j in range(FIELDS)]

    inside = jnp.logical_not(ends)

    def keep_of(k):
        keep = inside
        if k % tiles == 0:
            keep = jnp.logical_and(keep, row != 0)
        if k % tiles == tiles - 1:
            keep = jnp.logical_and(keep, row != SUB - 1)
        return keep

    def grown(r, s):
        gp = jnp.maximum(r, 0.0)
        gm = jnp.maximum(-r, 0.0)
        square = s * s
        p = square * (1.001 * gp + 0.001 * gm + RAA)
        q = square * (0.001 * gp + 1.001 * gm + RAA)
        return p, q, s * (1.002 * (gp + gm) + 2 * RAA)

    def rows(f, j, packed, ks):
        total = zero
        for k in ks:
            x, t = divmod(k, tiles)
            value = mid[f, k]
            for i in range(2):
                if x == (0, nx - 1)[i]:
                    y = SUB + t * SUB
                    h = xpad[i, f, y : y + SUB, :]
                    pair = xpad[i, f, y - 1 : y - 1 + SUB, :] + xpad[i, f, y + 1 : y + 1 + SUB, :]
                    value += along(W1 * h + W2 * pair, W2 * h + W3 * pair)
            for i, y in enumerate((0, ny - 1)):
                if t == y // SUB:
                    ymid[i, f, x : x + 1, :] = value[y % SUB : y % SUB + 1, :]
            packed = place(packed, value, k, j)
            s = piece(span_ref, k)
            pp[f, k], qq[f, k], base = grown(value * invden[k], s)
            total += jnp.where(keep_of(k), base, 0.0)
        if f:
            acc[SUMS - 1 + f] = total + (zero if ks is core else acc[SUMS - 1 + f])
        return packed

    def respond(k, weights):
        big_p, big_q = pp[0, k], qq[0, k]
        for j in range(FIELDS):
            big_p += weights[j] * pp[j + 1, k]
            big_q += weights[j] * qq[j + 1, k]
        s = piece(span_ref, k) if k < chunks else around[0, k - chunks]
        d = piece(dens_ref, k) if k < chunks else around[1, k - chunks]
        root_p = jnp.sqrt(big_p)
        root_q = jnp.sqrt(big_q)
        lower, upper = d - s, d + s
        moved = (root_p * lower + root_q * upper) / (root_p + root_q)
        low = jnp.maximum(0.0, d - MOVE * s)
        high = jnp.minimum(1.0, d + MOVE * s)
        return jnp.minimum(jnp.maximum(moved, low), high), big_p, big_q, lower, upper

    def terms(k, weights, keep=None):
        moved, big_p, big_q, lower, upper = respond(k, weights)
        ia = 1.0 / (upper - moved)
        ib = 1.0 / (moved - lower)
        ia2, ib2 = ia * ia, ib * ib
        inv = 1.0 / (2.0 * big_p * (ia2 * ia) + 2.0 * big_q * (ib2 * ib))
        if keep is not None:
            ia, ib, ia2, ib2 = [jnp.where(keep, v, 0.0) for v in (ia, ib, ia2, ib2)]
        grads, slopes, ratios = [], [], []
        for j in range(FIELDS):
            p, q = pp[j + 1, k], qq[j + 1, k]
            grads.append(p * ia + q * ib)
            a = p * ia2 - q * ib2
            slopes.append(a)
            ratios.append(a * inv)
        return grads, slopes, ratios

    def main_sums(weights, ks, masked, more):
        grads = [acc[j] if more else zero for j in range(FIELDS)]
        for k in ks:
            extra, slopes, ratios = terms(k, weights, keep_of(k) if masked else None)
            for j in range(FIELDS):
                grads[j] += extra[j]
                slope[j, k] = slopes[j]
                scaled[j, k] = ratios[j]
        for j in range(FIELDS):
            acc[j] = grads[j]
        at_row = FIELDS
        for group in ((0, 1), (2, 3), (4, 5, 6, 7, 8)):
            keys = [(i, j) for i in group for j in range(i, FIELDS)]
            sums = {key: acc[at_row + n] if more else zero for n, key in enumerate(keys)}
            for k in ks:
                right = {j: slope[j, k] for j in range(group[0], FIELDS)}
                for i in group:
                    left = scaled[i, k]
                    for j in range(i, FIELDS):
                        sums[i, j] += left * right[j]
            for key in keys:
                acc[at_row] = sums[key]
                at_row += 1

    def combined(ref, *index):
        return jnp.where(odd, pltpu.roll(ref[(0,) + index], 1, 1), pltpu.roll(ref[(1,) + index], LANE - 1, 1))

    def outer_edges():
        last_x, last_t = wide_x * (nx - 1), 2 * (tiles - 1)
        yz = [combined(yzrecv, n) for n in range(2)]
        xz = [combined(xzrecv, n) for n in range(2)]
        cz_ = [combined(czrecv, n) for n in range(4)]

        def pick(value, g, shift):
            return turned(jnp.broadcast_to(value[g : g + 1, :], (SUB, LANE)), shift)

        def beside(c, first, final):
            down = pltpu.roll(c, 1, 0)
            up = pltpu.roll(c, SUB - 1, 0)
            before = jnp.where(row == 0, jnp.where(t_of == 0, first, turned(down, 2)), down)
            after = jnp.where(row == SUB - 1, jnp.where(t_of == tiles - 1, final, turned(up, LANE - 2)), up)
            return before + after

        out = []
        for g in range(count_of):
            c = combined(zrecv, g)
            s = beside(c, pick(yz[0], g, -last_t), pick(yz[1], g, last_t))
            c_low = turned(xz[0], -wide_x * g)
            c_high = turned(xz[1], last_x - wide_x * g)
            s_low = beside(c_low, pick(cz_[0], g, -last_x - last_t), pick(cz_[1], g, -last_x + last_t))
            s_high = beside(c_high, pick(cz_[2], g, last_x - last_t), pick(cz_[3], g, last_x + last_t))

            def pair(own, low, high):
                return (jnp.where(x_of == 0, low, turned(own, wide_x))
                        + jnp.where(x_of == nx - 1, high, turned(own, -wide_x)))
            out.append(W1 * c + W2 * (s + pair(c, c_low, c_high)) + W3 * pair(s, s_low, s_high))
        return out

    def face_rows():
        drops = [[zero, zero] for _ in groups]
        bases = []
        for g, fields in enumerate(groups):
            for j, f in enumerate(fields):
                base = zero
                for i in range(2):
                    h = yrecv[i, f]
                    low = jnp.broadcast_to(crecv[i, f], (SUB, LANE))
                    high = jnp.broadcast_to(crecv[2 + i, f], (SUB, LANE))
                    pair = (jnp.where(row == 0, low, pltpu.roll(h, 1, 0))
                            + jnp.where(row == nx - 1, high, pltpu.roll(h, nx - 1, 0)))
                    extra = along(W1 * h + W2 * pair, W2 * h + W3 * pair)
                    s = around[0, 1 + i]
                    p, q, more = grown((ymid[i, f] + extra) * around[2, 1 + i], s)
                    pp[f, chunks + 1 + i] = p
                    qq[f, chunks + 1 + i] = q
                    base += jnp.where(inside, more, 0.0)
                    here = jnp.logical_and(row == x_of, lane // slots == j)
                    side = jnp.where(odd, jnp.broadcast_to(extra[:, :1], (SUB, LANE)),
                                     jnp.broadcast_to(extra[:, LANE - 1 :], (SUB, LANE)))
                    drops[g][i] = jnp.where(here, side, drops[g][i])
                bases.append(base)
        for i in range(2):
            s = around[0, 1 + i]
            pp[FIELDS, chunks + 1 + i] = s * s * (1.001 + RAA)
            qq[FIELDS, chunks + 1 + i] = s * s * (0.001 + RAA)
        extras = []
        for g in range(count_of):
            value = zero
            for i, y in enumerate((0, ny - 1)):
                full = jnp.broadcast_to(jnp.sum(drops[g][i], axis=0, keepdims=True), (SUB, LANE))
                here = jnp.logical_and(row == y % SUB, t_of == y // SUB)
                value += jnp.where(here, full, 0.0)
            extras.append(value)
        return extras, bases[1:]

    def edge_rows(extras):
        outer = outer_edges()
        s = around[0, 0]
        bases = []
        for g, fields in enumerate(groups):
            p, q, base = grown((inner[g] + extras[g] + outer[g]) * around[2, 0], s)
            for j, f in enumerate(fields):
                pp[f, chunks] = turned(p, -j * slots)
                qq[f, chunks] = turned(q, -j * slots)
                bases.append(turned(base, -j * slots))
        pp[FIELDS, chunks] = s * s * (1.001 + RAA)
        qq[FIELDS, chunks] = s * s * (0.001 + RAA)
        return bases[1:]

    def extra_sums(weights, ks, keep, bases):
        pieces = [terms(k, weights, keep) for k in ks]
        grads = [sum((p[0][j] for p in pieces[1:]), pieces[0][0][j]) for j in range(FIELDS)]
        squares = [sum((p[2][i] * p[1][j] for p in pieces[1:]), pieces[0][2][i] * pieces[0][1][j])
                   for i in range(FIELDS) for j in range(i, FIELDS)]
        for r, value in enumerate(grads + squares + list(bases)):
            acc[r] += value

    def repair():
        for f in range(FIELDS):
            for ref in (pp, qq):
                edge = ref[f, chunks]
                for k in range(chunks):
                    x, t = divmod(k, tiles)
                    value = ref[f, k]
                    for i, y in enumerate((0, ny - 1)):
                        if t == y // SUB:
                            line = jnp.broadcast_to(ref[f, chunks + 1 + i, x : x + 1, :], (SUB, LANE))
                            value = jnp.where(row == y % SUB, line, value)
                    ref[f, k] = jnp.where(ends, turned(edge, -2 * k - 1), value)

    def flat(axes):
        index = 0
        for a in axes:
            index = index * shape[a] + me[a]
        return index

    def exchange(it, meanwhile):
        packed = zero
        for r in range(ROWS):
            packed = jnp.where(lane == r, jnp.sum(acc[r], axis=1, keepdims=True), packed)
        value = jnp.sum(packed, axis=0, keepdims=True)
        for n, axes in enumerate(stages):
            size = math.prod(shape[a] for a in axes)
            part[it, n] = value
            recvs[n][it, flat(axes)] = value
            for o in sorted(offsets(axes, shape), key=lambda o: (-abs(o[-1] - 2), o), reverse=True):
                target = {a: lax.rem(me[a] + d, shape[a]) for a, d in zip(axes, o)}
                pltpu.make_async_remote_copy(
                    src_ref=part.at[it, n], dst_ref=recvs[n].at[it, flat(axes)],
                    send_sem=sum_send.at[it, n], recv_sem=sum_recv.at[it, n],
                    device_id=target, device_id_type=MESH).start()
            if n == 0:
                meanwhile()
            whole = recvs[n].at[it, pl.ds(0, size - 1)]
            pltpu.make_async_copy(whole, whole, sum_recv.at[it, n]).wait()
            values = [recvs[n][it, i] for i in range(size)]
            while len(values) > 1:
                values = [sum(values[i + 1 : i + 2], values[i]) for i in range(0, len(values), 2)]
            value = values[0]
        every = jnp.broadcast_to(value, (SUB, LANE))
        for g in range(wide.shape[0]):
            one = jnp.sum(jnp.where(lane == g * SUB + row, every, 0.0), axis=1, keepdims=True)
            wide[g] = jnp.broadcast_to(one, (SUB, LANE))

    def solve(weights):
        def read(r):
            return jnp.broadcast_to(wide[r // SUB, r % SUB : r % SUB + 1, :], (SUB, LANE))
        b = [read(j) - (1.0 - viol_ref[j]) * read(SUMS + j) for j in range(FIELDS)]
        m = {}
        at_row = FIELDS
        for i in range(FIELDS):
            for j in range(i, FIELDS):
                m[i, j] = read(at_row)
                at_row += 1
        trace = m[0, 0]
        for i in range(1, FIELDS):
            trace += m[i, i]
        shift = REG * trace / FIELDS
        for i in range(FIELDS):
            m[i, i] += shift
        inverse = []
        for k in range(FIELDS):
            inverse.append(1.0 / m[k, k])
            for i in range(k + 1, FIELDS):
                factor = m[k, i] * inverse[k]
                for j in range(i, FIELDS):
                    m[i, j] -= factor * m[k, j]
                b[i] -= factor * b[k]
        delta = [None] * FIELDS
        for k in reversed(range(FIELDS)):
            v = b[k]
            for j in range(k + 1, FIELDS):
                v -= m[k, j] * delta[j]
            delta[k] = v * inverse[k]
        for k in range(FIELDS):
            lam[k] = jnp.maximum(weights[k] + delta[k], FLOOR * weights[k])

    def newton(it, carry):
        weights = [lam[j] for j in range(FIELDS)]
        main_sums(weights, range(chunks), False, False)
        exchange(it, lambda: None)
        solve(weights)
        return carry

    core = range(tiles, chunks - tiles)
    faces = [k for k in range(chunks) if k not in core]
    inner = []
    for g, fields in enumerate(groups):
        packed = zero
        for j, f in enumerate(fields):
            packed = rows(f, j, packed, core)
        inner.append(packed)
    main_sums(weights, core, True, False)
    if near:
        pl.semaphore_wait(known.at[0], friends)
        tell(1)
    receive(moves_y)
    for g, fields in enumerate(groups):
        receive(xs[g])
        for j, f in enumerate(fields):
            inner[g] = rows(f, j, inner[g], faces)
    main_sums(weights, faces, True, True)
    receive(moves_c)
    extras, bases = face_rows()
    extra_sums(weights, (chunks + 1, chunks + 2), inside, bases)
    receive(moves_z)
    within = lane < slots
    bases = [jnp.where(within, v, 0.0) for v in edge_rows(extras)]
    extra_sums(weights, (chunks,), within, bases)
    if near:
        pl.semaphore_wait(known.at[1], friends)
    exchange(0, repair)
    solve(weights)
    lax.fori_loop(1, ITERS, newton, 0)

    weights = [lam[j] for j in range(FIELDS)]
    for k in range(chunks):
        x, t = divmod(k, tiles)
        out_ref[x, t * SUB : (t + 1) * SUB, :] = respond(k, weights)[0]
    final = zero
    for j in range(FIELDS):
        final = jnp.where(lane == j, weights[j], final)
    lam_out[...] = final

    for moves in [moves_c, moves_y] + xs + [moves_z]:
        for send, _, copy in moves:
            pl.when(send)(copy.wait_send)
    for it in range(ITERS):
        for n, axes in enumerate(stages):
            size = math.prod(shape[a] for a in axes)
            whole = recvs[n].at[it, pl.ds(0, size - 1)]
            pltpu.make_async_copy(whole, whole, sum_send.at[it, n]).wait()


def finish(field_ref, lam_ref, field_out, lam_out, row, sem):
    whole = pltpu.make_async_copy(field_ref, field_out, sem.at[0])
    whole.start()
    row[...] = lam_ref[0, :FIELDS]
    short = pltpu.make_async_copy(row, lam_out, sem.at[1])
    short.start()
    whole.wait()
    short.wait()


def shards(shape, density, spread, sensitivities, violation, multipliers_start):
    nx, ny, nz = density.shape
    chunks = nx * ny // SUB
    groups = len(steps())
    stages = plan(shape)
    corners = 9 if shape["gz"] == 2 else 18
    f32 = jnp.float32
    vmem = pl.BlockSpec(memory_space=pltpu.VMEM)
    dma = pltpu.SemaphoreType.DMA
    hbm = pl.BlockSpec(memory_space=pltpu.HBM)
    field, lam = pl.pallas_call(
        functools.partial(body, shape, (nx, ny, nz)),
        out_shape=(
            pltpu.VMEM((nx, ny, nz), f32),
            pltpu.VMEM((SUB, LANE), f32),
        ),
        in_specs=[hbm] * 5,
        out_specs=(vmem, vmem),
        scratch_shapes=[
            pltpu.VMEM((nx, ny, nz), f32),
            pltpu.VMEM((nx, ny, nz), f32),
            pltpu.SMEM((FIELDS,), f32),
            pltpu.SMEM((FIELDS,), f32),
            pltpu.VMEM((FIELDS, nx, ny + 2 * SUB, nz), f32),
            pltpu.VMEM((2, FIELDS, ny + 2 * SUB, nz), f32),
            pltpu.VMEM((2, FIELDS, nx, nz), f32),
            pltpu.VMEM((2, FIELDS, nx, nz), f32),
            pltpu.VMEM((4, FIELDS, 1, nz), f32),
            pltpu.VMEM((4, FIELDS, 1, nz), f32),
            pltpu.VMEM((2, FIELDS, nx, nz), f32),
            pltpu.VMEM((groups, SUB, LANE), f32),
            pltpu.VMEM((2, groups, SUB, LANE), f32),
            pltpu.VMEM((2, SUB, LANE), f32),
            pltpu.VMEM((2, 2, SUB, LANE), f32),
            pltpu.VMEM((2, SUB, LANE), f32),
            pltpu.VMEM((2, 2, SUB, LANE), f32),
            pltpu.VMEM((2, 4, SUB, LANE), f32),
            pltpu.VMEM((3, 3, SUB, LANE), f32),
            pltpu.VMEM((FIELDS, chunks, SUB, LANE), f32),
            pltpu.VMEM((chunks, SUB, LANE), f32),
            pltpu.VMEM((FIELDS + 1, chunks + 3, SUB, LANE), f32),
            pltpu.VMEM((FIELDS + 1, chunks + 3, SUB, LANE), f32),
            pltpu.VMEM((FIELDS, chunks, SUB, LANE), f32),
            pltpu.VMEM((FIELDS, chunks, SUB, LANE), f32),
            pltpu.VMEM((ROWS, SUB, LANE), f32),
            pltpu.VMEM((-(-ROWS // SUB), SUB, LANE), f32),
            pltpu.VMEM((FIELDS, SUB, LANE), f32),
            pltpu.VMEM((ITERS, len(stages), 1, LANE), f32),
        ] + [
            pltpu.VMEM((ITERS, math.prod(shape[a] for a in axes), 1, LANE), f32) for axes in stages
        ] + [
            dma((5,)), dma((6 + 2 * groups,)), dma((6 + 2 * groups,)), dma((corners,)), dma((corners,)),
            dma((ITERS, len(stages))), dma((ITERS, len(stages))), pltpu.SemaphoreType.REGULAR((2,)),
        ],
        compiler_params=pltpu.CompilerParams(
            collective_id=0, has_side_effects=True, vmem_limit_bytes=24 << 20),
        name="design_step",
    )(*[pltpu.with_memory_space_constraint(v, pltpu.HBM) for v in (density, spread, sensitivities, violation, multipliers_start)])
    return pl.pallas_call(
        finish,
        out_shape=(
            jax.ShapeDtypeStruct((nx, ny, nz), f32),
            jax.ShapeDtypeStruct((FIELDS,), f32),
        ),
        in_specs=[vmem, vmem],
        out_specs=(hbm, hbm),
        scratch_shapes=[pltpu.VMEM((FIELDS,), f32), dma((2,))],
        compiler_params=pltpu.CompilerParams(vmem_limit_bytes=1 << 20),
        name="finish",
    )(field, lam)


def solution(mesh):
    shape = {a: int(mesh.shape[a]) for a in AXES}
    return jax.shard_map(
        functools.partial(shards, shape),
        mesh=mesh,
        in_specs=(P("gx", "gy", "gz"), P("gx", "gy", "gz"), P(None, "gx", "gy", "gz"), P(), P()),
        out_specs=(P("gx", "gy", "gz"), P()),
        check_vma=False,
    )
```

```python
import functools
import math

import jax
import jax.numpy as jnp
from jax import lax
from jax.experimental import pallas as pl
from jax.experimental.pallas import tpu as pltpu
from jax.sharding import PartitionSpec as P

FIELDS = 9
ITERS = 3

RADIUS = 3.0
RAA = 1e-05
MOVE = 0.9
REG = 0.001
FLOOR = 0.2

W0 = RADIUS
W1 = RADIUS - 1.0
W2 = RADIUS - math.sqrt(2.0)
W3 = RADIUS - math.sqrt(3.0)

SUB, LANE = 8, 128
AXES = ("gz", "gy", "gx")
SUMS = FIELDS + FIELDS * (FIELDS + 1) // 2
ROWS = SUMS + FIELDS
MESH = pl.DeviceIdType.MESH
GROUP = 3


def plan(shape):
    total = math.prod(shape[a] for a in AXES)
    if total <= 32:
        return (AXES,)
    return tuple((a,) for a in AXES)


def offsets(axes, shape):
    out = [()]
    for a in axes:
        out = [o + (d,) for o in out for d in range(shape[a])]
    return [o for o in out if any(o)]


def steps():
    return [range(f, min(f + GROUP, FIELDS)) for f in range(0, FIELDS, GROUP)]


def body(shape, dims, dens_hbm, span_hbm, sens_ref, viol_hbm, lam0_hbm, out_ref, lam_out,
         dens_ref, span_ref, viol_ref, lam0_ref, pad, xpad, ypack, yrecv, cpack, crecv, ymid,
         zpack, zrecv, xzpack, xzrecv, yzpack, yzrecv, czrecv, around, mid, invden, pp, qq, slope, scaled,
         acc, wide, lam, part, *rest):
    stages = plan(shape)
    recvs = rest[: len(stages)]
    load_sem, send_sem, recv_sem, zsend_sem, zrecv_sem, sum_send, sum_recv, known = rest[len(stages):]
    nx, ny, nz = dims
    tiles = ny // SUB
    chunks = nx * tiles
    slots = 2 * chunks
    load = pltpu.make_async_copy(
        sens_ref, pad.at[:, :, SUB : SUB + ny, :], load_sem.at[0]
    )
    load.start()
    small = [
        pltpu.make_async_copy(src, dst, load_sem.at[1 + i])
        for i, (src, dst) in enumerate([
            (span_hbm, span_ref), (dens_hbm, dens_ref), (viol_hbm, viol_ref), (lam0_hbm, lam0_ref)])
    ]
    for copy in small:
        copy.start()
    wide_x = 2 * tiles
    groups = steps()
    count_of = len(groups)
    me = {a: lax.axis_index(a) for a in AXES}

    has = {}
    for a in AXES:
        has[a, -1] = me[a] > 0
        has[a, 0] = jnp.bool_(True)
        has[a, 1] = me[a] < shape[a] - 1

    def both(o):
        moved = [has[a, d] for a, d in zip(AXES, o) if d and not (single and a == "gz")]
        return functools.reduce(jnp.logical_and, moved, jnp.bool_(True))

    single = shape["gz"] == 2
    if single:
        has["gz", 1] = jnp.bool_(True)

    def at(**moves):
        out = {a: me[a] + d for a, d in moves.items()}
        if single and moves.get("gz"):
            out["gz"] = 1 - me["gz"]
        return out

    signs = (-1, 0, 1)
    plane = [(0, dy, dx) for dy in signs for dx in signs if dy or dx]
    ring = [(dz, dy, dx) for dz in ((1, 0) if single else signs) for dy in signs for dx in signs if dz or dy or dx]
    ring.sort(key=lambda o: (-sum(map(abs, o)), o))
    if single:
        has["gz", -1] = has["gz", 1]
    sides = ((0, 1),) if single else ((0, 1), (1, -1))
    barrier = pltpu.get_barrier_semaphore()
    near = shape["gz"] == 2 and shape["gy"] <= 4 and shape["gx"] <= 4
    if near:
        for o in ring:
            @pl.when(both(o))
            def _(o=o):
                pl.semaphore_signal(barrier, inc=1, device_id=at(gz=o[0], gy=o[1], gx=o[2]),
                                    device_id_type=MESH)
        arrivals = sum(both(o).astype(jnp.int32) for o in ring)
    else:
        partners = set()
        for axes in stages:
            for o in offsets(axes, shape):
                partners.add(tuple(dict(zip(axes, o)).get(a, 0) for a in AXES))
        for d in ring:
            o = tuple(d % shape[a] for a, d in zip(AXES, d))
            if any(o):
                partners.add(o)
        partners = sorted(partners)
        for o in partners:
            target = {a: lax.rem(me[a] + d, shape[a]) for a, d in zip(AXES, o)}
            pl.semaphore_signal(barrier, inc=1, device_id=target, device_id_type=MESH)
        arrivals = len(partners)

    lane = lax.broadcasted_iota(jnp.int32, (SUB, LANE), 1)
    row = lax.broadcasted_iota(jnp.int32, (SUB, LANE), 0)
    zero = jnp.zeros((SUB, LANE), jnp.float32)
    slot = lane % slots
    x_of = slot // wide_x
    t_of = (slot % wide_x) // 2
    odd = (lane % 2) == 1
    ends = jnp.logical_or(lane == 0, lane == LANE - 1)

    corners = [(sx, sy) for sx in (1, -1) for sy in (1, -1)]
    line = jnp.zeros((1, LANE), jnp.float32)
    for f in range(FIELDS):
        for x in range(nx):
            pad[f, x, SUB - 1 : SUB, :] = line
            pad[f, x, SUB + ny : SUB + ny + 1, :] = line
        for i in range(2):
            xpad[i, f, SUB - 1 : SUB, :] = line
            xpad[i, f, SUB + ny : SUB + ny + 1, :] = line
    for i, sx in enumerate((1, -1)):
        @pl.when(jnp.logical_not(has["gx", -sx]))
        def _(i=i):
            xpad[i, :, SUB : SUB + ny, :] = jnp.zeros((FIELDS, ny, LANE), jnp.float32)
    for i, sy in enumerate((1, -1)):
        @pl.when(jnp.logical_not(has["gy", -sy]))
        def _(i=i):
            yrecv[i] = jnp.zeros((FIELDS, nx, LANE), jnp.float32)
    for i, (sx, sy) in enumerate(corners):
        @pl.when(jnp.logical_not(jnp.logical_and(has["gx", -sx], has["gy", -sy])))
        def _(i=i):
            crecv[i] = jnp.zeros((FIELDS, 1, LANE), jnp.float32)
    for i, sz in sides:
        if not single:
            @pl.when(jnp.logical_not(has["gz", -sz]))
            def _(i=i):
                zrecv[i] = jnp.zeros(zrecv.shape[1:], jnp.float32)
        for n, sx in enumerate((1, -1)):
            @pl.when(jnp.logical_not(both((-sz, 0, -sx))))
            def _(i=i, n=n):
                xzrecv[i, n] = zero
        for n, sy in enumerate((1, -1)):
            @pl.when(jnp.logical_not(both((-sz, -sy, 0))))
            def _(i=i, n=n):
                yzrecv[i, n] = zero
        for n, (sx, sy) in enumerate(corners):
            @pl.when(jnp.logical_not(both((-sz, -sy, -sx))))
            def _(i=i, n=n):
                czrecv[i, n] = zero

    def count(a, index, extent):
        low = jnp.where(jnp.logical_and(me[a] == 0, index == 0), 0.0, 1.0)
        high = jnp.where(jnp.logical_and(me[a] == shape[a] - 1, index == extent - 1), 0.0, 1.0)
        return low + high
    cz = count("gz", lane, nz)
    for x in range(nx):
        cx = count("gx", jnp.full((SUB, LANE), x, jnp.int32), nx)
        for t in range(tiles):
            cy = count("gy", row + t * SUB, ny)
            den = W0 + W1 * (cx + cy + cz) + W2 * (cx * cy + cy * cz + cx * cz) + W3 * (cx * cy * cz)
            k = x * tiles + t
            invden[k] = 1.0 / den

    load.wait()

    def turned(value, shift, axis=1):
        shift %= value.shape[axis]
        return pltpu.roll(value, shift, axis) if shift else value

    def place(packed, value, k, j):
        here = lane // 2 == k + j * chunks
        return jnp.where(here, turned(value, 2 * k + 1 + j * slots), packed)

    edges = []
    for g, fields in enumerate(groups):
        packed = zero
        for j, f in enumerate(fields):
            for k in range(chunks):
                x, t = divmod(k, tiles)
                packed = place(packed, pad[f, x, SUB + t * SUB : 2 * SUB + t * SUB, :], k, j)
        zpack[g] = packed
        edges.append(packed)
    for n, x in enumerate((nx - 1, 0)):
        packed = zero
        for g in range(count_of):
            packed = jnp.where(x_of == g, turned(edges[g], (g - x) * wide_x), packed)
        xzpack[n] = packed
    for n, y in enumerate((SUB - 1, 0)):
        packed = zero
        for g in range(count_of):
            packed = jnp.where(row == g, jnp.broadcast_to(edges[g][y : y + 1, :], (SUB, LANE)), packed)
        yzpack[n] = packed
    for f in range(FIELDS):
        for i, y in enumerate((SUB + ny - 1, SUB)):
            for x in range(nx):
                ypack[i, f, x : x + 1, :] = pad[f, x, y : y + 1, :]
        for i, (sx, sy) in enumerate(corners):
            x = nx - 1 if sx > 0 else 0
            y = SUB + ny - 1 if sy > 0 else SUB
            cpack[i, f] = pad[f, x, y : y + 1, :]

    pl.semaphore_wait(barrier, arrivals)

    def remote(src, dst, sends, recvs_, index, **moves):
        copy = pltpu.make_async_remote_copy(
            src_ref=src, dst_ref=dst, send_sem=sends.at[index], recv_sem=recvs_.at[index],
            device_id=at(**moves), device_id_type=MESH)
        there = both([moves.get(a, 0) for a in AXES])
        back = both([-moves.get(a, 0) for a in AXES])
        return there, back, copy

    def moves_x(g):
        fields = pl.ds(groups[g][0], len(groups[g]))
        return [
            remote(pad.at[fields, nx - 1 if sx > 0 else 0, SUB : SUB + ny, :],
                   xpad.at[i, fields, SUB : SUB + ny, :], send_sem, recv_sem, 6 + 2 * g + i, gx=sx)
            for i, sx in enumerate((1, -1))
        ]

    moves_c = [remote(cpack.at[i], crecv.at[i], send_sem, recv_sem, 2 + i, gx=sx, gy=sy)
               for i, (sx, sy) in enumerate(corners)]
    moves_y = [remote(ypack.at[i], yrecv.at[i], send_sem, recv_sem, i, gy=sy)
               for i, sy in enumerate((1, -1))]
    moves_z = []
    for i, sz in sides:
        first = 9 * i
        for n, (sx, sy) in enumerate(corners):
            moves_z.append(remote(yzpack.at[n % 2], czrecv.at[i, n], zsend_sem, zrecv_sem, first + 5 + n,
                                  gz=sz, gx=sx, gy=sy))
        for n, sx in enumerate((1, -1)):
            moves_z.append(remote(xzpack.at[n], xzrecv.at[i, n], zsend_sem, zrecv_sem, first + 1 + n,
                                  gz=sz, gx=sx))
        for n, sy in enumerate((1, -1)):
            moves_z.append(remote(yzpack.at[n], yzrecv.at[i, n], zsend_sem, zrecv_sem, first + 3 + n,
                                  gz=sz, gy=sy))
        moves_z.append(remote(zpack, zrecv.at[i], zsend_sem, zrecv_sem, first, gz=sz))

    def start(moves):
        for send, _, copy in moves:
            pl.when(send)(copy.start)

    def receive(moves):
        for _, expected, copy in moves:
            pl.when(expected)(copy.wait_recv)

    friends = sum(both(o).astype(jnp.int32) for o in plane)

    def tell(n):
        for o in plane:
            @pl.when(both(o))
            def _(o=o):
                pl.semaphore_signal(known.at[n], inc=1, device_id=at(gy=o[1], gx=o[2]),
                                    device_id_type=MESH)

    xs = [moves_x(g) for g in range(count_of)]
    start(moves_z)
    start(moves_c)
    start(xs[0])
    start(moves_y)
    for g in range(1, count_of):
        start(xs[g])
    if near:
        tell(0)

    def along(s0, s1):
        up = jnp.where(lane == 0, 0.0, pltpu.roll(s1, 1, 1))
        down = jnp.where(lane == LANE - 1, 0.0, pltpu.roll(s1, LANE - 1, 1))
        return s0 + up + down

    for f in range(FIELDS):
        for t in range(tiles):
            y = SUB + t * SUB
            mids, sides = [None], [None]
            for x in range(nx):
                mids.append(pad[f, x, y : y + SUB, :])
                sides.append(pad[f, x, y - 1 : y - 1 + SUB, :] + pad[f, x, y + 1 : y + 1 + SUB, :])
            mids.append(None)
            sides.append(None)
            for x in range(nx):
                next_to = [v for v in (mids[x], mids[x + 2]) if v is not None]
                beyond = [v for v in (sides[x], sides[x + 2]) if v is not None]
                close = sides[x + 1] + sum(next_to[1:], next_to[0])
                far = sum(beyond[1:], beyond[0])
                s0 = W0 * mids[x + 1] + W1 * close + W2 * far
                s1 = W1 * mids[x + 1] + W2 * close + W3 * far
                mid[f, x * tiles + t] = along(s0, s1)

    def piece(ref, k):
        x, t = divmod(k, tiles)
        return ref[x, t * SUB : (t + 1) * SUB, :]

    for copy in small:
        copy.wait()
    for n, ref in enumerate((span_ref, dens_ref, invden)):
        packed = zero
        for k in range(chunks):
            value = ref[k] if n == 2 else piece(ref, k)
            for j in range(LANE // slots):
                packed = place(packed, value, k, j)
        around[n, 0] = packed
        for i, y in enumerate((0, ny - 1)):
            for x in range(nx):
                k = x * tiles + y // SUB
                around[n, 1 + i, x : x + 1, :] = (
                    ref[k, y % SUB : y % SUB + 1, :] if n == 2 else ref[x, y : y + 1, :])
    for k in range(FIELDS):
        lam[k] = jnp.full((SUB, LANE), lam0_ref[k], jnp.float32)
    total = zero
    for k in range(chunks):
        s = piece(span_ref, k)
        square = s * s
        pp[FIELDS, k] = square * (1.001 + RAA)
        qq[FIELDS, k] = square * (0.001 + RAA)
        total += s * (1.002 + 2 * RAA)
    acc[ROWS - 1] = total
    weights = [lam[j] for j in range(FIELDS)]

    inside = jnp.logical_not(ends)
    core = range(tiles, chunks - tiles)
    faces = [k for k in range(chunks) if k not in core]

    def keep_of(k):
        keep = inside
        if k in faces:
            return keep
        if k % tiles == 0:
            keep = jnp.logical_and(keep, row != 0)
        if k % tiles == tiles - 1:
            keep = jnp.logical_and(keep, row != SUB - 1)
        return keep

    def grown(r, s):
        gp = jnp.maximum(r, 0.0)
        gm = jnp.maximum(-r, 0.0)
        square = s * s
        p = square * (1.001 * gp + 0.001 * gm + RAA)
        q = square * (0.001 * gp + 1.001 * gm + RAA)
        return p, q, s * (1.002 * (gp + gm) + 2 * RAA)

    def rows(f, j, packed, ks):
        total = zero
        for k in ks:
            x, t = divmod(k, tiles)
            value = mid[f, k]
            for i in range(2):
                if x == (0, nx - 1)[i]:
                    y = SUB + t * SUB
                    h = xpad[i, f, y : y + SUB, :]
                    pair = xpad[i, f, y - 1 : y - 1 + SUB, :] + xpad[i, f, y + 1 : y + 1 + SUB, :]
                    value += along(W1 * h + W2 * pair, W2 * h + W3 * pair)
            packed = place(packed, value, k, j)
            for i, y in enumerate((0, ny - 1)):
                if t == y // SUB:
                    if k in faces:
                        line = jnp.broadcast_to(ymid[i, f, x : x + 1, :], (SUB, LANE))
                        value += jnp.where(row == y % SUB, line, 0.0)
                    else:
                        ymid[i, f, x : x + 1, :] = value[y % SUB : y % SUB + 1, :]
            s = piece(span_ref, k)
            pp[f, k], qq[f, k], base = grown(value * invden[k], s)
            total += jnp.where(keep_of(k), base, 0.0)
        if f:
            acc[SUMS - 1 + f] = total + (zero if ks is core else acc[SUMS - 1 + f])
        return packed

    def respond(k, weights):
        big_p, big_q = pp[0, k], qq[0, k]
        for j in range(FIELDS):
            big_p += weights[j] * pp[j + 1, k]
            big_q += weights[j] * qq[j + 1, k]
        s = piece(span_ref, k) if k < chunks else around[0, k - chunks]
        d = piece(dens_ref, k) if k < chunks else around[1, k - chunks]
        root_p = jnp.sqrt(big_p)
        root_q = jnp.sqrt(big_q)
        lower, upper = d - s, d + s
        moved = (root_p * lower + root_q * upper) / (root_p + root_q)
        low = jnp.maximum(0.0, d - MOVE * s)
        high = jnp.minimum(1.0, d + MOVE * s)
        return jnp.minimum(jnp.maximum(moved, low), high), big_p, big_q, lower, upper

    def terms(k, weights, keep=None):
        moved, big_p, big_q, lower, upper = respond(k, weights)
        ia = 1.0 / (upper - moved)
        ib = 1.0 / (moved - lower)
        ia2, ib2 = ia * ia, ib * ib
        inv = 1.0 / (2.0 * big_p * (ia2 * ia) + 2.0 * big_q * (ib2 * ib))
        if keep is not None:
            ia, ib, ia2, ib2 = [jnp.where(keep, v, 0.0) for v in (ia, ib, ia2, ib2)]
        grads, slopes, ratios = [], [], []
        for j in range(FIELDS):
            p, q = pp[j + 1, k], qq[j + 1, k]
            grads.append(p * ia + q * ib)
            a = p * ia2 - q * ib2
            slopes.append(a)
            ratios.append(a * inv)
        return grads, slopes, ratios

    def main_sums(weights, ks, masked, more):
        grads = [acc[j] if more else zero for j in range(FIELDS)]
        for k in ks:
            extra, slopes, ratios = terms(k, weights, keep_of(k) if masked else None)
            for j in range(FIELDS):
                grads[j] += extra[j]
                slope[j, k] = slopes[j]
                scaled[j, k] = ratios[j]
        for j in range(FIELDS):
            acc[j] = grads[j]
        at_row = FIELDS
        for group in ((0, 1), (2, 3), (4, 5, 6, 7, 8)):
            keys = [(i, j) for i in group for j in range(i, FIELDS)]
            sums = {key: acc[at_row + n] if more else zero for n, key in enumerate(keys)}
            for k in ks:
                right = {j: slope[j, k] for j in range(group[0], FIELDS)}
                for i in group:
                    left = scaled[i, k]
                    for j in range(i, FIELDS):
                        sums[i, j] += left * right[j]
            for key in keys:
                acc[at_row] = sums[key]
                at_row += 1

    def combined(ref, *index):
        last = 0 if single else 1
        low = pltpu.roll(ref[(0,) + index], 1, 1)
        high = pltpu.roll(ref[(last,) + index], LANE - 1, 1)
        if single:
            upper = me["gz"] == 1
            return jnp.where(odd, jnp.where(upper, low, 0.0), jnp.where(upper, 0.0, high))
        return jnp.where(odd, low, high)

    def outer_edges():
        last_x, last_t = wide_x * (nx - 1), 2 * (tiles - 1)
        yz = [combined(yzrecv, n) for n in range(2)]
        xz = [combined(xzrecv, n) for n in range(2)]
        cz_ = [combined(czrecv, n) for n in range(4)]

        def pick(value, g, shift):
            return turned(jnp.broadcast_to(value[g : g + 1, :], (SUB, LANE)), shift)

        def beside(c, first, final):
            down = pltpu.roll(c, 1, 0)
            up = pltpu.roll(c, SUB - 1, 0)
            before = jnp.where(row == 0, jnp.where(t_of == 0, first, turned(down, 2)), down)
            after = jnp.where(row == SUB - 1, jnp.where(t_of == tiles - 1, final, turned(up, LANE - 2)), up)
            return before + after

        out = []
        for g in range(count_of):
            c = combined(zrecv, g)
            s = beside(c, pick(yz[0], g, -last_t), pick(yz[1], g, last_t))
            c_low = turned(xz[0], -wide_x * g)
            c_high = turned(xz[1], last_x - wide_x * g)
            s_low = beside(c_low, pick(cz_[0], g, -last_x - last_t), pick(cz_[1], g, -last_x + last_t))
            s_high = beside(c_high, pick(cz_[2], g, last_x - last_t), pick(cz_[3], g, last_x + last_t))

            def pair(own, low, high):
                return (jnp.where(x_of == 0, low, turned(own, wide_x))
                        + jnp.where(x_of == nx - 1, high, turned(own, -wide_x)))
            out.append(W1 * c + W2 * (s + pair(c, c_low, c_high)) + W3 * pair(s, s_low, s_high))
        return out

    body_rows = jnp.logical_and(inside, jnp.logical_and(row != 0, row != nx - 1))

    def face_rows():
        drops = [[zero, zero] for _ in groups]
        bases = []
        for g, fields in enumerate(groups):
            for j, f in enumerate(fields):
                base = zero
                for i in range(2):
                    h = yrecv[i, f]
                    low = jnp.broadcast_to(crecv[i, f], (SUB, LANE))
                    high = jnp.broadcast_to(crecv[2 + i, f], (SUB, LANE))
                    pair = (jnp.where(row == 0, low, pltpu.roll(h, 1, 0))
                            + jnp.where(row == nx - 1, high, pltpu.roll(h, nx - 1, 0)))
                    extra = along(W1 * h + W2 * pair, W2 * h + W3 * pair)
                    s = around[0, 1 + i]
                    face = jnp.logical_or(row == 0, row == nx - 1)
                    value = jnp.where(face, 0.0, ymid[i, f]) + extra
                    p, q, more = grown(value * around[2, 1 + i], s)
                    pp[f, chunks + 1 + i] = p
                    qq[f, chunks + 1 + i] = q
                    base += jnp.where(body_rows, more, 0.0)
                    ymid[i, f, 0:1, :] = extra[:1]
                    ymid[i, f, nx - 1 : nx, :] = extra[nx - 1 :]
                    here = jnp.logical_and(row == x_of, lane // slots == j)
                    side = jnp.where(odd, jnp.broadcast_to(extra[:, :1], (SUB, LANE)),
                                     jnp.broadcast_to(extra[:, LANE - 1 :], (SUB, LANE)))
                    drops[g][i] = jnp.where(here, side, drops[g][i])
                bases.append(base)
        for i in range(2):
            s = around[0, 1 + i]
            pp[FIELDS, chunks + 1 + i] = s * s * (1.001 + RAA)
            qq[FIELDS, chunks + 1 + i] = s * s * (0.001 + RAA)
        extras = []
        for g in range(count_of):
            value = zero
            for i, y in enumerate((0, ny - 1)):
                full = jnp.broadcast_to(jnp.sum(drops[g][i], axis=0, keepdims=True), (SUB, LANE))
                here = jnp.logical_and(row == y % SUB, t_of == y // SUB)
                value += jnp.where(here, full, 0.0)
            extras.append(value)
        return extras, bases[1:]

    def edge_rows(extras):
        outer = outer_edges()
        s = around[0, 0]
        bases = []
        for g, fields in enumerate(groups):
            p, q, base = grown((inner[g] + extras[g] + outer[g]) * around[2, 0], s)
            for j, f in enumerate(fields):
                pp[f, chunks] = turned(p, -j * slots)
                qq[f, chunks] = turned(q, -j * slots)
                bases.append(turned(base, -j * slots))
        pp[FIELDS, chunks] = s * s * (1.001 + RAA)
        qq[FIELDS, chunks] = s * s * (0.001 + RAA)
        return bases[1:]

    def extra_sums(weights, ks, keep, bases):
        pieces = [terms(k, weights, keep) for k in ks]
        grads = [sum((p[0][j] for p in pieces[1:]), pieces[0][0][j]) for j in range(FIELDS)]
        squares = [sum((p[2][i] * p[1][j] for p in pieces[1:]), pieces[0][2][i] * pieces[0][1][j])
                   for i in range(FIELDS) for j in range(i, FIELDS)]
        for r, value in enumerate(grads + squares + list(bases)):
            acc[r] += value

    def between():
        repair()
        for moves in [moves_c, moves_y] + xs + [moves_z]:
            for send, _, copy in moves:
                pl.when(send)(copy.wait_send)

    def repair():
        for f in range(FIELDS):
            for ref in (pp, qq):
                edge = ref[f, chunks]
                for k in range(chunks):
                    x, t = divmod(k, tiles)
                    value = ref[f, k]
                    for i, y in enumerate((0, ny - 1)):
                        if t == y // SUB and k in core:
                            line = jnp.broadcast_to(ref[f, chunks + 1 + i, x : x + 1, :], (SUB, LANE))
                            value = jnp.where(row == y % SUB, line, value)
                    ref[f, k] = jnp.where(ends, turned(edge, -2 * k - 1), value)

    def flat(axes):
        index = 0
        for a in axes:
            index = index * shape[a] + me[a]
        return index

    def exchange(it, meanwhile):
        packed = zero
        for g in range(wide.shape[0]):
            values = [acc[r] if r < ROWS else zero for r in range(g * SUB, (g + 1) * SUB)]
            half = SUB // 2
            while half:
                upper = (row // half) % 2 == 1
                step = len(values) // 2
                values = [
                    jnp.where(upper, b, a) + pltpu.roll(jnp.where(upper, a, b), half, 0)
                    if half == SUB // 2 else
                    jnp.where(upper, b + turned(b, half, 0), a + turned(a, -half, 0))
                    for a, b in zip(values[:step], values[step:])
                ]
                half //= 2
            packed = jnp.where(lane == g * SUB + row, jnp.sum(values[0], axis=1, keepdims=True), packed)
        value = jnp.sum(packed, axis=0, keepdims=True)
        for n, axes in enumerate(stages):
            size = math.prod(shape[a] for a in axes)
            part[it, n] = value
            recvs[n][it, flat(axes)] = value
            for o in sorted(offsets(axes, shape), key=lambda o: (-abs(o[-1] - 2), o), reverse=True):
                target = {a: lax.rem(me[a] + d, shape[a]) for a, d in zip(axes, o)}
                pltpu.make_async_remote_copy(
                    src_ref=part.at[it, n], dst_ref=recvs[n].at[it, flat(axes)],
                    send_sem=sum_send.at[it, n], recv_sem=sum_recv.at[it, n],
                    device_id=target, device_id_type=MESH).start()
            if n == 0:
                meanwhile()
            whole = recvs[n].at[it, pl.ds(0, size - 1)]
            pltpu.make_async_copy(whole, whole, sum_recv.at[it, n]).wait()
            values = [recvs[n][it, i] for i in range(size)]
            while len(values) > 1:
                values = [sum(values[i + 1 : i + 2], values[i]) for i in range(0, len(values), 2)]
            value = values[0]
        every = jnp.broadcast_to(value, (SUB, LANE))
        for g in range(wide.shape[0]):
            one = jnp.sum(jnp.where(lane == g * SUB + row, every, 0.0), axis=1, keepdims=True)
            wide[g] = jnp.broadcast_to(one, (SUB, LANE))

    def solve(weights):
        def read(r):
            return jnp.broadcast_to(wide[r // SUB, r % SUB : r % SUB + 1, :], (SUB, LANE))
        b = [read(j) - (1.0 - viol_ref[j]) * read(SUMS + j) for j in range(FIELDS)]
        m = {}
        at_row = FIELDS
        for i in range(FIELDS):
            for j in range(i, FIELDS):
                m[i, j] = read(at_row)
                at_row += 1
        trace = m[0, 0]
        for i in range(1, FIELDS):
            trace += m[i, i]
        shift = REG * trace / FIELDS
        for i in range(FIELDS):
            m[i, i] += shift
        inverse = []
        for k in range(FIELDS):
            inverse.append(1.0 / m[k, k])
            for i in range(k + 1, FIELDS):
                factor = m[k, i] * inverse[k]
                for j in range(i, FIELDS):
                    m[i, j] -= factor * m[k, j]
                b[i] -= factor * b[k]
        delta = [None] * FIELDS
        for k in reversed(range(FIELDS)):
            v = b[k]
            for j in range(k + 1, FIELDS):
                v -= m[k, j] * delta[j]
            delta[k] = v * inverse[k]
        for k in range(FIELDS):
            lam[k] = jnp.maximum(weights[k] + delta[k], FLOOR * weights[k])

    def newton(it, carry):
        weights = [lam[j] for j in range(FIELDS)]
        main_sums(weights, range(chunks), False, False)
        exchange(it, lambda: None)
        solve(weights)
        return carry

    inner = []
    for g, fields in enumerate(groups):
        packed = zero
        for j, f in enumerate(fields):
            packed = rows(f, j, packed, core)
        inner.append(packed)
    main_sums(weights, core, True, False)
    if near:
        pl.semaphore_wait(known.at[0], friends)
        tell(1)
    receive(moves_y)
    receive(moves_c)
    extras, bases = face_rows()
    extra_sums(weights, (chunks + 1, chunks + 2), body_rows, bases)
    for g, fields in enumerate(groups):
        receive(xs[g])
        for j, f in enumerate(fields):
            inner[g] = rows(f, j, inner[g], faces)
    main_sums(weights, faces, True, True)
    receive(moves_z)
    within = lane < slots
    bases = [jnp.where(within, v, 0.0) for v in edge_rows(extras)]
    extra_sums(weights, (chunks,), within, bases)
    if near:
        pl.semaphore_wait(known.at[1], friends)
    exchange(0, between)
    solve(weights)
    lax.fori_loop(1, ITERS, newton, 0)

    weights = [lam[j] for j in range(FIELDS)]
    for k in range(chunks):
        x, t = divmod(k, tiles)
        out_ref[x, t * SUB : (t + 1) * SUB, :] = respond(k, weights)[0]
    final = zero
    for j in range(FIELDS):
        final = jnp.where(lane == j, weights[j], final)
    lam_out[...] = final

    for it in range(ITERS):
        for n, axes in enumerate(stages):
            size = math.prod(shape[a] for a in axes)
            whole = recvs[n].at[it, pl.ds(0, size - 1)]
            pltpu.make_async_copy(whole, whole, sum_send.at[it, n]).wait()


def finish(field_ref, lam_ref, field_out, lam_out, row, sem):
    whole = pltpu.make_async_copy(field_ref, field_out, sem.at[0])
    whole.start()
    row[...] = lam_ref[0, :FIELDS]
    short = pltpu.make_async_copy(row, lam_out, sem.at[1])
    short.start()
    whole.wait()
    short.wait()


def shards(shape, density, spread, sensitivities, violation, multipliers_start):
    nx, ny, nz = density.shape
    chunks = nx * ny // SUB
    groups = len(steps())
    stages = plan(shape)
    corners = 9 if shape["gz"] == 2 else 18
    depth = corners // 9
    f32 = jnp.float32
    vmem = pl.BlockSpec(memory_space=pltpu.VMEM)
    dma = pltpu.SemaphoreType.DMA
    hbm = pl.BlockSpec(memory_space=pltpu.HBM)
    field, lam = pl.pallas_call(
        functools.partial(body, shape, (nx, ny, nz)),
        out_shape=(
            pltpu.VMEM((nx, ny, nz), f32),
            pltpu.VMEM((SUB, LANE), f32),
        ),
        in_specs=[hbm] * 5,
        out_specs=(vmem, vmem),
        scratch_shapes=[
            pltpu.VMEM((nx, ny, nz), f32),
            pltpu.VMEM((nx, ny, nz), f32),
            pltpu.SMEM((FIELDS,), f32),
            pltpu.SMEM((FIELDS,), f32),
            pltpu.VMEM((FIELDS, nx, ny + 2 * SUB, nz), f32),
            pltpu.VMEM((2, FIELDS, ny + 2 * SUB, nz), f32),
            pltpu.VMEM((2, FIELDS, nx, nz), f32),
            pltpu.VMEM((2, FIELDS, nx, nz), f32),
            pltpu.VMEM((4, FIELDS, 1, nz), f32),
            pltpu.VMEM((4, FIELDS, 1, nz), f32),
            pltpu.VMEM((2, FIELDS, nx, nz), f32),
            pltpu.VMEM((groups, SUB, LANE), f32),
            pltpu.VMEM((depth, groups, SUB, LANE), f32),
            pltpu.VMEM((2, SUB, LANE), f32),
            pltpu.VMEM((depth, 2, SUB, LANE), f32),
            pltpu.VMEM((2, SUB, LANE), f32),
            pltpu.VMEM((depth, 2, SUB, LANE), f32),
            pltpu.VMEM((depth, 4, SUB, LANE), f32),
            pltpu.VMEM((3, 3, SUB, LANE), f32),
            pltpu.VMEM((FIELDS, chunks, SUB, LANE), f32),
            pltpu.VMEM((chunks, SUB, LANE), f32),
            pltpu.VMEM((FIELDS + 1, chunks + 3, SUB, LANE), f32),
            pltpu.VMEM((FIELDS + 1, chunks + 3, SUB, LANE), f32),
            pltpu.VMEM((FIELDS, chunks, SUB, LANE), f32),
            pltpu.VMEM((FIELDS, chunks, SUB, LANE), f32),
            pltpu.VMEM((ROWS, SUB, LANE), f32),
            pltpu.VMEM((-(-ROWS // SUB), SUB, LANE), f32),
            pltpu.VMEM((FIELDS, SUB, LANE), f32),
            pltpu.VMEM((ITERS, len(stages), 1, LANE), f32),
        ] + [
            pltpu.VMEM((ITERS, math.prod(shape[a] for a in axes), 1, LANE), f32) for axes in stages
        ] + [
            dma((5,)), dma((6 + 2 * groups,)), dma((6 + 2 * groups,)), dma((corners,)), dma((corners,)),
            dma((ITERS, len(stages))), dma((ITERS, len(stages))), pltpu.SemaphoreType.REGULAR((2,)),
        ],
        compiler_params=pltpu.CompilerParams(
            collective_id=0, has_side_effects=True, vmem_limit_bytes=24 << 20),
        name="design_step",
    )(*[pltpu.with_memory_space_constraint(v, pltpu.HBM) for v in (density, spread, sensitivities, violation, multipliers_start)])
    return pl.pallas_call(
        finish,
        out_shape=(
            jax.ShapeDtypeStruct((nx, ny, nz), f32),
            jax.ShapeDtypeStruct((FIELDS,), f32),
        ),
        in_specs=[vmem, vmem],
        out_specs=(hbm, hbm),
        scratch_shapes=[pltpu.VMEM((FIELDS,), f32), dma((2,))],
        compiler_params=pltpu.CompilerParams(vmem_limit_bytes=1 << 20),
        name="finish",
    )(field, lam)


def solution(mesh):
    shape = {a: int(mesh.shape[a]) for a in AXES}
    return jax.shard_map(
        functools.partial(shards, shape),
        mesh=mesh,
        in_specs=(P("gx", "gy", "gz"), P("gx", "gy", "gz"), P(None, "gx", "gy", "gz"), P(), P()),
        out_specs=(P("gx", "gy", "gz"), P()),
        check_vma=False,
    )
```

```python
import functools
import math

import jax
import jax.numpy as jnp
from jax import lax
from jax.experimental import pallas as pl
from jax.experimental.pallas import tpu as pltpu
from jax.sharding import PartitionSpec as P

FIELDS = 9
ITERS = 3

RADIUS = 3.0
RAA = 1e-05
MOVE = 0.9
REG = 0.001
FLOOR = 0.2

W0 = RADIUS
W1 = RADIUS - 1.0
W2 = RADIUS - math.sqrt(2.0)
W3 = RADIUS - math.sqrt(3.0)

SUB, LANE = 8, 128
AXES = ("gz", "gy", "gx")
SUMS = FIELDS + FIELDS * (FIELDS + 1) // 2
ROWS = SUMS + FIELDS
MESH = pl.DeviceIdType.MESH
GROUP = 3
KEPT = 2


def compact(shape):
    return shape["gz"] == 2 and shape["gy"] in (2, 4) and shape["gx"] <= 4


def plan(shape):
    total = math.prod(shape[a] for a in AXES)
    if total <= 32:
        return (AXES,)
    return tuple((a,) for a in AXES)


def offsets(axes, shape):
    out = [()]
    for a in axes:
        out = [o + (d,) for o in out for d in range(shape[a])]
    return [o for o in out if any(o)]


def steps():
    return [range(f, min(f + GROUP, FIELDS)) for f in range(0, FIELDS, GROUP)]


def body(shape, dims, dens_hbm, span_hbm, sens_ref, viol_hbm, lam0_hbm, out_ref, lam_out,
         dens_ref, span_ref, dens_more, span_more, viol_ref, lam0_ref, pad, xpad, ypack, yrecv, cpack, crecv, ymid,
         zpack, zrecv, xzpack, xzrecv, yzpack, yzrecv, czrecv, around, mid, invden, pp, qq, slope, scaled,
         acc, wide, lam, part, *rest):
    stages = plan(shape)
    recvs = rest[: len(stages)]
    load_sem, send_sem, recv_sem, zsend_sem, zrecv_sem, lend_send, lend_recv, sum_send, sum_recv, known = rest[len(stages):]
    nx, ny, nz = dims
    tiles = ny // SUB
    chunks = nx * tiles
    slots = 2 * chunks
    load = pltpu.make_async_copy(
        sens_ref, pad.at[:, :, SUB : SUB + ny, :], load_sem.at[0]
    )
    load.start()
    small = [
        pltpu.make_async_copy(src, dst, load_sem.at[1 + i])
        for i, (src, dst) in enumerate([
            (span_hbm, span_ref), (dens_hbm, dens_ref), (viol_hbm, viol_ref), (lam0_hbm, lam0_ref)])
    ]
    for copy in small:
        copy.start()
    wide_x = 2 * tiles
    groups = steps()
    count_of = len(groups)
    me = {a: lax.axis_index(a) for a in AXES}

    has = {}
    for a in AXES:
        has[a, -1] = me[a] > 0
        has[a, 0] = jnp.bool_(True)
        has[a, 1] = me[a] < shape[a] - 1

    def both(o):
        moved = [has[a, d] for a, d in zip(AXES, o) if d and not (single and a == "gz")]
        return functools.reduce(jnp.logical_and, moved, jnp.bool_(True))

    single = shape["gz"] == 2
    if single:
        has["gz", 1] = jnp.bool_(True)

    def at(**moves):
        out = {a: me[a] + d for a, d in moves.items()}
        if single and moves.get("gz"):
            out["gz"] = 1 - me["gz"]
        return out

    signs = (-1, 0, 1)
    plane = [(0, dy, dx) for dy in signs for dx in signs if dy or dx]
    ring = [(dz, dy, dx) for dz in ((1, 0) if single else signs) for dy in signs for dx in signs if dz or dy or dx]
    ring.sort(key=lambda o: (-sum(map(abs, o)), o))
    if single:
        has["gz", -1] = has["gz", 1]
    sides = ((0, 1),) if single else ((0, 1), (1, -1))
    barrier = pltpu.get_barrier_semaphore()
    near = compact(shape)
    distant = lax.rem(me["gy"], 2) == 0
    lent = chunks + 3
    if near:
        for o in ring:
            @pl.when(both(o))
            def _(o=o):
                pl.semaphore_signal(barrier, inc=1, device_id=at(gz=o[0], gy=o[1], gx=o[2]),
                                    device_id_type=MESH)
        arrivals = sum(both(o).astype(jnp.int32) for o in ring)
    else:
        partners = set()
        for axes in stages:
            for o in offsets(axes, shape):
                partners.add(tuple(dict(zip(axes, o)).get(a, 0) for a in AXES))
        for d in ring:
            o = tuple(d % shape[a] for a, d in zip(AXES, d))
            if any(o):
                partners.add(o)
        partners = sorted(partners)
        for o in partners:
            target = {a: lax.rem(me[a] + d, shape[a]) for a, d in zip(AXES, o)}
            pl.semaphore_signal(barrier, inc=1, device_id=target, device_id_type=MESH)
        arrivals = len(partners)

    lane = lax.broadcasted_iota(jnp.int32, (SUB, LANE), 1)
    row = lax.broadcasted_iota(jnp.int32, (SUB, LANE), 0)
    zero = jnp.zeros((SUB, LANE), jnp.float32)
    slot = lane % slots
    x_of = slot // wide_x
    t_of = (slot % wide_x) // 2
    odd = (lane % 2) == 1
    ends = jnp.logical_or(lane == 0, lane == LANE - 1)

    corners = [(sx, sy) for sx in (1, -1) for sy in (1, -1)]
    line = jnp.zeros((1, LANE), jnp.float32)
    for f in range(FIELDS):
        for x in range(nx):
            pad[f, x, SUB - 1 : SUB, :] = line
            pad[f, x, SUB + ny : SUB + ny + 1, :] = line
        for i in range(2):
            xpad[i, f, SUB - 1 : SUB, :] = line
            xpad[i, f, SUB + ny : SUB + ny + 1, :] = line
    for i, sx in enumerate((1, -1)):
        @pl.when(jnp.logical_not(has["gx", -sx]))
        def _(i=i):
            xpad[i, :, SUB : SUB + ny, :] = jnp.zeros((FIELDS, ny, LANE), jnp.float32)
    for i, sy in enumerate((1, -1)):
        @pl.when(jnp.logical_not(has["gy", -sy]))
        def _(i=i):
            yrecv[i] = jnp.zeros((FIELDS, nx, LANE), jnp.float32)
    for i, (sx, sy) in enumerate(corners):
        @pl.when(jnp.logical_not(jnp.logical_and(has["gx", -sx], has["gy", -sy])))
        def _(i=i):
            crecv[i] = jnp.zeros((FIELDS, 1, LANE), jnp.float32)
    for i, sz in sides:
        if not single:
            @pl.when(jnp.logical_not(has["gz", -sz]))
            def _(i=i):
                zrecv[i] = jnp.zeros(zrecv.shape[1:], jnp.float32)
        for n, sx in enumerate((1, -1)):
            @pl.when(jnp.logical_not(both((-sz, 0, -sx))))
            def _(i=i, n=n):
                xzrecv[i, n] = zero
        for n, sy in enumerate((1, -1)):
            @pl.when(jnp.logical_not(both((-sz, -sy, 0))))
            def _(i=i, n=n):
                yzrecv[i, n] = zero
        for n, (sx, sy) in enumerate(corners):
            @pl.when(jnp.logical_not(both((-sz, -sy, -sx))))
            def _(i=i, n=n):
                czrecv[i, n] = zero

    def count(a, index, extent):
        low = jnp.where(jnp.logical_and(me[a] == 0, index == 0), 0.0, 1.0)
        high = jnp.where(jnp.logical_and(me[a] == shape[a] - 1, index == extent - 1), 0.0, 1.0)
        return low + high
    cz = count("gz", lane, nz)
    for x in range(nx):
        cx = count("gx", jnp.full((SUB, LANE), x, jnp.int32), nx)
        for t in range(tiles):
            cy = count("gy", row + t * SUB, ny)
            den = W0 + W1 * (cx + cy + cz) + W2 * (cx * cy + cy * cz + cx * cz) + W3 * (cx * cy * cz)
            k = x * tiles + t
            invden[k] = 1.0 / den

    load.wait()

    def turned(value, shift, axis=1):
        shift %= value.shape[axis]
        return pltpu.roll(value, shift, axis) if shift else value

    def place(packed, value, k, j):
        here = lane // 2 == k + j * chunks
        return jnp.where(here, turned(value, 2 * k + 1 + j * slots), packed)

    edges = []
    for g, fields in enumerate(groups):
        packed = zero
        for j, f in enumerate(fields):
            for k in range(chunks):
                x, t = divmod(k, tiles)
                packed = place(packed, pad[f, x, SUB + t * SUB : 2 * SUB + t * SUB, :], k, j)
        zpack[g] = packed
        edges.append(packed)
    for n, x in enumerate((nx - 1, 0)):
        packed = zero
        for g in range(count_of):
            packed = jnp.where(x_of == g, turned(edges[g], (g - x) * wide_x), packed)
        xzpack[n] = packed
    for n, y in enumerate((SUB - 1, 0)):
        packed = zero
        for g in range(count_of):
            packed = jnp.where(row == g, jnp.broadcast_to(edges[g][y : y + 1, :], (SUB, LANE)), packed)
        yzpack[n] = packed
    for f in range(FIELDS):
        for i, y in enumerate((SUB + ny - 1, SUB)):
            for x in range(nx):
                ypack[i, f, x : x + 1, :] = pad[f, x, y : y + 1, :]
        for i, (sx, sy) in enumerate(corners):
            x = nx - 1 if sx > 0 else 0
            y = SUB + ny - 1 if sy > 0 else SUB
            cpack[i, f] = pad[f, x, y : y + 1, :]

    pl.semaphore_wait(barrier, arrivals)

    def remote(src, dst, sends, recvs_, index, **moves):
        copy = pltpu.make_async_remote_copy(
            src_ref=src, dst_ref=dst, send_sem=sends.at[index], recv_sem=recvs_.at[index],
            device_id=at(**moves), device_id_type=MESH)
        there = both([moves.get(a, 0) for a in AXES])
        back = both([-moves.get(a, 0) for a in AXES])
        return there, back, copy

    def moves_x(g):
        fields = pl.ds(groups[g][0], len(groups[g]))
        return [
            remote(pad.at[fields, nx - 1 if sx > 0 else 0, SUB : SUB + ny, :],
                   xpad.at[i, fields, SUB : SUB + ny, :], send_sem, recv_sem, 6 + 2 * g + i, gx=sx)
            for i, sx in enumerate((1, -1))
        ]

    moves_c = [remote(cpack.at[i], crecv.at[i], send_sem, recv_sem, 2 + i, gx=sx, gy=sy)
               for i, (sx, sy) in enumerate(corners)]
    moves_y = [remote(ypack.at[i], yrecv.at[i], send_sem, recv_sem, i, gy=sy)
               for i, sy in enumerate((1, -1))]
    moves_z = []
    for i, sz in sides:
        first = 9 * i
        for n, (sx, sy) in enumerate(corners):
            moves_z.append(remote(yzpack.at[n % 2], czrecv.at[i, n], zsend_sem, zrecv_sem, first + 5 + n,
                                  gz=sz, gx=sx, gy=sy))
        for n, sx in enumerate((1, -1)):
            moves_z.append(remote(xzpack.at[n], xzrecv.at[i, n], zsend_sem, zrecv_sem, first + 1 + n,
                                  gz=sz, gx=sx))
        for n, sy in enumerate((1, -1)):
            moves_z.append(remote(yzpack.at[n], yzrecv.at[i, n], zsend_sem, zrecv_sem, first + 3 + n,
                                  gz=sz, gy=sy))
        moves_z.append(remote(zpack, zrecv.at[i], zsend_sem, zrecv_sem, first, gz=sz))

    lend = [
        pltpu.make_async_remote_copy(
            src_ref=src, dst_ref=dst, send_sem=lend_send.at[n], recv_sem=lend_recv.at[n],
            device_id={"gy": me["gy"] + 1 - 2 * lax.rem(me["gy"], 2)}, device_id_type=MESH)
        for n, (src, dst) in enumerate([
            (span_ref.at[pl.ds(KEPT, nx - KEPT)], span_more), (dens_ref.at[pl.ds(KEPT, nx - KEPT)], dens_more),
            (pp.at[:, pl.ds(KEPT * tiles, chunks - KEPT * tiles)], pp.at[:, pl.ds(lent, chunks - KEPT * tiles)]),
            (qq.at[:, pl.ds(KEPT * tiles, chunks - KEPT * tiles)], qq.at[:, pl.ds(lent, chunks - KEPT * tiles)])])
    ] if near else []

    def start(moves):
        for send, _, copy in moves:
            pl.when(send)(copy.start)

    def receive(moves):
        for _, expected, copy in moves:
            pl.when(expected)(copy.wait_recv)

    friends = sum(both(o).astype(jnp.int32) for o in plane)

    def tell(n):
        for o in plane:
            @pl.when(both(o))
            def _(o=o):
                pl.semaphore_signal(known.at[n], inc=1, device_id=at(gy=o[1], gx=o[2]),
                                    device_id_type=MESH)

    xs = [moves_x(g) for g in range(count_of)]
    start(moves_z)
    start(moves_c)
    start(xs[0])
    start(moves_y)
    for g in range(1, count_of):
        start(xs[g])
    if near:
        tell(0)

    def along(s0, s1):
        up = jnp.where(lane == 0, 0.0, pltpu.roll(s1, 1, 1))
        down = jnp.where(lane == LANE - 1, 0.0, pltpu.roll(s1, LANE - 1, 1))
        return s0 + up + down

    for f in range(FIELDS):
        for t in range(tiles):
            y = SUB + t * SUB
            mids, sides = [None], [None]
            for x in range(nx):
                mids.append(pad[f, x, y : y + SUB, :])
                sides.append(pad[f, x, y - 1 : y - 1 + SUB, :] + pad[f, x, y + 1 : y + 1 + SUB, :])
            mids.append(None)
            sides.append(None)
            for x in range(nx):
                next_to = [v for v in (mids[x], mids[x + 2]) if v is not None]
                beyond = [v for v in (sides[x], sides[x + 2]) if v is not None]
                close = sides[x + 1] + sum(next_to[1:], next_to[0])
                far = sum(beyond[1:], beyond[0])
                s0 = W0 * mids[x + 1] + W1 * close + W2 * far
                s1 = W1 * mids[x + 1] + W2 * close + W3 * far
                mid[f, x * tiles + t] = along(s0, s1)

    def piece(ref, k):
        x, t = divmod(k, tiles)
        return ref[x, t * SUB : (t + 1) * SUB, :]

    for copy in small:
        copy.wait()
    for copy in lend[:2]:
        pl.when(distant)(copy.start)
    for n, ref in enumerate((span_ref, dens_ref, invden)):
        packed = zero
        for k in range(chunks):
            value = ref[k] if n == 2 else piece(ref, k)
            for j in range(LANE // slots):
                packed = place(packed, value, k, j)
        around[n, 0] = packed
        for i, y in enumerate((0, ny - 1)):
            for x in range(nx):
                k = x * tiles + y // SUB
                around[n, 1 + i, x : x + 1, :] = (
                    ref[k, y % SUB : y % SUB + 1, :] if n == 2 else ref[x, y : y + 1, :])
    for k in range(FIELDS):
        lam[k] = jnp.full((SUB, LANE), lam0_ref[k], jnp.float32)
    total = zero
    for k in range(chunks):
        s = piece(span_ref, k)
        square = s * s
        pp[FIELDS, k] = square * (1.001 + RAA)
        qq[FIELDS, k] = square * (0.001 + RAA)
        total += s * (1.002 + 2 * RAA)
    acc[ROWS - 1] = total
    weights = [lam[j] for j in range(FIELDS)]

    inside = jnp.logical_not(ends)
    core = range(tiles, chunks - tiles)
    faces = [k for k in range(chunks) if k not in core]

    def keep_of(k):
        keep = inside
        if k in faces:
            return keep
        if k % tiles == 0:
            keep = jnp.logical_and(keep, row != 0)
        if k % tiles == tiles - 1:
            keep = jnp.logical_and(keep, row != SUB - 1)
        return keep

    def grown(r, s):
        gp = jnp.maximum(r, 0.0)
        gm = jnp.maximum(-r, 0.0)
        square = s * s
        p = square * (1.001 * gp + 0.001 * gm + RAA)
        q = square * (0.001 * gp + 1.001 * gm + RAA)
        return p, q, s * (1.002 * (gp + gm) + 2 * RAA)

    def rows(f, j, packed, ks):
        total = zero
        for k in ks:
            x, t = divmod(k, tiles)
            value = mid[f, k]
            for i in range(2):
                if x == (0, nx - 1)[i]:
                    y = SUB + t * SUB
                    h = xpad[i, f, y : y + SUB, :]
                    pair = xpad[i, f, y - 1 : y - 1 + SUB, :] + xpad[i, f, y + 1 : y + 1 + SUB, :]
                    value += along(W1 * h + W2 * pair, W2 * h + W3 * pair)
            packed = place(packed, value, k, j)
            for i, y in enumerate((0, ny - 1)):
                if t == y // SUB:
                    if k in faces:
                        line = jnp.broadcast_to(ymid[i, f, x : x + 1, :], (SUB, LANE))
                        value += jnp.where(row == y % SUB, line, 0.0)
                    else:
                        ymid[i, f, x : x + 1, :] = value[y % SUB : y % SUB + 1, :]
            s = piece(span_ref, k)
            pp[f, k], qq[f, k], base = grown(value * invden[k], s)
            total += jnp.where(keep_of(k), base, 0.0)
        if f:
            acc[SUMS - 1 + f] = total + (zero if ks is core else acc[SUMS - 1 + f])
        return packed

    def respond(k, weights):
        big_p, big_q = pp[0, k], qq[0, k]
        for j in range(FIELDS):
            big_p += weights[j] * pp[j + 1, k]
            big_q += weights[j] * qq[j + 1, k]
        if k >= lent:
            s, d = piece(span_more, k - lent), piece(dens_more, k - lent)
        elif k >= chunks:
            s, d = around[0, k - chunks], around[1, k - chunks]
        else:
            s, d = piece(span_ref, k), piece(dens_ref, k)
        root_p = jnp.sqrt(big_p)
        root_q = jnp.sqrt(big_q)
        lower, upper = d - s, d + s
        moved = (root_p * lower + root_q * upper) / (root_p + root_q)
        low = jnp.maximum(0.0, d - MOVE * s)
        high = jnp.minimum(1.0, d + MOVE * s)
        return jnp.minimum(jnp.maximum(moved, low), high), big_p, big_q, lower, upper

    def terms(k, weights, keep=None):
        moved, big_p, big_q, lower, upper = respond(k, weights)
        ia = 1.0 / (upper - moved)
        ib = 1.0 / (moved - lower)
        ia2, ib2 = ia * ia, ib * ib
        inv = 1.0 / (2.0 * big_p * (ia2 * ia) + 2.0 * big_q * (ib2 * ib))
        if keep is not None:
            ia, ib, ia2, ib2 = [jnp.where(keep, v, 0.0) for v in (ia, ib, ia2, ib2)]
        grads, slopes, ratios = [], [], []
        for j in range(FIELDS):
            p, q = pp[j + 1, k], qq[j + 1, k]
            grads.append(p * ia + q * ib)
            a = p * ia2 - q * ib2
            slopes.append(a)
            ratios.append(a * inv)
        return grads, slopes, ratios

    def main_sums(weights, ks, masked, more):
        grads = [acc[j] if more else zero for j in range(FIELDS)]
        for n, k in enumerate(ks):
            extra, slopes, ratios = terms(k, weights, keep_of(k) if masked else None)
            for j in range(FIELDS):
                grads[j] += extra[j]
                slope[j, n] = slopes[j]
                scaled[j, n] = ratios[j]
        for j in range(FIELDS):
            acc[j] = grads[j]
        at_row = FIELDS
        for group in ((0, 1), (2, 3), (4, 5, 6, 7, 8)):
            keys = [(i, j) for i in group for j in range(i, FIELDS)]
            sums = {key: acc[at_row + n] if more else zero for n, key in enumerate(keys)}
            for n in range(len(ks)):
                right = {j: slope[j, n] for j in range(group[0], FIELDS)}
                for i in group:
                    left = scaled[i, n]
                    for j in range(i, FIELDS):
                        sums[i, j] += left * right[j]
            for key in keys:
                acc[at_row] = sums[key]
                at_row += 1

    def combined(ref, *index):
        last = 0 if single else 1
        low = pltpu.roll(ref[(0,) + index], 1, 1)
        high = pltpu.roll(ref[(last,) + index], LANE - 1, 1)
        if single:
            upper = me["gz"] == 1
            return jnp.where(odd, jnp.where(upper, low, 0.0), jnp.where(upper, 0.0, high))
        return jnp.where(odd, low, high)

    def outer_edges():
        last_x, last_t = wide_x * (nx - 1), 2 * (tiles - 1)
        yz = [combined(yzrecv, n) for n in range(2)]
        xz = [combined(xzrecv, n) for n in range(2)]
        cz_ = [combined(czrecv, n) for n in range(4)]

        def pick(value, g, shift):
            return turned(jnp.broadcast_to(value[g : g + 1, :], (SUB, LANE)), shift)

        def beside(c, first, final):
            down = pltpu.roll(c, 1, 0)
            up = pltpu.roll(c, SUB - 1, 0)
            before = jnp.where(row == 0, jnp.where(t_of == 0, first, turned(down, 2)), down)
            after = jnp.where(row == SUB - 1, jnp.where(t_of == tiles - 1, final, turned(up, LANE - 2)), up)
            return before + after

        out = []
        for g in range(count_of):
            c = combined(zrecv, g)
            s = beside(c, pick(yz[0], g, -last_t), pick(yz[1], g, last_t))
            c_low = turned(xz[0], -wide_x * g)
            c_high = turned(xz[1], last_x - wide_x * g)
            s_low = beside(c_low, pick(cz_[0], g, -last_x - last_t), pick(cz_[1], g, -last_x + last_t))
            s_high = beside(c_high, pick(cz_[2], g, last_x - last_t), pick(cz_[3], g, last_x + last_t))

            def pair(own, low, high):
                return (jnp.where(x_of == 0, low, turned(own, wide_x))
                        + jnp.where(x_of == nx - 1, high, turned(own, -wide_x)))
            out.append(W1 * c + W2 * (s + pair(c, c_low, c_high)) + W3 * pair(s, s_low, s_high))
        return out

    body_rows = jnp.logical_and(inside, jnp.logical_and(row != 0, row != nx - 1))

    def face_rows():
        drops = [[zero, zero] for _ in groups]
        bases = []
        for g, fields in enumerate(groups):
            for j, f in enumerate(fields):
                base = zero
                for i in range(2):
                    h = yrecv[i, f]
                    low = jnp.broadcast_to(crecv[i, f], (SUB, LANE))
                    high = jnp.broadcast_to(crecv[2 + i, f], (SUB, LANE))
                    pair = (jnp.where(row == 0, low, pltpu.roll(h, 1, 0))
                            + jnp.where(row == nx - 1, high, pltpu.roll(h, nx - 1, 0)))
                    extra = along(W1 * h + W2 * pair, W2 * h + W3 * pair)
                    s = around[0, 1 + i]
                    face = jnp.logical_or(row == 0, row == nx - 1)
                    value = jnp.where(face, 0.0, ymid[i, f]) + extra
                    p, q, more = grown(value * around[2, 1 + i], s)
                    pp[f, chunks + 1 + i] = p
                    qq[f, chunks + 1 + i] = q
                    base += jnp.where(body_rows, more, 0.0)
                    ymid[i, f, 0:1, :] = extra[:1]
                    ymid[i, f, nx - 1 : nx, :] = extra[nx - 1 :]
                    here = jnp.logical_and(row == x_of, lane // slots == j)
                    side = jnp.where(odd, jnp.broadcast_to(extra[:, :1], (SUB, LANE)),
                                     jnp.broadcast_to(extra[:, LANE - 1 :], (SUB, LANE)))
                    drops[g][i] = jnp.where(here, side, drops[g][i])
                bases.append(base)
        for i in range(2):
            s = around[0, 1 + i]
            pp[FIELDS, chunks + 1 + i] = s * s * (1.001 + RAA)
            qq[FIELDS, chunks + 1 + i] = s * s * (0.001 + RAA)
        extras = []
        for g in range(count_of):
            value = zero
            for i, y in enumerate((0, ny - 1)):
                full = jnp.broadcast_to(jnp.sum(drops[g][i], axis=0, keepdims=True), (SUB, LANE))
                here = jnp.logical_and(row == y % SUB, t_of == y // SUB)
                value += jnp.where(here, full, 0.0)
            extras.append(value)
        return extras, bases[1:]

    def edge_rows(extras):
        outer = outer_edges()
        s = around[0, 0]
        bases = []
        for g, fields in enumerate(groups):
            p, q, base = grown((inner[g] + extras[g] + outer[g]) * around[2, 0], s)
            for j, f in enumerate(fields):
                pp[f, chunks] = turned(p, -j * slots)
                qq[f, chunks] = turned(q, -j * slots)
                bases.append(turned(base, -j * slots))
        pp[FIELDS, chunks] = s * s * (1.001 + RAA)
        qq[FIELDS, chunks] = s * s * (0.001 + RAA)
        return bases[1:]

    def extra_sums(weights, ks, keep, bases):
        pieces = [terms(k, weights, keep) for k in ks]
        grads = [sum((p[0][j] for p in pieces[1:]), pieces[0][0][j]) for j in range(FIELDS)]
        squares = [sum((p[2][i] * p[1][j] for p in pieces[1:]), pieces[0][2][i] * pieces[0][1][j])
                   for i in range(FIELDS) for j in range(i, FIELDS)]
        for r, value in enumerate(grads + squares + list(bases)):
            acc[r] += value

    def between():
        repair()
        if near:
            for copy in lend[2:]:
                pl.when(distant)(copy.start)
        for moves in [moves_c, moves_y] + xs + [moves_z]:
            for send, _, copy in moves:
                pl.when(send)(copy.wait_send)
        if near:
            for copy in lend:
                pl.when(jnp.logical_not(distant))(copy.wait_recv)

    def repair():
        for f in range(FIELDS):
            for ref in (pp, qq):
                edge = ref[f, chunks]
                for k in range(chunks):
                    x, t = divmod(k, tiles)
                    value = ref[f, k]
                    for i, y in enumerate((0, ny - 1)):
                        if t == y // SUB and k in core:
                            line = jnp.broadcast_to(ref[f, chunks + 1 + i, x : x + 1, :], (SUB, LANE))
                            value = jnp.where(row == y % SUB, line, value)
                    ref[f, k] = jnp.where(ends, turned(edge, -2 * k - 1), value)

    def flat(axes):
        index = 0
        for a in axes:
            index = index * shape[a] + me[a]
        return index

    def exchange(it, count, meanwhile):
        packed = zero
        for g in range(count):
            values = [acc[r] if r < ROWS else zero for r in range(g * SUB, (g + 1) * SUB)]
            half = SUB // 2
            while half:
                upper = (row // half) % 2 == 1
                step = len(values) // 2
                values = [
                    jnp.where(upper, b, a) + pltpu.roll(jnp.where(upper, a, b), half, 0)
                    if half == SUB // 2 else
                    jnp.where(upper, b + turned(b, half, 0), a + turned(a, -half, 0))
                    for a, b in zip(values[:step], values[step:])
                ]
                half //= 2
            packed = jnp.where(lane == g * SUB + row, jnp.sum(values[0], axis=1, keepdims=True), packed)
        value = jnp.sum(packed, axis=0, keepdims=True)
        for n, axes in enumerate(stages):
            size = math.prod(shape[a] for a in axes)
            part[it, n] = value
            recvs[n][it, flat(axes)] = value
            for o in sorted(offsets(axes, shape), key=lambda o: (-abs(o[-1] - 2), o), reverse=True):
                target = {a: lax.rem(me[a] + d, shape[a]) for a, d in zip(axes, o)}
                pltpu.make_async_remote_copy(
                    src_ref=part.at[it, n], dst_ref=recvs[n].at[it, flat(axes)],
                    send_sem=sum_send.at[it, n], recv_sem=sum_recv.at[it, n],
                    device_id=target, device_id_type=MESH).start()
            if n == 0:
                meanwhile()
            whole = recvs[n].at[it, pl.ds(0, size - 1)]
            pltpu.make_async_copy(whole, whole, sum_recv.at[it, n]).wait()
            values = [recvs[n][it, i] for i in range(size)]
            while len(values) > 1:
                values = [sum(values[i + 1 : i + 2], values[i]) for i in range(0, len(values), 2)]
            value = values[0]
        every = jnp.broadcast_to(value, (SUB, LANE))
        for g in range(count):
            one = jnp.sum(jnp.where(lane == g * SUB + row, every, 0.0), axis=1, keepdims=True)
            wide[g] = jnp.broadcast_to(one, (SUB, LANE))

    def solve(weights):
        def read(r):
            return jnp.broadcast_to(wide[r // SUB, r % SUB : r % SUB + 1, :], (SUB, LANE))
        b = [read(j) - (1.0 - viol_ref[j]) * read(SUMS + j) for j in range(FIELDS)]
        m = {}
        at_row = FIELDS
        for i in range(FIELDS):
            for j in range(i, FIELDS):
                m[i, j] = read(at_row)
                at_row += 1
        trace = m[0, 0]
        for i in range(1, FIELDS):
            trace += m[i, i]
        shift = REG * trace / FIELDS
        for i in range(FIELDS):
            m[i, i] += shift
        inverse = []
        for k in range(FIELDS):
            inverse.append(1.0 / m[k, k])
            for i in range(k + 1, FIELDS):
                factor = m[k, i] * inverse[k]
                for j in range(i, FIELDS):
                    m[i, j] -= factor * m[k, j]
                b[i] -= factor * b[k]
        delta = [None] * FIELDS
        for k in reversed(range(FIELDS)):
            v = b[k]
            for j in range(k + 1, FIELDS):
                v -= m[k, j] * delta[j]
            delta[k] = v * inverse[k]
        for k in range(FIELDS):
            lam[k] = jnp.maximum(weights[k] + delta[k], FLOOR * weights[k])

    def newton(it, carry):
        weights = [lam[j] for j in range(FIELDS)]
        if near:
            @pl.when(distant)
            def _():
                main_sums(weights, range(KEPT * tiles), False, False)

            @pl.when(jnp.logical_not(distant))
            def _():
                main_sums(weights, list(range(chunks)) + list(range(lent, pp.shape[1])), False, False)
        else:
            main_sums(weights, range(chunks), False, False)
        exchange(it, -(-SUMS // SUB), lambda: None)
        solve(weights)
        return carry

    inner = []
    for g, fields in enumerate(groups):
        packed = zero
        for j, f in enumerate(fields):
            packed = rows(f, j, packed, core)
        inner.append(packed)
    main_sums(weights, core, True, False)
    if near:
        pl.semaphore_wait(known.at[0], friends)
        tell(1)
    receive(moves_y)
    receive(moves_c)
    extras, bases = face_rows()
    extra_sums(weights, (chunks + 1, chunks + 2), body_rows, bases)
    for g, fields in enumerate(groups):
        receive(xs[g])
        for j, f in enumerate(fields):
            inner[g] = rows(f, j, inner[g], faces)
    receive(moves_z)
    main_sums(weights, faces, True, True)
    within = lane < slots
    bases = [jnp.where(within, v, 0.0) for v in edge_rows(extras)]
    extra_sums(weights, (chunks,), within, bases)
    if near:
        pl.semaphore_wait(known.at[1], friends)
    exchange(0, wide.shape[0], between)
    solve(weights)
    lax.fori_loop(1, ITERS, newton, 0)

    weights = [lam[j] for j in range(FIELDS)]
    for k in range(chunks):
        x, t = divmod(k, tiles)
        out_ref[x, t * SUB : (t + 1) * SUB, :] = respond(k, weights)[0]
    final = zero
    for j in range(FIELDS):
        final = jnp.where(lane == j, weights[j], final)
    lam_out[...] = final

    for copy in lend:
        pl.when(distant)(copy.wait_send)
    for it in range(ITERS):
        for n, axes in enumerate(stages):
            size = math.prod(shape[a] for a in axes)
            whole = recvs[n].at[it, pl.ds(0, size - 1)]
            pltpu.make_async_copy(whole, whole, sum_send.at[it, n]).wait()


def finish(field_ref, lam_ref, field_out, lam_out, row, sem):
    whole = pltpu.make_async_copy(field_ref, field_out, sem.at[0])
    whole.start()
    row[...] = lam_ref[0, :FIELDS]
    short = pltpu.make_async_copy(row, lam_out, sem.at[1])
    short.start()
    whole.wait()
    short.wait()


def shards(shape, density, spread, sensitivities, violation, multipliers_start):
    nx, ny, nz = density.shape
    chunks = nx * ny // SUB
    groups = len(steps())
    stages = plan(shape)
    corners = 9 if shape["gz"] == 2 else 18
    depth = corners // 9
    more = nx - KEPT if compact(shape) else 1
    every = chunks + 3 + (more * ny // SUB if compact(shape) else 0)
    f32 = jnp.float32
    vmem = pl.BlockSpec(memory_space=pltpu.VMEM)
    dma = pltpu.SemaphoreType.DMA
    hbm = pl.BlockSpec(memory_space=pltpu.HBM)
    field, lam = pl.pallas_call(
        functools.partial(body, shape, (nx, ny, nz)),
        out_shape=(
            pltpu.VMEM((nx, ny, nz), f32),
            pltpu.VMEM((SUB, LANE), f32),
        ),
        in_specs=[hbm] * 5,
        out_specs=(vmem, vmem),
        scratch_shapes=[
            pltpu.VMEM((nx, ny, nz), f32),
            pltpu.VMEM((nx, ny, nz), f32),
            pltpu.VMEM((more, ny, nz), f32),
            pltpu.VMEM((more, ny, nz), f32),
            pltpu.SMEM((FIELDS,), f32),
            pltpu.SMEM((FIELDS,), f32),
            pltpu.VMEM((FIELDS, nx, ny + 2 * SUB, nz), f32),
            pltpu.VMEM((2, FIELDS, ny + 2 * SUB, nz), f32),
            pltpu.VMEM((2, FIELDS, nx, nz), f32),
            pltpu.VMEM((2, FIELDS, nx, nz), f32),
            pltpu.VMEM((4, FIELDS, 1, nz), f32),
            pltpu.VMEM((4, FIELDS, 1, nz), f32),
            pltpu.VMEM((2, FIELDS, nx, nz), f32),
            pltpu.VMEM((groups, SUB, LANE), f32),
            pltpu.VMEM((depth, groups, SUB, LANE), f32),
            pltpu.VMEM((2, SUB, LANE), f32),
            pltpu.VMEM((depth, 2, SUB, LANE), f32),
            pltpu.VMEM((2, SUB, LANE), f32),
            pltpu.VMEM((depth, 2, SUB, LANE), f32),
            pltpu.VMEM((depth, 4, SUB, LANE), f32),
            pltpu.VMEM((3, 3, SUB, LANE), f32),
            pltpu.VMEM((FIELDS, chunks, SUB, LANE), f32),
            pltpu.VMEM((chunks, SUB, LANE), f32),
            pltpu.VMEM((FIELDS + 1, every, SUB, LANE), f32),
            pltpu.VMEM((FIELDS + 1, every, SUB, LANE), f32),
            pltpu.VMEM((FIELDS, every, SUB, LANE), f32),
            pltpu.VMEM((FIELDS, every, SUB, LANE), f32),
            pltpu.VMEM((ROWS, SUB, LANE), f32),
            pltpu.VMEM((-(-ROWS // SUB), SUB, LANE), f32),
            pltpu.VMEM((FIELDS, SUB, LANE), f32),
            pltpu.VMEM((ITERS, len(stages), 1, LANE), f32),
        ] + [
            pltpu.VMEM((ITERS, math.prod(shape[a] for a in axes), 1, LANE), f32) for axes in stages
        ] + [
            dma((5,)), dma((6 + 2 * groups,)), dma((6 + 2 * groups,)), dma((corners,)), dma((corners,)), dma((4,)), dma((4,)),
            dma((ITERS, len(stages))), dma((ITERS, len(stages))), pltpu.SemaphoreType.REGULAR((2,)),
        ],
        compiler_params=pltpu.CompilerParams(
            collective_id=0, has_side_effects=True, vmem_limit_bytes=24 << 20),
        name="design_step",
    )(*[pltpu.with_memory_space_constraint(v, pltpu.HBM) for v in (density, spread, sensitivities, violation, multipliers_start)])
    return pl.pallas_call(
        finish,
        out_shape=(
            jax.ShapeDtypeStruct((nx, ny, nz), f32),
            jax.ShapeDtypeStruct((FIELDS,), f32),
        ),
        in_specs=[vmem, vmem],
        out_specs=(hbm, hbm),
        scratch_shapes=[pltpu.VMEM((FIELDS,), f32), dma((2,))],
        compiler_params=pltpu.CompilerParams(vmem_limit_bytes=1 << 20),
        name="finish",
    )(field, lam)


def solution(mesh):
    shape = {a: int(mesh.shape[a]) for a in AXES}
    return jax.shard_map(
        functools.partial(shards, shape),
        mesh=mesh,
        in_specs=(P("gx", "gy", "gz"), P("gx", "gy", "gz"), P(None, "gx", "gy", "gz"), P(), P()),
        out_specs=(P("gx", "gy", "gz"), P()),
        check_vma=False,
    )
```

```python
import functools
import math

import jax
import jax.numpy as jnp
from jax import lax
from jax.experimental import pallas as pl
from jax.experimental.pallas import tpu as pltpu
from jax.sharding import PartitionSpec as P

FIELDS = 9
ITERS = 3

RADIUS = 3.0
RAA = 1e-05
MOVE = 0.9
REG = 0.001
FLOOR = 0.2

W0 = RADIUS
W1 = RADIUS - 1.0
W2 = RADIUS - math.sqrt(2.0)
W3 = RADIUS - math.sqrt(3.0)

SUB, LANE = 8, 128
AXES = ("gz", "gy", "gx")
SUMS = FIELDS + FIELDS * (FIELDS + 1) // 2
ROWS = SUMS + FIELDS
MESH = pl.DeviceIdType.MESH
GROUP = 3
KEPT = 2


def compact(shape):
    return shape["gz"] == 2 and shape["gy"] in (2, 4) and shape["gx"] <= 4


def plan(shape):
    total = math.prod(shape[a] for a in AXES)
    if total <= 32:
        return (AXES,)
    return tuple((a,) for a in AXES)


def offsets(axes, shape):
    out = [()]
    for a in axes:
        out = [o + (d,) for o in out for d in range(shape[a])]
    return [o for o in out if any(o)]


def steps():
    return [range(f, min(f + GROUP, FIELDS)) for f in range(0, FIELDS, GROUP)]


def body(shape, dims, dens_hbm, span_hbm, sens_ref, viol_hbm, lam0_hbm, out_ref, lam_out,
         fields_ref, fields_more, viol_ref, lam0_ref, pad, xpad, ypack, yrecv, cpack, crecv, ymid,
         zpack, zrecv, xzpack, xzrecv, yzpack, yzrecv, czrecv, around, mid, invden, both_pq, slope, scaled,
         acc, wide, lam, part, *rest):
    stages = plan(shape)
    recvs = rest[: len(stages)]
    load_sem, send_sem, recv_sem, zsend_sem, zrecv_sem, lend_send, lend_recv, sum_send, sum_recv, known = rest[len(stages):]
    pp, qq = both_pq.at[0], both_pq.at[1]
    span_ref, dens_ref = fields_ref.at[0], fields_ref.at[1]
    span_more, dens_more = fields_more.at[0], fields_more.at[1]
    nx, ny, nz = dims
    tiles = ny // SUB
    chunks = nx * tiles
    slots = 2 * chunks
    groups = steps()
    count_of = len(groups)
    me = {a: lax.axis_index(a) for a in AXES}

    has = {}
    for a in AXES:
        has[a, -1] = me[a] > 0
        has[a, 0] = jnp.bool_(True)
        has[a, 1] = me[a] < shape[a] - 1

    def both(o):
        moved = [has[a, d] for a, d in zip(AXES, o) if d and not (single and a == "gz")]
        return functools.reduce(jnp.logical_and, moved, jnp.bool_(True))

    single = shape["gz"] == 2
    if single:
        has["gz", 1] = jnp.bool_(True)

    def at(**moves):
        out = {a: me[a] + d for a, d in moves.items()}
        if single and moves.get("gz"):
            out["gz"] = 1 - me["gz"]
        return out

    signs = (-1, 0, 1)
    plane = [(0, dy, dx) for dy in signs for dx in signs if dy or dx]
    ring = [(dz, dy, dx) for dz in ((1, 0) if single else signs) for dy in signs for dx in signs if dz or dy or dx]
    ring.sort(key=lambda o: (-sum(map(abs, o)), o))
    if single:
        has["gz", -1] = has["gz", 1]
    sides = ((0, 1),) if single else ((0, 1), (1, -1))
    barrier = pltpu.get_barrier_semaphore()
    near = compact(shape)
    distant = lax.rem(me["gy"], 2) == 0
    lent = chunks + 3
    if near:
        for o in ring:
            @pl.when(both(o))
            def _(o=o):
                pl.semaphore_signal(barrier, inc=1, device_id=at(gz=o[0], gy=o[1], gx=o[2]),
                                    device_id_type=MESH)
        arrivals = sum(both(o).astype(jnp.int32) for o in ring)
    else:
        partners = set()
        for axes in stages:
            for o in offsets(axes, shape):
                partners.add(tuple(dict(zip(axes, o)).get(a, 0) for a in AXES))
        for d in ring:
            o = tuple(d % shape[a] for a, d in zip(AXES, d))
            if any(o):
                partners.add(o)
        partners = sorted(partners)
        for o in partners:
            target = {a: lax.rem(me[a] + d, shape[a]) for a, d in zip(AXES, o)}
            pl.semaphore_signal(barrier, inc=1, device_id=target, device_id_type=MESH)
        arrivals = len(partners)

    load = pltpu.make_async_copy(
        sens_ref, pad.at[:, :, SUB : SUB + ny, :], load_sem.at[0]
    )
    load.start()
    small = [
        pltpu.make_async_copy(src, dst, load_sem.at[1 + i])
        for i, (src, dst) in enumerate([
            (span_hbm, span_ref), (dens_hbm, dens_ref), (viol_hbm, viol_ref), (lam0_hbm, lam0_ref)])
    ]
    for copy in small:
        copy.start()
    wide_x = 2 * tiles
    lane = lax.broadcasted_iota(jnp.int32, (SUB, LANE), 1)
    row = lax.broadcasted_iota(jnp.int32, (SUB, LANE), 0)
    zero = jnp.zeros((SUB, LANE), jnp.float32)
    slot = lane % slots
    x_of = slot // wide_x
    t_of = (slot % wide_x) // 2
    odd = (lane % 2) == 1
    ends = jnp.logical_or(lane == 0, lane == LANE - 1)

    corners = [(sx, sy) for sx in (1, -1) for sy in (1, -1)]
    line = jnp.zeros((1, LANE), jnp.float32)
    for f in range(FIELDS):
        for x in range(nx):
            pad[f, x, SUB - 1 : SUB, :] = line
            pad[f, x, SUB + ny : SUB + ny + 1, :] = line
        for i in range(2):
            xpad[i, f, SUB - 1 : SUB, :] = line
            xpad[i, f, SUB + ny : SUB + ny + 1, :] = line
    for i, sx in enumerate((1, -1)):
        @pl.when(jnp.logical_not(has["gx", -sx]))
        def _(i=i):
            xpad[i, :, SUB : SUB + ny, :] = jnp.zeros((FIELDS, ny, LANE), jnp.float32)
    for i, sy in enumerate((1, -1)):
        @pl.when(jnp.logical_not(has["gy", -sy]))
        def _(i=i):
            yrecv[i] = jnp.zeros((FIELDS, nx, LANE), jnp.float32)
    for i, (sx, sy) in enumerate(corners):
        @pl.when(jnp.logical_not(jnp.logical_and(has["gx", -sx], has["gy", -sy])))
        def _(i=i):
            crecv[i] = jnp.zeros((FIELDS, 1, LANE), jnp.float32)
    for i, sz in sides:
        if not single:
            @pl.when(jnp.logical_not(has["gz", -sz]))
            def _(i=i):
                zrecv[i] = jnp.zeros(zrecv.shape[1:], jnp.float32)
        for n, sx in enumerate((1, -1)):
            @pl.when(jnp.logical_not(both((-sz, 0, -sx))))
            def _(i=i, n=n):
                xzrecv[i, n] = zero
        for n, sy in enumerate((1, -1)):
            @pl.when(jnp.logical_not(both((-sz, -sy, 0))))
            def _(i=i, n=n):
                yzrecv[i, n] = zero
        for n, (sx, sy) in enumerate(corners):
            @pl.when(jnp.logical_not(both((-sz, -sy, -sx))))
            def _(i=i, n=n):
                czrecv[i, n] = zero

    def count(a, index, extent):
        low = jnp.where(jnp.logical_and(me[a] == 0, index == 0), 0.0, 1.0)
        high = jnp.where(jnp.logical_and(me[a] == shape[a] - 1, index == extent - 1), 0.0, 1.0)
        return low + high
    cz = count("gz", lane, nz)
    for x in range(nx):
        cx = count("gx", jnp.full((SUB, LANE), x, jnp.int32), nx)
        for t in range(tiles):
            cy = count("gy", row + t * SUB, ny)
            den = W0 + W1 * (cx + cy + cz) + W2 * (cx * cy + cy * cz + cx * cz) + W3 * (cx * cy * cz)
            k = x * tiles + t
            invden[k] = 1.0 / den

    load.wait()

    def turned(value, shift, axis=1):
        shift %= value.shape[axis]
        return pltpu.roll(value, shift, axis) if shift else value

    def place(packed, value, k, j):
        here = lane // 2 == k + j * chunks
        return jnp.where(here, turned(value, 2 * k + 1 + j * slots), packed)

    edges = []
    for g, fields in enumerate(groups):
        packed = zero
        for j, f in enumerate(fields):
            for k in range(chunks):
                x, t = divmod(k, tiles)
                packed = place(packed, pad[f, x, SUB + t * SUB : 2 * SUB + t * SUB, :], k, j)
        zpack[g] = packed
        edges.append(packed)
    for n, x in enumerate((nx - 1, 0)):
        packed = zero
        for g in range(count_of):
            packed = jnp.where(x_of == g, turned(edges[g], (g - x) * wide_x), packed)
        xzpack[n] = packed
    for n, y in enumerate((SUB - 1, 0)):
        packed = zero
        for g in range(count_of):
            packed = jnp.where(row == g, jnp.broadcast_to(edges[g][y : y + 1, :], (SUB, LANE)), packed)
        yzpack[n] = packed
    for f in range(FIELDS):
        for i, y in enumerate((SUB + ny - 1, SUB)):
            for x in range(nx):
                ypack[i, f, x : x + 1, :] = pad[f, x, y : y + 1, :]
        for i, (sx, sy) in enumerate(corners):
            x = nx - 1 if sx > 0 else 0
            y = SUB + ny - 1 if sy > 0 else SUB
            cpack[i, f] = pad[f, x, y : y + 1, :]

    pl.semaphore_wait(barrier, arrivals)

    def remote(src, dst, sends, recvs_, index, **moves):
        copy = pltpu.make_async_remote_copy(
            src_ref=src, dst_ref=dst, send_sem=sends.at[index], recv_sem=recvs_.at[index],
            device_id=at(**moves), device_id_type=MESH)
        there = both([moves.get(a, 0) for a in AXES])
        back = both([-moves.get(a, 0) for a in AXES])
        return there, back, copy

    def moves_x(g):
        fields = pl.ds(groups[g][0], len(groups[g]))
        return [
            remote(pad.at[fields, nx - 1 if sx > 0 else 0, SUB : SUB + ny, :],
                   xpad.at[i, fields, SUB : SUB + ny, :], send_sem, recv_sem, 6 + 2 * g + i, gx=sx)
            for i, sx in enumerate((1, -1))
        ]

    moves_c = [remote(cpack.at[i], crecv.at[i], send_sem, recv_sem, 2 + i, gx=sx, gy=sy)
               for i, (sx, sy) in enumerate(corners)]
    moves_y = [remote(ypack.at[i], yrecv.at[i], send_sem, recv_sem, i, gy=sy)
               for i, sy in enumerate((1, -1))]
    moves_z = []
    for i, sz in sides:
        first = 9 * i
        for n, (sx, sy) in enumerate(corners):
            moves_z.append(remote(yzpack.at[n % 2], czrecv.at[i, n], zsend_sem, zrecv_sem, first + 5 + n,
                                  gz=sz, gx=sx, gy=sy))
        for n, sx in enumerate((1, -1)):
            moves_z.append(remote(xzpack.at[n], xzrecv.at[i, n], zsend_sem, zrecv_sem, first + 1 + n,
                                  gz=sz, gx=sx))
        for n, sy in enumerate((1, -1)):
            moves_z.append(remote(yzpack.at[n], yzrecv.at[i, n], zsend_sem, zrecv_sem, first + 3 + n,
                                  gz=sz, gy=sy))
        moves_z.append(remote(zpack, zrecv.at[i], zsend_sem, zrecv_sem, first, gz=sz))

    lend = [
        pltpu.make_async_remote_copy(
            src_ref=src, dst_ref=dst, send_sem=lend_send.at[n], recv_sem=lend_recv.at[n],
            device_id={"gy": me["gy"] + 1 - 2 * lax.rem(me["gy"], 2)}, device_id_type=MESH)
        for n, (src, dst) in enumerate([
            (fields_ref.at[:, pl.ds(KEPT, nx - KEPT)], fields_more),
            (both_pq.at[:, :, pl.ds(KEPT * tiles, chunks - KEPT * tiles)],
             both_pq.at[:, :, pl.ds(lent, chunks - KEPT * tiles)])])
    ] if near else []

    def start(moves):
        for send, _, copy in moves:
            pl.when(send)(copy.start)

    def receive(moves):
        for _, expected, copy in moves:
            pl.when(expected)(copy.wait_recv)

    friends = sum(both(o).astype(jnp.int32) for o in plane)

    def tell(n):
        for o in plane:
            @pl.when(both(o))
            def _(o=o):
                pl.semaphore_signal(known.at[n], inc=1, device_id=at(gy=o[1], gx=o[2]),
                                    device_id_type=MESH)

    xs = [moves_x(g) for g in range(count_of)]
    start(moves_z)
    start(moves_c)
    start(xs[0])
    start(moves_y)
    for g in range(1, count_of):
        start(xs[g])
    if near:
        tell(0)

    def along(s0, s1):
        up = jnp.where(lane == 0, 0.0, pltpu.roll(s1, 1, 1))
        down = jnp.where(lane == LANE - 1, 0.0, pltpu.roll(s1, LANE - 1, 1))
        return s0 + up + down

    for f in range(FIELDS):
        for t in range(tiles):
            y = SUB + t * SUB
            mids, sides = [None], [None]
            for x in range(nx):
                mids.append(pad[f, x, y : y + SUB, :])
                sides.append(pad[f, x, y - 1 : y - 1 + SUB, :] + pad[f, x, y + 1 : y + 1 + SUB, :])
            mids.append(None)
            sides.append(None)
            for x in range(nx):
                next_to = [v for v in (mids[x], mids[x + 2]) if v is not None]
                beyond = [v for v in (sides[x], sides[x + 2]) if v is not None]
                close = sides[x + 1] + sum(next_to[1:], next_to[0])
                far = sum(beyond[1:], beyond[0])
                s0 = W0 * mids[x + 1] + W1 * close + W2 * far
                s1 = W1 * mids[x + 1] + W2 * close + W3 * far
                mid[f, x * tiles + t] = along(s0, s1)

    def piece(ref, k):
        x, t = divmod(k, tiles)
        return ref[x, t * SUB : (t + 1) * SUB, :]

    for copy in small:
        copy.wait()
    for copy in lend[:1]:
        pl.when(distant)(copy.start)
    for n, ref in enumerate((span_ref, dens_ref, invden)):
        packed = zero
        for k in range(chunks):
            value = ref[k] if n == 2 else piece(ref, k)
            for j in range(LANE // slots):
                packed = place(packed, value, k, j)
        around[n, 0] = packed
        for i, y in enumerate((0, ny - 1)):
            for x in range(nx):
                k = x * tiles + y // SUB
                around[n, 1 + i, x : x + 1, :] = (
                    ref[k, y % SUB : y % SUB + 1, :] if n == 2 else ref[x, y : y + 1, :])
    for k in range(FIELDS):
        lam[k] = jnp.full((SUB, LANE), lam0_ref[k], jnp.float32)
    total = zero
    for k in range(chunks):
        s = piece(span_ref, k)
        square = s * s
        pp[FIELDS, k] = square * (1.001 + RAA)
        qq[FIELDS, k] = square * (0.001 + RAA)
        total += s * (1.002 + 2 * RAA)
    acc[ROWS - 1] = total
    weights = [lam[j] for j in range(FIELDS)]

    inside = jnp.logical_not(ends)
    core = range(tiles, chunks - tiles)
    faces = [k for k in range(chunks) if k not in core]

    def keep_of(k):
        keep = inside
        if k in faces:
            return keep
        if k % tiles == 0:
            keep = jnp.logical_and(keep, row != 0)
        if k % tiles == tiles - 1:
            keep = jnp.logical_and(keep, row != SUB - 1)
        return keep

    def grown(r, s):
        gp = jnp.maximum(r, 0.0)
        gm = jnp.maximum(-r, 0.0)
        square = s * s
        p = square * (1.001 * gp + 0.001 * gm + RAA)
        q = square * (0.001 * gp + 1.001 * gm + RAA)
        return p, q, s * (1.002 * (gp + gm) + 2 * RAA)

    def rows(f, j, packed, ks):
        total = zero
        for k in ks:
            x, t = divmod(k, tiles)
            value = mid[f, k]
            for i in range(2):
                if x == (0, nx - 1)[i]:
                    y = SUB + t * SUB
                    h = xpad[i, f, y : y + SUB, :]
                    pair = xpad[i, f, y - 1 : y - 1 + SUB, :] + xpad[i, f, y + 1 : y + 1 + SUB, :]
                    value += along(W1 * h + W2 * pair, W2 * h + W3 * pair)
            packed = place(packed, value, k, j)
            for i, y in enumerate((0, ny - 1)):
                if t == y // SUB:
                    if k in faces:
                        line = jnp.broadcast_to(ymid[i, f, x : x + 1, :], (SUB, LANE))
                        value += jnp.where(row == y % SUB, line, 0.0)
                    else:
                        ymid[i, f, x : x + 1, :] = value[y % SUB : y % SUB + 1, :]
            s = piece(span_ref, k)
            pp[f, k], qq[f, k], base = grown(value * invden[k], s)
            total += jnp.where(keep_of(k), base, 0.0)
        if f:
            acc[SUMS - 1 + f] = total + (zero if ks is core else acc[SUMS - 1 + f])
        return packed

    def respond(k, weights):
        big_p, big_q = pp[0, k], qq[0, k]
        for j in range(FIELDS):
            big_p += weights[j] * pp[j + 1, k]
            big_q += weights[j] * qq[j + 1, k]
        if k >= lent:
            s, d = piece(span_more, k - lent), piece(dens_more, k - lent)
        elif k >= chunks:
            s, d = around[0, k - chunks], around[1, k - chunks]
        else:
            s, d = piece(span_ref, k), piece(dens_ref, k)
        root_p = jnp.sqrt(big_p)
        root_q = jnp.sqrt(big_q)
        lower, upper = d - s, d + s
        moved = (root_p * lower + root_q * upper) / (root_p + root_q)
        low = jnp.maximum(0.0, d - MOVE * s)
        high = jnp.minimum(1.0, d + MOVE * s)
        return jnp.minimum(jnp.maximum(moved, low), high), big_p, big_q, lower, upper

    def terms(k, weights, keep=None):
        moved, big_p, big_q, lower, upper = respond(k, weights)
        ia = 1.0 / (upper - moved)
        ib = 1.0 / (moved - lower)
        ia2, ib2 = ia * ia, ib * ib
        inv = 1.0 / (2.0 * big_p * (ia2 * ia) + 2.0 * big_q * (ib2 * ib))
        if keep is not None:
            ia, ib, ia2, ib2 = [jnp.where(keep, v, 0.0) for v in (ia, ib, ia2, ib2)]
        grads, slopes, ratios = [], [], []
        for j in range(FIELDS):
            p, q = pp[j + 1, k], qq[j + 1, k]
            grads.append(p * ia + q * ib)
            a = p * ia2 - q * ib2
            slopes.append(a)
            ratios.append(a * inv)
        return grads, slopes, ratios

    def main_sums(weights, ks, masked, more):
        grads = [acc[j] if more else zero for j in range(FIELDS)]
        for n, k in enumerate(ks):
            extra, slopes, ratios = terms(k, weights, keep_of(k) if masked else None)
            for j in range(FIELDS):
                grads[j] += extra[j]
                slope[j, n] = slopes[j]
                scaled[j, n] = ratios[j]
        for j in range(FIELDS):
            acc[j] = grads[j]
        at_row = FIELDS
        for group in ((0, 1), (2, 3), (4, 5, 6, 7, 8)):
            keys = [(i, j) for i in group for j in range(i, FIELDS)]
            sums = {key: acc[at_row + n] if more else zero for n, key in enumerate(keys)}
            for n in range(len(ks)):
                right = {j: slope[j, n] for j in range(group[0], FIELDS)}
                for i in group:
                    left = scaled[i, n]
                    for j in range(i, FIELDS):
                        sums[i, j] += left * right[j]
            for key in keys:
                acc[at_row] = sums[key]
                at_row += 1

    def combined(ref, *index):
        last = 0 if single else 1
        low = pltpu.roll(ref[(0,) + index], 1, 1)
        high = pltpu.roll(ref[(last,) + index], LANE - 1, 1)
        if single:
            upper = me["gz"] == 1
            return jnp.where(odd, jnp.where(upper, low, 0.0), jnp.where(upper, 0.0, high))
        return jnp.where(odd, low, high)

    def outer_edges():
        last_x, last_t = wide_x * (nx - 1), 2 * (tiles - 1)
        yz = [combined(yzrecv, n) for n in range(2)]
        xz = [combined(xzrecv, n) for n in range(2)]
        cz_ = [combined(czrecv, n) for n in range(4)]

        def pick(value, g, shift):
            return turned(jnp.broadcast_to(value[g : g + 1, :], (SUB, LANE)), shift)

        def beside(c, first, final):
            down = pltpu.roll(c, 1, 0)
            up = pltpu.roll(c, SUB - 1, 0)
            before = jnp.where(row == 0, jnp.where(t_of == 0, first, turned(down, 2)), down)
            after = jnp.where(row == SUB - 1, jnp.where(t_of == tiles - 1, final, turned(up, LANE - 2)), up)
            return before + after

        out = []
        for g in range(count_of):
            c = combined(zrecv, g)
            s = beside(c, pick(yz[0], g, -last_t), pick(yz[1], g, last_t))
            c_low = turned(xz[0], -wide_x * g)
            c_high = turned(xz[1], last_x - wide_x * g)
            s_low = beside(c_low, pick(cz_[0], g, -last_x - last_t), pick(cz_[1], g, -last_x + last_t))
            s_high = beside(c_high, pick(cz_[2], g, last_x - last_t), pick(cz_[3], g, last_x + last_t))

            def pair(own, low, high):
                return (jnp.where(x_of == 0, low, turned(own, wide_x))
                        + jnp.where(x_of == nx - 1, high, turned(own, -wide_x)))
            out.append(W1 * c + W2 * (s + pair(c, c_low, c_high)) + W3 * pair(s, s_low, s_high))
        return out

    body_rows = jnp.logical_and(inside, jnp.logical_and(row != 0, row != nx - 1))

    def face_rows():
        drops = [[zero, zero] for _ in groups]
        bases = []
        for g, fields in enumerate(groups):
            for j, f in enumerate(fields):
                base = zero
                for i in range(2):
                    h = yrecv[i, f]
                    low = jnp.broadcast_to(crecv[i, f], (SUB, LANE))
                    high = jnp.broadcast_to(crecv[2 + i, f], (SUB, LANE))
                    pair = (jnp.where(row == 0, low, pltpu.roll(h, 1, 0))
                            + jnp.where(row == nx - 1, high, pltpu.roll(h, nx - 1, 0)))
                    extra = along(W1 * h + W2 * pair, W2 * h + W3 * pair)
                    s = around[0, 1 + i]
                    face = jnp.logical_or(row == 0, row == nx - 1)
                    value = jnp.where(face, 0.0, ymid[i, f]) + extra
                    p, q, more = grown(value * around[2, 1 + i], s)
                    pp[f, chunks + 1 + i] = p
                    qq[f, chunks + 1 + i] = q
                    base += jnp.where(body_rows, more, 0.0)
                    ymid[i, f, 0:1, :] = extra[:1]
                    ymid[i, f, nx - 1 : nx, :] = extra[nx - 1 :]
                    here = jnp.logical_and(row == x_of, lane // slots == j)
                    side = jnp.where(odd, jnp.broadcast_to(extra[:, :1], (SUB, LANE)),
                                     jnp.broadcast_to(extra[:, LANE - 1 :], (SUB, LANE)))
                    drops[g][i] = jnp.where(here, side, drops[g][i])
                bases.append(base)
        for i in range(2):
            s = around[0, 1 + i]
            pp[FIELDS, chunks + 1 + i] = s * s * (1.001 + RAA)
            qq[FIELDS, chunks + 1 + i] = s * s * (0.001 + RAA)
        extras = []
        for g in range(count_of):
            value = zero
            for i, y in enumerate((0, ny - 1)):
                full = jnp.broadcast_to(jnp.sum(drops[g][i], axis=0, keepdims=True), (SUB, LANE))
                here = jnp.logical_and(row == y % SUB, t_of == y // SUB)
                value += jnp.where(here, full, 0.0)
            extras.append(value)
        return extras, bases[1:]

    def edge_rows(extras):
        outer = outer_edges()
        s = around[0, 0]
        bases = []
        for g, fields in enumerate(groups):
            p, q, base = grown((inner[g] + extras[g] + outer[g]) * around[2, 0], s)
            for j, f in enumerate(fields):
                pp[f, chunks] = turned(p, -j * slots)
                qq[f, chunks] = turned(q, -j * slots)
                bases.append(turned(base, -j * slots))
        pp[FIELDS, chunks] = s * s * (1.001 + RAA)
        qq[FIELDS, chunks] = s * s * (0.001 + RAA)
        return bases[1:]

    def extra_sums(weights, ks, keep, bases):
        pieces = [terms(k, weights, keep) for k in ks]
        grads = [sum((p[0][j] for p in pieces[1:]), pieces[0][0][j]) for j in range(FIELDS)]
        squares = [sum((p[2][i] * p[1][j] for p in pieces[1:]), pieces[0][2][i] * pieces[0][1][j])
                   for i in range(FIELDS) for j in range(i, FIELDS)]
        for r, value in enumerate(grads + squares + list(bases)):
            acc[r] += value

    def between():
        repair()
        if near:
            for copy in lend[1:]:
                pl.when(distant)(copy.start)
        for moves in [moves_c, moves_y] + xs + [moves_z]:
            for send, _, copy in moves:
                pl.when(send)(copy.wait_send)
        if near:
            @pl.when(jnp.logical_not(distant))
            def _():
                for copy in lend:
                    copy.wait_recv()

    def repair():
        for f in range(FIELDS):
            for ref in (pp, qq):
                edge = ref[f, chunks]
                for k in range(chunks):
                    x, t = divmod(k, tiles)
                    value = ref[f, k]
                    for i, y in enumerate((0, ny - 1)):
                        if t == y // SUB and k in core:
                            line = jnp.broadcast_to(ref[f, chunks + 1 + i, x : x + 1, :], (SUB, LANE))
                            value = jnp.where(row == y % SUB, line, value)
                    ref[f, k] = jnp.where(ends, turned(edge, -2 * k - 1), value)

    def flat(axes):
        index = 0
        for a in axes:
            index = index * shape[a] + me[a]
        return index

    def moved(a, d):
        size = shape[a]
        if size & (size - 1) or d < 1 or d > 3:
            return lax.rem(me[a] + d, size)
        if d == 1:
            return me[a] + 1 - 2 * lax.rem(me[a], 2)
        if d == 2:
            return me[a] + 2 - 4 * lax.rem(me[a] // 2, 2)
        return me[a] + 3 - 2 * lax.rem(me[a], 4)

    targets = []
    for axes in stages:
        to = {(a, d): moved(a, d) if d else me[a] for a in axes for d in range(shape[a])}
        far = sorted(offsets(axes, shape), reverse=True, key=lambda o: (
            sum(d // 2 if a == "gy" else d for a, d in zip(axes, o)), [-d for d in o]))
        targets.append([{a: to[a, d] for a, d in zip(axes, o)} for o in far])

    def exchange(it, count, meanwhile):
        packed = zero
        for g in range(count):
            values = [acc[r] if r < ROWS else zero for r in range(g * SUB, (g + 1) * SUB)]
            half = SUB // 2
            while half:
                upper = (row // half) % 2 == 1
                step = len(values) // 2
                values = [
                    jnp.where(upper, b, a) + pltpu.roll(jnp.where(upper, a, b), half, 0)
                    if half == SUB // 2 else
                    jnp.where(upper, b + turned(b, half, 0), a + turned(a, -half, 0))
                    for a, b in zip(values[:step], values[step:])
                ]
                half //= 2
            packed = jnp.where(lane == g * SUB + row, jnp.sum(values[0], axis=1, keepdims=True), packed)
        value = jnp.sum(packed, axis=0, keepdims=True)
        for n, axes in enumerate(stages):
            size = math.prod(shape[a] for a in axes)
            part[it, n] = value
            recvs[n][it, flat(axes)] = value
            for target in targets[n]:
                pltpu.make_async_remote_copy(
                    src_ref=part.at[it, n], dst_ref=recvs[n].at[it, flat(axes)],
                    send_sem=sum_send.at[n], recv_sem=sum_recv.at[it, n],
                    device_id=target, device_id_type=MESH).start()
            if n == 0:
                meanwhile()
            whole = recvs[n].at[it, pl.ds(0, size - 1)]
            pltpu.make_async_copy(whole, whole, sum_recv.at[it, n]).wait()
            values = [recvs[n][it, i] for i in range(size)]
            while len(values) > 1:
                values = [sum(values[i + 1 : i + 2], values[i]) for i in range(0, len(values), 2)]
            value = values[0]
        every = jnp.broadcast_to(value, (SUB, LANE))
        for g in range(count):
            one = jnp.sum(jnp.where(lane == g * SUB + row, every, 0.0), axis=1, keepdims=True)
            wide[g] = jnp.broadcast_to(one, (SUB, LANE))

    def solve(weights):
        def read(r):
            return jnp.broadcast_to(wide[r // SUB, r % SUB : r % SUB + 1, :], (SUB, LANE))
        b = [read(j) - (1.0 - viol_ref[j]) * read(SUMS + j) for j in range(FIELDS)]
        m = {}
        at_row = FIELDS
        for i in range(FIELDS):
            for j in range(i, FIELDS):
                m[i, j] = read(at_row)
                at_row += 1
        trace = m[0, 0]
        for i in range(1, FIELDS):
            trace += m[i, i]
        shift = REG * trace / FIELDS
        for i in range(FIELDS):
            m[i, i] += shift
        inverse = []
        for k in range(FIELDS):
            inverse.append(1.0 / m[k, k])
            for i in range(k + 1, FIELDS):
                factor = m[k, i] * inverse[k]
                for j in range(i, FIELDS):
                    m[i, j] -= factor * m[k, j]
                b[i] -= factor * b[k]
        delta = [None] * FIELDS
        for k in reversed(range(FIELDS)):
            v = b[k]
            for j in range(k + 1, FIELDS):
                v -= m[k, j] * delta[j]
            delta[k] = v * inverse[k]
        for k in range(FIELDS):
            lam[k] = jnp.maximum(weights[k] + delta[k], FLOOR * weights[k])

    def newton(it, carry):
        weights = [lam[j] for j in range(FIELDS)]
        if near:
            @pl.when(distant)
            def _():
                main_sums(weights, range(KEPT * tiles), False, False)

            @pl.when(jnp.logical_not(distant))
            def _():
                main_sums(weights, list(range(chunks)) + list(range(lent, both_pq.shape[2])), False, False)
        else:
            main_sums(weights, range(chunks), False, False)
        exchange(it, -(-SUMS // SUB), lambda: None)
        solve(weights)
        return carry

    inner = []
    for g, fields in enumerate(groups):
        packed = zero
        for j, f in enumerate(fields):
            packed = rows(f, j, packed, core)
        inner.append(packed)
    main_sums(weights, core, True, False)
    if near:
        pl.semaphore_wait(known.at[0], friends)
        tell(1)
    receive(moves_y)
    receive(moves_c)
    extras, bases = face_rows()
    extra_sums(weights, (chunks + 1, chunks + 2), body_rows, bases)
    for g, fields in enumerate(groups):
        receive(xs[g])
        for j, f in enumerate(fields):
            inner[g] = rows(f, j, inner[g], faces)
    receive(moves_z)
    main_sums(weights, faces, True, True)
    within = lane < slots
    bases = [jnp.where(within, v, 0.0) for v in edge_rows(extras)]
    extra_sums(weights, (chunks,), within, bases)
    if near:
        pl.semaphore_wait(known.at[1], friends)
    exchange(0, wide.shape[0], between)
    solve(weights)
    lax.fori_loop(1, ITERS, newton, 0)

    weights = [lam[j] for j in range(FIELDS)]
    for k in range(chunks):
        x, t = divmod(k, tiles)
        out_ref[x, t * SUB : (t + 1) * SUB, :] = respond(k, weights)[0]
    final = zero
    for j in range(FIELDS):
        final = jnp.where(lane == j, weights[j], final)
    lam_out[...] = final

    if near:
        @pl.when(distant)
        def _():
            for copy in lend:
                copy.wait_send()
    for n, axes in enumerate(stages):
        size = math.prod(shape[a] for a in axes)
        whole = recvs[n].at[:, pl.ds(0, size - 1)]
        pltpu.make_async_copy(whole, whole, sum_send.at[n]).wait()


def finish(field_ref, lam_ref, field_out, lam_out, row, sem):
    whole = pltpu.make_async_copy(field_ref, field_out, sem.at[0])
    whole.start()
    row[...] = lam_ref[0, :FIELDS]
    short = pltpu.make_async_copy(row, lam_out, sem.at[1])
    short.start()
    whole.wait()
    short.wait()


def shards(shape, density, spread, sensitivities, violation, multipliers_start):
    nx, ny, nz = density.shape
    chunks = nx * ny // SUB
    groups = len(steps())
    stages = plan(shape)
    corners = 9 if shape["gz"] == 2 else 18
    depth = corners // 9
    more = nx - KEPT if compact(shape) else 1
    every = chunks + 3 + (more * ny // SUB if compact(shape) else 0)
    f32 = jnp.float32
    vmem = pl.BlockSpec(memory_space=pltpu.VMEM)
    dma = pltpu.SemaphoreType.DMA
    hbm = pl.BlockSpec(memory_space=pltpu.HBM)
    field, lam = pl.pallas_call(
        functools.partial(body, shape, (nx, ny, nz)),
        out_shape=(
            pltpu.VMEM((nx, ny, nz), f32),
            pltpu.VMEM((SUB, LANE), f32),
        ),
        in_specs=[hbm] * 5,
        out_specs=(vmem, vmem),
        scratch_shapes=[
            pltpu.VMEM((2, nx, ny, nz), f32),
            pltpu.VMEM((2, more, ny, nz), f32),
            pltpu.SMEM((FIELDS,), f32),
            pltpu.SMEM((FIELDS,), f32),
            pltpu.VMEM((FIELDS, nx, ny + 2 * SUB, nz), f32),
            pltpu.VMEM((2, FIELDS, ny + 2 * SUB, nz), f32),
            pltpu.VMEM((2, FIELDS, nx, nz), f32),
            pltpu.VMEM((2, FIELDS, nx, nz), f32),
            pltpu.VMEM((4, FIELDS, 1, nz), f32),
            pltpu.VMEM((4, FIELDS, 1, nz), f32),
            pltpu.VMEM((2, FIELDS, nx, nz), f32),
            pltpu.VMEM((groups, SUB, LANE), f32),
            pltpu.VMEM((depth, groups, SUB, LANE), f32),
            pltpu.VMEM((2, SUB, LANE), f32),
            pltpu.VMEM((depth, 2, SUB, LANE), f32),
            pltpu.VMEM((2, SUB, LANE), f32),
            pltpu.VMEM((depth, 2, SUB, LANE), f32),
            pltpu.VMEM((depth, 4, SUB, LANE), f32),
            pltpu.VMEM((3, 3, SUB, LANE), f32),
            pltpu.VMEM((FIELDS, chunks, SUB, LANE), f32),
            pltpu.VMEM((chunks, SUB, LANE), f32),
            pltpu.VMEM((2, FIELDS + 1, every, SUB, LANE), f32),
            pltpu.VMEM((FIELDS, every, SUB, LANE), f32),
            pltpu.VMEM((FIELDS, every, SUB, LANE), f32),
            pltpu.VMEM((ROWS, SUB, LANE), f32),
            pltpu.VMEM((-(-ROWS // SUB), SUB, LANE), f32),
            pltpu.VMEM((FIELDS, SUB, LANE), f32),
            pltpu.VMEM((ITERS, len(stages), 1, LANE), f32),
        ] + [
            pltpu.VMEM((ITERS, math.prod(shape[a] for a in axes), 1, LANE), f32) for axes in stages
        ] + [
            dma((5,)), dma((6 + 2 * groups,)), dma((6 + 2 * groups,)), dma((corners,)), dma((corners,)), dma((2,)), dma((2,)),
            dma((len(stages),)), dma((ITERS, len(stages))), pltpu.SemaphoreType.REGULAR((2,)),
        ],
        compiler_params=pltpu.CompilerParams(
            collective_id=0, has_side_effects=True, vmem_limit_bytes=24 << 20),
        name="design_step",
    )(*[pltpu.with_memory_space_constraint(v, pltpu.HBM) for v in (density, spread, sensitivities, violation, multipliers_start)])
    return pl.pallas_call(
        finish,
        out_shape=(
            jax.ShapeDtypeStruct((nx, ny, nz), f32),
            jax.ShapeDtypeStruct((FIELDS,), f32),
        ),
        in_specs=[vmem, vmem],
        out_specs=(hbm, hbm),
        scratch_shapes=[pltpu.VMEM((FIELDS,), f32), dma((2,))],
        compiler_params=pltpu.CompilerParams(vmem_limit_bytes=1 << 20),
        name="finish",
    )(field, lam)


def solution(mesh):
    shape = {a: int(mesh.shape[a]) for a in AXES}
    return jax.shard_map(
        functools.partial(shards, shape),
        mesh=mesh,
        in_specs=(P("gx", "gy", "gz"), P("gx", "gy", "gz"), P(None, "gx", "gy", "gz"), P(), P()),
        out_specs=(P("gx", "gy", "gz"), P()),
        check_vma=False,
    )
```

```python
import functools
import math

import jax
import jax.numpy as jnp
from jax import lax
from jax.experimental import pallas as pl
from jax.experimental.pallas import tpu as pltpu
from jax.sharding import PartitionSpec as P

FIELDS = 9
ITERS = 3

RADIUS = 3.0
RAA = 1e-05
MOVE = 0.9
REG = 0.001
FLOOR = 0.2

W0 = RADIUS
W1 = RADIUS - 1.0
W2 = RADIUS - math.sqrt(2.0)
W3 = RADIUS - math.sqrt(3.0)

SUB, LANE = 8, 128
AXES = ("gz", "gy", "gx")
SUMS = FIELDS + FIELDS * (FIELDS + 1) // 2
ROWS = SUMS + FIELDS
MESH = pl.DeviceIdType.MESH
GROUP = 3
KEPT = 2


def compact(shape):
    return shape["gz"] == 2 and shape["gy"] in (2, 4) and shape["gx"] <= 4


def plan(shape):
    total = math.prod(shape[a] for a in AXES)
    if total <= 32:
        return (AXES,)
    return tuple((a,) for a in AXES)


def offsets(axes, shape):
    out = [()]
    for a in axes:
        out = [o + (d,) for o in out for d in range(shape[a])]
    return [o for o in out if any(o)]


def steps():
    return [range(f, min(f + GROUP, FIELDS)) for f in range(0, FIELDS, GROUP)]


def body(shape, dims, dens_hbm, span_hbm, sens_ref, viol_hbm, lam0_hbm, out_ref, lam_out,
         fields_ref, fields_more, viol_ref, lam0_ref, pad, xpad, ypack, yrecv, cpack, crecv, ymid,
         zpack, zrecv, xzpack, xzrecv, yzpack, yzrecv, czrecv, around, mid, invden, both_pq, slope, scaled,
         acc, wide, lam, part, *rest):
    stages = plan(shape)
    recvs = rest[: len(stages)]
    load_sem, send_sem, recv_sem, zsend_sem, zrecv_sem, lend_send, lend_recv, sum_send, sum_recv, known = rest[len(stages):]
    pp, qq = both_pq.at[0], both_pq.at[1]
    span_ref, dens_ref = fields_ref.at[0], fields_ref.at[1]
    span_more, dens_more = fields_more.at[0], fields_more.at[1]
    nx, ny, nz = dims
    tiles = ny // SUB
    chunks = nx * tiles
    slots = 2 * chunks
    groups = steps()
    count_of = len(groups)
    loads = []
    for g, fields in enumerate(groups):
        part_of = pl.ds(fields[0], len(fields))
        loads.append(pltpu.make_async_copy(
            sens_ref.at[part_of], pad.at[part_of, :, SUB : SUB + ny, :], load_sem.at[4 + g]))
        loads[g].start()
    me = {a: lax.axis_index(a) for a in AXES}

    has = {}
    for a in AXES:
        has[a, -1] = me[a] > 0
        has[a, 0] = jnp.bool_(True)
        has[a, 1] = me[a] < shape[a] - 1

    def both(o):
        moved = [has[a, d] for a, d in zip(AXES, o) if d and not (single and a == "gz")]
        return functools.reduce(jnp.logical_and, moved, jnp.bool_(True))

    single = shape["gz"] == 2
    if single:
        has["gz", 1] = jnp.bool_(True)

    def at(**moves):
        out = {a: me[a] + d for a, d in moves.items()}
        if single and moves.get("gz"):
            out["gz"] = 1 - me["gz"]
        return out

    signs = (-1, 0, 1)
    plane = [(0, dy, dx) for dy in signs for dx in signs if dy or dx]
    ring = [(dz, dy, dx) for dz in ((1, 0) if single else signs) for dy in signs for dx in signs if dz or dy or dx]
    ring.sort(key=lambda o: (-sum(map(abs, o)), o))
    if single:
        has["gz", -1] = has["gz", 1]
    sides = ((0, 1),) if single else ((0, 1), (1, -1))
    barrier = pltpu.get_barrier_semaphore()
    near = compact(shape)
    distant = lax.rem(me["gy"], 2) == 0
    lent = chunks + 3
    if near:
        for o in ring:
            @pl.when(both(o))
            def _(o=o):
                pl.semaphore_signal(barrier, inc=1, device_id=at(gz=o[0], gy=o[1], gx=o[2]),
                                    device_id_type=MESH)
        arrivals = sum(both(o).astype(jnp.int32) for o in ring)
    else:
        partners = set()
        for axes in stages:
            for o in offsets(axes, shape):
                partners.add(tuple(dict(zip(axes, o)).get(a, 0) for a in AXES))
        for d in ring:
            o = tuple(d % shape[a] for a, d in zip(AXES, d))
            if any(o):
                partners.add(o)
        partners = sorted(partners)
        for o in partners:
            target = {a: lax.rem(me[a] + d, shape[a]) for a, d in zip(AXES, o)}
            pl.semaphore_signal(barrier, inc=1, device_id=target, device_id_type=MESH)
        arrivals = len(partners)

    small = [
        pltpu.make_async_copy(src, dst, load_sem.at[i])
        for i, (src, dst) in enumerate([
            (span_hbm, span_ref), (dens_hbm, dens_ref), (viol_hbm, viol_ref), (lam0_hbm, lam0_ref)])
    ]
    for copy in small:
        copy.start()
    wide_x = 2 * tiles
    lane = lax.broadcasted_iota(jnp.int32, (SUB, LANE), 1)
    row = lax.broadcasted_iota(jnp.int32, (SUB, LANE), 0)
    zero = jnp.zeros((SUB, LANE), jnp.float32)
    slot = lane % slots
    x_of = slot // wide_x
    t_of = (slot % wide_x) // 2
    odd = (lane % 2) == 1
    ends = jnp.logical_or(lane == 0, lane == LANE - 1)

    corners = [(sx, sy) for sx in (1, -1) for sy in (1, -1)]
    line = jnp.zeros((1, LANE), jnp.float32)
    for f in range(FIELDS):
        for x in range(nx):
            pad[f, x, SUB - 1 : SUB, :] = line
            pad[f, x, SUB + ny : SUB + ny + 1, :] = line
        for i in range(2):
            xpad[i, f, SUB - 1 : SUB, :] = line
            xpad[i, f, SUB + ny : SUB + ny + 1, :] = line
    for i, sx in enumerate((1, -1)):
        @pl.when(jnp.logical_not(has["gx", -sx]))
        def _(i=i):
            xpad[i, :, SUB : SUB + ny, :] = jnp.zeros((FIELDS, ny, LANE), jnp.float32)
    for i, sy in enumerate((1, -1)):
        @pl.when(jnp.logical_not(has["gy", -sy]))
        def _(i=i):
            yrecv[i] = jnp.zeros((FIELDS, nx, LANE), jnp.float32)
    for i, (sx, sy) in enumerate(corners):
        @pl.when(jnp.logical_not(jnp.logical_and(has["gx", -sx], has["gy", -sy])))
        def _(i=i):
            crecv[i] = jnp.zeros((FIELDS, 1, LANE), jnp.float32)
    for i, sz in sides:
        if not single:
            @pl.when(jnp.logical_not(has["gz", -sz]))
            def _(i=i):
                zrecv[i] = jnp.zeros(zrecv.shape[1:], jnp.float32)
        for n, sx in enumerate((1, -1)):
            @pl.when(jnp.logical_not(both((-sz, 0, -sx))))
            def _(i=i, n=n):
                xzrecv[i, n] = zero
        for n, sy in enumerate((1, -1)):
            @pl.when(jnp.logical_not(both((-sz, -sy, 0))))
            def _(i=i, n=n):
                yzrecv[i, n] = zero
        for n, (sx, sy) in enumerate(corners):
            @pl.when(jnp.logical_not(both((-sz, -sy, -sx))))
            def _(i=i, n=n):
                czrecv[i, n] = zero

    def count(a, index, extent):
        low = jnp.where(jnp.logical_and(me[a] == 0, index == 0), 0.0, 1.0)
        high = jnp.where(jnp.logical_and(me[a] == shape[a] - 1, index == extent - 1), 0.0, 1.0)
        return low + high
    cz = count("gz", lane, nz)
    for x in range(nx):
        cx = count("gx", jnp.full((SUB, LANE), x, jnp.int32), nx)
        for t in range(tiles):
            cy = count("gy", row + t * SUB, ny)
            den = W0 + W1 * (cx + cy + cz) + W2 * (cx * cy + cy * cz + cx * cz) + W3 * (cx * cy * cz)
            k = x * tiles + t
            invden[k] = 1.0 / den


    def turned(value, shift, axis=1):
        shift %= value.shape[axis]
        return pltpu.roll(value, shift, axis) if shift else value

    def place(packed, value, k, j):
        here = lane // 2 == k + j * chunks
        return jnp.where(here, turned(value, 2 * k + 1 + j * slots), packed)

    lines = pad.reshape(FIELDS, nx * (ny + 2 * SUB), nz)
    edges = []
    for g, fields in enumerate(groups):
        loads[g].wait()
        packed = zero
        for j, f in enumerate(fields):
            for i, y in enumerate((SUB + ny - 1, SUB)):
                ypack[i, f] = lines[f, pl.ds(y, nx, stride=ny + 2 * SUB), :]
            for i, (sx, sy) in enumerate(corners):
                x = nx - 1 if sx > 0 else 0
                y = SUB + ny - 1 if sy > 0 else SUB
                cpack[i, f] = pad[f, x, y : y + 1, :]
            for k in range(chunks):
                x, t = divmod(k, tiles)
                packed = place(packed, pad[f, x, SUB + t * SUB : 2 * SUB + t * SUB, :], k, j)
        zpack[g] = packed
        edges.append(packed)
    for n, x in enumerate((nx - 1, 0)):
        packed = zero
        for g in range(count_of):
            packed = jnp.where(x_of == g, turned(edges[g], (g - x) * wide_x), packed)
        xzpack[n] = packed
    for n, y in enumerate((SUB - 1, 0)):
        packed = zero
        for g in range(count_of):
            packed = jnp.where(row == g, jnp.broadcast_to(edges[g][y : y + 1, :], (SUB, LANE)), packed)
        yzpack[n] = packed
    pl.semaphore_wait(barrier, arrivals)

    def remote(src, dst, sends, recvs_, index, **moves):
        copy = pltpu.make_async_remote_copy(
            src_ref=src, dst_ref=dst, send_sem=sends.at[index], recv_sem=recvs_.at[index],
            device_id=at(**moves), device_id_type=MESH)
        there = both([moves.get(a, 0) for a in AXES])
        back = both([-moves.get(a, 0) for a in AXES])
        return there, back, copy

    def moves_x(g):
        fields = pl.ds(groups[g][0], len(groups[g]))
        return [
            remote(pad.at[fields, nx - 1 if sx > 0 else 0, SUB : SUB + ny, :],
                   xpad.at[i, fields, SUB : SUB + ny, :], send_sem, recv_sem, 6 + 2 * g + i, gx=sx)
            for i, sx in enumerate((1, -1))
        ]

    moves_c = [remote(cpack.at[i], crecv.at[i], send_sem, recv_sem, 2 + i, gx=sx, gy=sy)
               for i, (sx, sy) in enumerate(corners)]
    moves_y = [remote(ypack.at[i], yrecv.at[i], send_sem, recv_sem, i, gy=sy)
               for i, sy in enumerate((1, -1))]
    moves_z = []
    for i, sz in sides:
        first = 9 * i
        for n, (sx, sy) in enumerate(corners):
            moves_z.append(remote(yzpack.at[n % 2], czrecv.at[i, n], zsend_sem, zrecv_sem, first + 5 + n,
                                  gz=sz, gx=sx, gy=sy))
        for n, sx in enumerate((1, -1)):
            moves_z.append(remote(xzpack.at[n], xzrecv.at[i, n], zsend_sem, zrecv_sem, first + 1 + n,
                                  gz=sz, gx=sx))
        for n, sy in enumerate((1, -1)):
            moves_z.append(remote(yzpack.at[n], yzrecv.at[i, n], zsend_sem, zrecv_sem, first + 3 + n,
                                  gz=sz, gy=sy))
        moves_z.append(remote(zpack, zrecv.at[i], zsend_sem, zrecv_sem, first, gz=sz))

    lend = [
        pltpu.make_async_remote_copy(
            src_ref=src, dst_ref=dst, send_sem=lend_send.at[n], recv_sem=lend_recv.at[n],
            device_id={"gy": me["gy"] + 1 - 2 * lax.rem(me["gy"], 2)}, device_id_type=MESH)
        for n, (src, dst) in enumerate([
            (fields_ref.at[:, pl.ds(KEPT, nx - KEPT)], fields_more),
            (both_pq.at[:, pl.ds(0, FIELDS), pl.ds(KEPT * tiles, chunks - KEPT * tiles)],
             both_pq.at[:, pl.ds(0, FIELDS), pl.ds(lent, chunks - KEPT * tiles)])])
    ] if near else []

    def start(moves):
        for send, _, copy in moves:
            pl.when(send)(copy.start)

    def receive(moves):
        for _, expected, copy in moves:
            pl.when(expected)(copy.wait_recv)

    friends = sum(both(o).astype(jnp.int32) for o in plane)

    def tell(n):
        for o in plane:
            @pl.when(both(o))
            def _(o=o):
                pl.semaphore_signal(known.at[n], inc=1, device_id=at(gy=o[1], gx=o[2]),
                                    device_id_type=MESH)

    xs = [moves_x(g) for g in range(count_of)]
    start(moves_z)
    start(moves_c)
    start(xs[0])
    start(moves_y)
    for g in range(1, count_of):
        start(xs[g])
    if near:
        tell(0)

    def along(s0, s1):
        up = jnp.where(lane == 0, 0.0, pltpu.roll(s1, 1, 1))
        down = jnp.where(lane == LANE - 1, 0.0, pltpu.roll(s1, LANE - 1, 1))
        return s0 + up + down

    for f in range(FIELDS):
        for t in range(tiles):
            y = SUB + t * SUB
            mids, sides = [None], [None]
            for x in range(nx):
                mids.append(pad[f, x, y : y + SUB, :])
                sides.append(pad[f, x, y - 1 : y - 1 + SUB, :] + pad[f, x, y + 1 : y + 1 + SUB, :])
            mids.append(None)
            sides.append(None)
            for x in range(nx):
                next_to = [v for v in (mids[x], mids[x + 2]) if v is not None]
                beyond = [v for v in (sides[x], sides[x + 2]) if v is not None]
                close = sides[x + 1] + sum(next_to[1:], next_to[0])
                far = sum(beyond[1:], beyond[0])
                s0 = W0 * mids[x + 1] + W1 * close + W2 * far
                s1 = W1 * mids[x + 1] + W2 * close + W3 * far
                mid[f, x * tiles + t] = along(s0, s1)

    def piece(ref, k):
        x, t = divmod(k, tiles)
        return ref[x, t * SUB : (t + 1) * SUB, :]

    for copy in small:
        copy.wait()
    for copy in lend[:1]:
        pl.when(distant)(copy.start)
    for n, ref in enumerate((span_ref, dens_ref, invden)):
        packed = zero
        for k in range(chunks):
            value = ref[k] if n == 2 else piece(ref, k)
            for j in range(LANE // slots):
                packed = place(packed, value, k, j)
        around[n, 0] = packed
        for i, y in enumerate((0, ny - 1)):
            for x in range(nx):
                k = x * tiles + y // SUB
                around[n, 1 + i, x : x + 1, :] = (
                    ref[k, y % SUB : y % SUB + 1, :] if n == 2 else ref[x, y : y + 1, :])
    for k in range(FIELDS):
        lam[k] = jnp.full((SUB, LANE), lam0_ref[k], jnp.float32)
    total = zero
    for k in range(chunks):
        s = piece(span_ref, k)
        square = s * s
        pp[FIELDS, k] = square * (1.001 + RAA)
        qq[FIELDS, k] = square * (0.001 + RAA)
        total += s * (1.002 + 2 * RAA)
    acc[ROWS - 1] = total
    weights = [lam[j] for j in range(FIELDS)]

    inside = jnp.logical_not(ends)
    core = range(tiles, chunks - tiles)
    faces = [k for k in range(chunks) if k not in core]

    def keep_of(k):
        keep = inside
        if k in faces:
            return keep
        if k % tiles == 0:
            keep = jnp.logical_and(keep, row != 0)
        if k % tiles == tiles - 1:
            keep = jnp.logical_and(keep, row != SUB - 1)
        return keep

    def grown(r, s):
        gp = jnp.maximum(r, 0.0)
        gm = jnp.maximum(-r, 0.0)
        square = s * s
        p = square * (1.001 * gp + 0.001 * gm + RAA)
        q = square * (0.001 * gp + 1.001 * gm + RAA)
        return p, q, s * (1.002 * (gp + gm) + 2 * RAA)

    def rows(f, j, packed, ks):
        total = zero
        for k in ks:
            x, t = divmod(k, tiles)
            value = mid[f, k]
            for i in range(2):
                if x == (0, nx - 1)[i]:
                    y = SUB + t * SUB
                    h = xpad[i, f, y : y + SUB, :]
                    pair = xpad[i, f, y - 1 : y - 1 + SUB, :] + xpad[i, f, y + 1 : y + 1 + SUB, :]
                    value += along(W1 * h + W2 * pair, W2 * h + W3 * pair)
            packed = place(packed, value, k, j)
            for i, y in enumerate((0, ny - 1)):
                if t == y // SUB:
                    if k in faces:
                        line = jnp.broadcast_to(ymid[i, f, x : x + 1, :], (SUB, LANE))
                        value += jnp.where(row == y % SUB, line, 0.0)
                    else:
                        ymid[i, f, x : x + 1, :] = value[y % SUB : y % SUB + 1, :]
            s = piece(span_ref, k)
            pp[f, k], qq[f, k], base = grown(value * invden[k], s)
            total += jnp.where(keep_of(k), base, 0.0)
        if f:
            acc[SUMS - 1 + f] = total + (zero if ks is core else acc[SUMS - 1 + f])
        return packed

    def respond(k, weights):
        big_p, big_q = pp[0, k], qq[0, k]
        for j in range(FIELDS):
            big_p += weights[j] * pp[j + 1, k]
            big_q += weights[j] * qq[j + 1, k]
        if k >= lent:
            s, d = piece(span_more, k - lent), piece(dens_more, k - lent)
        elif k >= chunks:
            s, d = around[0, k - chunks], around[1, k - chunks]
        else:
            s, d = piece(span_ref, k), piece(dens_ref, k)
        root_p = jnp.sqrt(big_p)
        root_q = jnp.sqrt(big_q)
        lower, upper = d - s, d + s
        moved = (root_p * lower + root_q * upper) / (root_p + root_q)
        low = jnp.maximum(0.0, d - MOVE * s)
        high = jnp.minimum(1.0, d + MOVE * s)
        return jnp.minimum(jnp.maximum(moved, low), high), big_p, big_q, lower, upper

    def terms(k, weights, keep=None):
        moved, big_p, big_q, lower, upper = respond(k, weights)
        ia = 1.0 / (upper - moved)
        ib = 1.0 / (moved - lower)
        ia2, ib2 = ia * ia, ib * ib
        inv = 1.0 / (2.0 * big_p * (ia2 * ia) + 2.0 * big_q * (ib2 * ib))
        if keep is not None:
            ia, ib, ia2, ib2 = [jnp.where(keep, v, 0.0) for v in (ia, ib, ia2, ib2)]
        grads, slopes, ratios = [], [], []
        for j in range(FIELDS):
            p, q = pp[j + 1, k], qq[j + 1, k]
            grads.append(p * ia + q * ib)
            a = p * ia2 - q * ib2
            slopes.append(a)
            ratios.append(a * inv)
        return grads, slopes, ratios

    def main_sums(weights, ks, masked, more):
        grads = [acc[j] if more else zero for j in range(FIELDS)]
        for n, k in enumerate(ks):
            extra, slopes, ratios = terms(k, weights, keep_of(k) if masked else None)
            for j in range(FIELDS):
                grads[j] += extra[j]
                slope[j, n] = slopes[j]
                scaled[j, n] = ratios[j]
        for j in range(FIELDS):
            acc[j] = grads[j]
        at_row = FIELDS
        for group in ((0, 1), (2, 3), (4, 5, 6, 7, 8)):
            keys = [(i, j) for i in group for j in range(i, FIELDS)]
            sums = {key: acc[at_row + n] if more else zero for n, key in enumerate(keys)}
            for n in range(len(ks)):
                right = {j: slope[j, n] for j in range(group[0], FIELDS)}
                for i in group:
                    left = scaled[i, n]
                    for j in range(i, FIELDS):
                        sums[i, j] += left * right[j]
            for key in keys:
                acc[at_row] = sums[key]
                at_row += 1

    def combined(ref, *index):
        last = 0 if single else 1
        low = pltpu.roll(ref[(0,) + index], 1, 1)
        high = pltpu.roll(ref[(last,) + index], LANE - 1, 1)
        if single:
            upper = me["gz"] == 1
            return jnp.where(odd, jnp.where(upper, low, 0.0), jnp.where(upper, 0.0, high))
        return jnp.where(odd, low, high)

    def outer_edges():
        last_x, last_t = wide_x * (nx - 1), 2 * (tiles - 1)
        yz = [combined(yzrecv, n) for n in range(2)]
        xz = [combined(xzrecv, n) for n in range(2)]
        cz_ = [combined(czrecv, n) for n in range(4)]

        def pick(value, g, shift):
            return turned(jnp.broadcast_to(value[g : g + 1, :], (SUB, LANE)), shift)

        def beside(c, first, final):
            down = pltpu.roll(c, 1, 0)
            up = pltpu.roll(c, SUB - 1, 0)
            before = jnp.where(row == 0, jnp.where(t_of == 0, first, turned(down, 2)), down)
            after = jnp.where(row == SUB - 1, jnp.where(t_of == tiles - 1, final, turned(up, LANE - 2)), up)
            return before + after

        out = []
        for g in range(count_of):
            c = combined(zrecv, g)
            s = beside(c, pick(yz[0], g, -last_t), pick(yz[1], g, last_t))
            c_low = turned(xz[0], -wide_x * g)
            c_high = turned(xz[1], last_x - wide_x * g)
            s_low = beside(c_low, pick(cz_[0], g, -last_x - last_t), pick(cz_[1], g, -last_x + last_t))
            s_high = beside(c_high, pick(cz_[2], g, last_x - last_t), pick(cz_[3], g, last_x + last_t))

            def pair(own, low, high):
                return (jnp.where(x_of == 0, low, turned(own, wide_x))
                        + jnp.where(x_of == nx - 1, high, turned(own, -wide_x)))
            out.append(W1 * c + W2 * (s + pair(c, c_low, c_high)) + W3 * pair(s, s_low, s_high))
        return out

    body_rows = jnp.logical_and(inside, jnp.logical_and(row != 0, row != nx - 1))

    def face_rows():
        drops = [[zero, zero] for _ in groups]
        bases = []
        for g, fields in enumerate(groups):
            for j, f in enumerate(fields):
                base = zero
                for i in range(2):
                    h = yrecv[i, f]
                    low = jnp.broadcast_to(crecv[i, f], (SUB, LANE))
                    high = jnp.broadcast_to(crecv[2 + i, f], (SUB, LANE))
                    pair = (jnp.where(row == 0, low, pltpu.roll(h, 1, 0))
                            + jnp.where(row == nx - 1, high, pltpu.roll(h, nx - 1, 0)))
                    extra = along(W1 * h + W2 * pair, W2 * h + W3 * pair)
                    s = around[0, 1 + i]
                    face = jnp.logical_or(row == 0, row == nx - 1)
                    value = jnp.where(face, 0.0, ymid[i, f]) + extra
                    p, q, more = grown(value * around[2, 1 + i], s)
                    pp[f, chunks + 1 + i] = p
                    qq[f, chunks + 1 + i] = q
                    base += jnp.where(body_rows, more, 0.0)
                    ymid[i, f, 0:1, :] = extra[:1]
                    ymid[i, f, nx - 1 : nx, :] = extra[nx - 1 :]
                    here = jnp.logical_and(row == x_of, lane // slots == j)
                    side = jnp.where(odd, jnp.broadcast_to(extra[:, :1], (SUB, LANE)),
                                     jnp.broadcast_to(extra[:, LANE - 1 :], (SUB, LANE)))
                    drops[g][i] = jnp.where(here, side, drops[g][i])
                bases.append(base)
        for i in range(2):
            s = around[0, 1 + i]
            pp[FIELDS, chunks + 1 + i] = s * s * (1.001 + RAA)
            qq[FIELDS, chunks + 1 + i] = s * s * (0.001 + RAA)
        extras = []
        for g in range(count_of):
            value = zero
            for i, y in enumerate((0, ny - 1)):
                full = jnp.broadcast_to(jnp.sum(drops[g][i], axis=0, keepdims=True), (SUB, LANE))
                here = jnp.logical_and(row == y % SUB, t_of == y // SUB)
                value += jnp.where(here, full, 0.0)
            extras.append(value)
        return extras, bases[1:]

    def edge_rows(extras):
        outer = outer_edges()
        s = around[0, 0]
        bases = []
        for g, fields in enumerate(groups):
            p, q, base = grown((inner[g] + extras[g] + outer[g]) * around[2, 0], s)
            for j, f in enumerate(fields):
                pp[f, chunks] = turned(p, -j * slots)
                qq[f, chunks] = turned(q, -j * slots)
                bases.append(turned(base, -j * slots))
        pp[FIELDS, chunks] = s * s * (1.001 + RAA)
        qq[FIELDS, chunks] = s * s * (0.001 + RAA)
        return bases[1:]

    def extra_sums(weights, ks, keep, bases):
        pieces = [terms(k, weights, keep) for k in ks]
        grads = [sum((p[0][j] for p in pieces[1:]), pieces[0][0][j]) for j in range(FIELDS)]
        squares = [sum((p[2][i] * p[1][j] for p in pieces[1:]), pieces[0][2][i] * pieces[0][1][j])
                   for i in range(FIELDS) for j in range(i, FIELDS)]
        for r, value in enumerate(grads + squares + list(bases)):
            acc[r] += value

    def between():
        for fields in groups:
            for f in fields:
                repair(f, range(KEPT * tiles, chunks))
            if near:
                of, at_k = pl.ds(fields[0], len(fields)), pl.ds(KEPT * tiles, chunks - KEPT * tiles)
                pl.when(distant)(pltpu.make_async_remote_copy(
                    src_ref=both_pq.at[:, of, at_k],
                    dst_ref=both_pq.at[:, of, pl.ds(lent, chunks - KEPT * tiles)],
                    send_sem=lend_send.at[1], recv_sem=lend_recv.at[1],
                    device_id={"gy": me["gy"] + 1 - 2 * lax.rem(me["gy"], 2)}, device_id_type=MESH).start)
        for f in range(FIELDS):
            repair(f, range(KEPT * tiles))
        for moves in [moves_c, moves_y] + xs + [moves_z]:
            for send, _, copy in moves:
                pl.when(send)(copy.wait_send)
        if near:
            @pl.when(jnp.logical_not(distant))
            def _():
                lend[0].wait_recv()
                for k in range(lent, both_pq.shape[2]):
                    s = piece(span_more, k - lent)
                    pp[FIELDS, k] = s * s * (1.001 + RAA)
                    qq[FIELDS, k] = s * s * (0.001 + RAA)
                lend[1].wait_recv()

    def repair(f, ks):
        for ref in (pp, qq):
            edge = ref[f, chunks]
            for k in ks:
                x, t = divmod(k, tiles)
                value = ref[f, k]
                for i, y in enumerate((0, ny - 1)):
                    if t == y // SUB and k in core:
                        line = jnp.broadcast_to(ref[f, chunks + 1 + i, x : x + 1, :], (SUB, LANE))
                        value = jnp.where(row == y % SUB, line, value)
                ref[f, k] = jnp.where(ends, turned(edge, -2 * k - 1), value)

    def flat(axes):
        index = 0
        for a in axes:
            index = index * shape[a] + me[a]
        return index

    def moved(a, d):
        size = shape[a]
        if size & (size - 1) or d < 1 or d > 3:
            return lax.rem(me[a] + d, size)
        if d == 1:
            return me[a] + 1 - 2 * lax.rem(me[a], 2)
        if d == 2:
            return me[a] + 2 - 4 * lax.rem(me[a] // 2, 2)
        return me[a] + 3 - 2 * lax.rem(me[a], 4)

    targets = []
    for axes in stages:
        to = {(a, d): moved(a, d) if d else me[a] for a in axes for d in range(shape[a])}
        far = sorted(offsets(axes, shape), reverse=True, key=lambda o: (
            sum(d // 2 if a == "gy" else d for a, d in zip(axes, o)), [-d for d in o]))
        targets.append([{a: to[a, d] for a, d in zip(axes, o)} for o in far])

    def exchange(it, count, meanwhile):
        packed = zero
        for g in range(count):
            values = [acc[r] if r < ROWS else zero for r in range(g * SUB, (g + 1) * SUB)]
            half = SUB // 2
            while half:
                upper = (row // half) % 2 == 1
                step = len(values) // 2
                values = [
                    jnp.where(upper, b, a) + pltpu.roll(jnp.where(upper, a, b), half, 0)
                    if half == SUB // 2 else
                    jnp.where(upper, b + turned(b, half, 0), a + turned(a, -half, 0))
                    for a, b in zip(values[:step], values[step:])
                ]
                half //= 2
            packed = jnp.where(lane == g * SUB + row, jnp.sum(values[0], axis=1, keepdims=True), packed)
        value = jnp.sum(packed, axis=0, keepdims=True)
        for n, axes in enumerate(stages):
            size = math.prod(shape[a] for a in axes)
            part[it, n] = value
            recvs[n][it, flat(axes)] = value
            for target in targets[n]:
                pltpu.make_async_remote_copy(
                    src_ref=part.at[it, n], dst_ref=recvs[n].at[it, flat(axes)],
                    send_sem=sum_send.at[n], recv_sem=sum_recv.at[it, n],
                    device_id=target, device_id_type=MESH).start()
            if n == 0:
                meanwhile()
            whole = recvs[n].at[it, pl.ds(0, size - 1)]
            pltpu.make_async_copy(whole, whole, sum_recv.at[it, n]).wait()
            values = [recvs[n][it, i] for i in range(size)]
            while len(values) > 1:
                values = [sum(values[i + 1 : i + 2], values[i]) for i in range(0, len(values), 2)]
            value = values[0]
        every = jnp.broadcast_to(value, (SUB, LANE))
        for g in range(count):
            one = jnp.sum(jnp.where(lane == g * SUB + row, every, 0.0), axis=1, keepdims=True)
            wide[g] = jnp.broadcast_to(one, (SUB, LANE))

    def solve(weights):
        def read(r):
            return jnp.broadcast_to(wide[r // SUB, r % SUB : r % SUB + 1, :], (SUB, LANE))
        b = [read(j) - (1.0 - viol_ref[j]) * read(SUMS + j) for j in range(FIELDS)]
        m = {}
        at_row = FIELDS
        for i in range(FIELDS):
            for j in range(i, FIELDS):
                m[i, j] = read(at_row)
                at_row += 1
        trace = m[0, 0]
        for i in range(1, FIELDS):
            trace += m[i, i]
        shift = REG * trace / FIELDS
        for i in range(FIELDS):
            m[i, i] += shift
        inverse = []
        for k in range(FIELDS):
            inverse.append(1.0 / m[k, k])
            for i in range(k + 1, FIELDS):
                factor = m[k, i] * inverse[k]
                for j in range(i, FIELDS):
                    m[i, j] -= factor * m[k, j]
                b[i] -= factor * b[k]
        delta = [None] * FIELDS
        for k in reversed(range(FIELDS)):
            v = b[k]
            for j in range(k + 1, FIELDS):
                v -= m[k, j] * delta[j]
            delta[k] = v * inverse[k]
        for k in range(FIELDS):
            lam[k] = jnp.maximum(weights[k] + delta[k], FLOOR * weights[k])

    def newton(it, carry):
        weights = [lam[j] for j in range(FIELDS)]
        if near:
            @pl.when(distant)
            def _():
                main_sums(weights, range(KEPT * tiles), False, False)

            @pl.when(jnp.logical_not(distant))
            def _():
                main_sums(weights, list(range(chunks)) + list(range(lent, both_pq.shape[2])), False, False)
        else:
            main_sums(weights, range(chunks), False, False)
        exchange(it, -(-SUMS // SUB), lambda: None)
        solve(weights)
        return carry

    inner = []
    for g, fields in enumerate(groups):
        packed = zero
        for j, f in enumerate(fields):
            packed = rows(f, j, packed, core)
        inner.append(packed)
    main_sums(weights, core, True, False)
    if near:
        pl.semaphore_wait(known.at[0], friends)
        tell(1)
    receive(moves_y)
    receive(moves_c)
    extras, bases = face_rows()
    extra_sums(weights, (chunks + 1, chunks + 2), body_rows, bases)
    for g, fields in enumerate(groups):
        receive(xs[g])
        for j, f in enumerate(fields):
            inner[g] = rows(f, j, inner[g], faces)
    receive(moves_z)
    main_sums(weights, faces, True, True)
    within = lane < slots
    bases = [jnp.where(within, v, 0.0) for v in edge_rows(extras)]
    extra_sums(weights, (chunks,), within, bases)
    if near:
        pl.semaphore_wait(known.at[1], friends)
    exchange(0, wide.shape[0], between)
    solve(weights)
    lax.fori_loop(1, ITERS, newton, 0)

    weights = [lam[j] for j in range(FIELDS)]
    for k in range(chunks):
        x, t = divmod(k, tiles)
        out_ref[x, t * SUB : (t + 1) * SUB, :] = respond(k, weights)[0]
    final = zero
    for j in range(FIELDS):
        final = jnp.where(lane == j, weights[j], final)
    lam_out[...] = final

    if near:
        @pl.when(distant)
        def _():
            for copy in lend:
                copy.wait_send()
    for n, axes in enumerate(stages):
        size = math.prod(shape[a] for a in axes)
        whole = recvs[n].at[:, pl.ds(0, size - 1)]
        pltpu.make_async_copy(whole, whole, sum_send.at[n]).wait()


def finish(field_ref, lam_ref, field_out, lam_out, row, sem):
    whole = pltpu.make_async_copy(field_ref, field_out, sem.at[0])
    whole.start()
    row[...] = lam_ref[0, :FIELDS]
    short = pltpu.make_async_copy(row, lam_out, sem.at[1])
    short.start()
    whole.wait()
    short.wait()


def shards(shape, density, spread, sensitivities, violation, multipliers_start):
    nx, ny, nz = density.shape
    chunks = nx * ny // SUB
    groups = len(steps())
    stages = plan(shape)
    corners = 9 if shape["gz"] == 2 else 18
    depth = corners // 9
    more = nx - KEPT if compact(shape) else 1
    every = chunks + 3 + (more * ny // SUB if compact(shape) else 0)
    f32 = jnp.float32
    vmem = pl.BlockSpec(memory_space=pltpu.VMEM)
    dma = pltpu.SemaphoreType.DMA
    hbm = pl.BlockSpec(memory_space=pltpu.HBM)
    field, lam = pl.pallas_call(
        functools.partial(body, shape, (nx, ny, nz)),
        out_shape=(
            pltpu.VMEM((nx, ny, nz), f32),
            pltpu.VMEM((SUB, LANE), f32),
        ),
        in_specs=[hbm] * 5,
        out_specs=(vmem, vmem),
        scratch_shapes=[
            pltpu.VMEM((2, nx, ny, nz), f32),
            pltpu.VMEM((2, more, ny, nz), f32),
            pltpu.SMEM((FIELDS,), f32),
            pltpu.SMEM((FIELDS,), f32),
            pltpu.VMEM((FIELDS, nx, ny + 2 * SUB, nz), f32),
            pltpu.VMEM((2, FIELDS, ny + 2 * SUB, nz), f32),
            pltpu.VMEM((2, FIELDS, nx, nz), f32),
            pltpu.VMEM((2, FIELDS, nx, nz), f32),
            pltpu.VMEM((4, FIELDS, 1, nz), f32),
            pltpu.VMEM((4, FIELDS, 1, nz), f32),
            pltpu.VMEM((2, FIELDS, nx, nz), f32),
            pltpu.VMEM((groups, SUB, LANE), f32),
            pltpu.VMEM((depth, groups, SUB, LANE), f32),
            pltpu.VMEM((2, SUB, LANE), f32),
            pltpu.VMEM((depth, 2, SUB, LANE), f32),
            pltpu.VMEM((2, SUB, LANE), f32),
            pltpu.VMEM((depth, 2, SUB, LANE), f32),
            pltpu.VMEM((depth, 4, SUB, LANE), f32),
            pltpu.VMEM((3, 3, SUB, LANE), f32),
            pltpu.VMEM((FIELDS, chunks, SUB, LANE), f32),
            pltpu.VMEM((chunks, SUB, LANE), f32),
            pltpu.VMEM((2, FIELDS + 1, every, SUB, LANE), f32),
            pltpu.VMEM((FIELDS, every, SUB, LANE), f32),
            pltpu.VMEM((FIELDS, every, SUB, LANE), f32),
            pltpu.VMEM((ROWS, SUB, LANE), f32),
            pltpu.VMEM((-(-ROWS // SUB), SUB, LANE), f32),
            pltpu.VMEM((FIELDS, SUB, LANE), f32),
            pltpu.VMEM((ITERS, len(stages), 1, LANE), f32),
        ] + [
            pltpu.VMEM((ITERS, math.prod(shape[a] for a in axes), 1, LANE), f32) for axes in stages
        ] + [
            dma((4 + groups,)), dma((6 + 2 * groups,)), dma((6 + 2 * groups,)), dma((corners,)), dma((corners,)), dma((2,)), dma((2,)),
            dma((len(stages),)), dma((ITERS, len(stages))), pltpu.SemaphoreType.REGULAR((2,)),
        ],
        compiler_params=pltpu.CompilerParams(
            collective_id=0, has_side_effects=True, vmem_limit_bytes=24 << 20),
        name="design_step",
    )(*[pltpu.with_memory_space_constraint(v, pltpu.HBM) for v in (density, spread, sensitivities, violation, multipliers_start)])
    return pl.pallas_call(
        finish,
        out_shape=(
            jax.ShapeDtypeStruct((nx, ny, nz), f32),
            jax.ShapeDtypeStruct((FIELDS,), f32),
        ),
        in_specs=[vmem, vmem],
        out_specs=(hbm, hbm),
        scratch_shapes=[pltpu.VMEM((FIELDS,), f32), dma((2,))],
        compiler_params=pltpu.CompilerParams(vmem_limit_bytes=1 << 20),
        name="finish",
    )(field, lam)


def solution(mesh):
    shape = {a: int(mesh.shape[a]) for a in AXES}
    return jax.shard_map(
        functools.partial(shards, shape),
        mesh=mesh,
        in_specs=(P("gx", "gy", "gz"), P("gx", "gy", "gz"), P(None, "gx", "gy", "gz"), P(), P()),
        out_specs=(P("gx", "gy", "gz"), P()),
        check_vma=False,
    )
```

```python
import functools
import math

import jax
import jax.numpy as jnp
from jax import lax
from jax.experimental import pallas as pl
from jax.experimental.pallas import tpu as pltpu
from jax.sharding import PartitionSpec as P

FIELDS = 9
ITERS = 3

RADIUS = 3.0
RAA = 1e-05
MOVE = 0.9
REG = 0.001
FLOOR = 0.2

W0 = RADIUS
W1 = RADIUS - 1.0
W2 = RADIUS - math.sqrt(2.0)
W3 = RADIUS - math.sqrt(3.0)

SUB, LANE = 8, 128
AXES = ("gz", "gy", "gx")
SUMS = FIELDS + FIELDS * (FIELDS + 1) // 2
ROWS = SUMS + FIELDS
MESH = pl.DeviceIdType.MESH
GROUP = 3
KEPT = 2


def compact(shape):
    return shape["gz"] == 2 and shape["gy"] in (2, 4) and shape["gx"] <= 4


def plan(shape):
    total = math.prod(shape[a] for a in AXES)
    if total <= 32:
        return (AXES,)
    return tuple((a,) for a in AXES)


def offsets(axes, shape):
    out = [()]
    for a in axes:
        out = [o + (d,) for o in out for d in range(shape[a])]
    return [o for o in out if any(o)]


PARTS = (4, 4, 1)


def steps():
    return [range(f, min(f + GROUP, FIELDS)) for f in range(0, FIELDS, GROUP)]


def body(shape, dims, dens_hbm, span_hbm, sens_ref, viol_hbm, lam0_hbm, out_ref, lam_out,
         fields_ref, fields_more, viol_ref, lam0_ref, pad, xpad, ypack, yrecv, cpack, crecv, ymid,
         zpack, zrecv, xzpack, xzrecv, yzpack, yzrecv, czrecv, around, mid, invden, both_pq, slope, scaled,
         acc, wide, lam, part, *rest):
    stages = plan(shape)
    recvs = rest[: len(stages)]
    load_sem, send_sem, recv_sem, zsend_sem, zrecv_sem, lend_send, lend_recv, sum_send, sum_recv, known = rest[len(stages):]
    pp, qq = both_pq.at[0], both_pq.at[1]
    span_ref, dens_ref = fields_ref.at[0], fields_ref.at[1]
    span_more, dens_more = fields_more.at[0], fields_more.at[1]
    nx, ny, nz = dims
    tiles = ny // SUB
    chunks = nx * tiles
    slots = 2 * chunks
    groups = steps()
    count_of = len(groups)
    loads = []
    for g, fields in enumerate(groups):
        part_of = pl.ds(fields[0], len(fields))
        loads.append(pltpu.make_async_copy(
            sens_ref.at[part_of], pad.at[part_of, :, SUB : SUB + ny, :], load_sem.at[4 + g]))
        loads[g].start()
    me = {a: lax.axis_index(a) for a in AXES}

    has = {}
    for a in AXES:
        has[a, -1] = me[a] > 0
        has[a, 0] = jnp.bool_(True)
        has[a, 1] = me[a] < shape[a] - 1

    def both(o):
        moved = [has[a, d] for a, d in zip(AXES, o) if d and not (single and a == "gz")]
        return functools.reduce(jnp.logical_and, moved, jnp.bool_(True))

    single = shape["gz"] == 2
    if single:
        has["gz", 1] = jnp.bool_(True)

    def at(**moves):
        out = {a: me[a] + d for a, d in moves.items()}
        if single and moves.get("gz"):
            out["gz"] = 1 - me["gz"]
        return out

    signs = (-1, 0, 1)
    plane = [(0, dy, dx) for dy in signs for dx in signs if dy or dx]
    ring = [(dz, dy, dx) for dz in ((1, 0) if single else signs) for dy in signs for dx in signs if dz or dy or dx]
    ring.sort(key=lambda o: (-sum(map(abs, o)), o))
    if single:
        has["gz", -1] = has["gz", 1]
    sides = ((0, 1),) if single else ((0, 1), (1, -1))
    barrier = pltpu.get_barrier_semaphore()
    near = compact(shape)
    distant = lax.rem(me["gy"], 2) == 0
    lent = chunks + 3
    if near:
        for o in ring:
            @pl.when(both(o))
            def _(o=o):
                pl.semaphore_signal(barrier, inc=1, device_id=at(gz=o[0], gy=o[1], gx=o[2]),
                                    device_id_type=MESH)
        arrivals = sum(both(o).astype(jnp.int32) for o in ring)
    else:
        partners = set()
        for axes in stages:
            for o in offsets(axes, shape):
                partners.add(tuple(dict(zip(axes, o)).get(a, 0) for a in AXES))
        for d in ring:
            o = tuple(d % shape[a] for a, d in zip(AXES, d))
            if any(o):
                partners.add(o)
        partners = sorted(partners)
        for o in partners:
            target = {a: lax.rem(me[a] + d, shape[a]) for a, d in zip(AXES, o)}
            pl.semaphore_signal(barrier, inc=1, device_id=target, device_id_type=MESH)
        arrivals = len(partners)

    small = [
        pltpu.make_async_copy(src, dst, load_sem.at[i])
        for i, (src, dst) in enumerate([
            (span_hbm, span_ref), (dens_hbm, dens_ref), (viol_hbm, viol_ref), (lam0_hbm, lam0_ref)])
    ]
    for copy in small:
        copy.start()
    wide_x = 2 * tiles
    lane = lax.broadcasted_iota(jnp.int32, (SUB, LANE), 1)
    row = lax.broadcasted_iota(jnp.int32, (SUB, LANE), 0)
    zero = jnp.zeros((SUB, LANE), jnp.float32)
    slot = lane % slots
    x_of = slot // wide_x
    t_of = (slot % wide_x) // 2
    odd = (lane % 2) == 1
    ends = jnp.logical_or(lane == 0, lane == LANE - 1)

    corners = [(sx, sy) for sx in (1, -1) for sy in (1, -1)]
    line = jnp.zeros((1, LANE), jnp.float32)
    for f in range(FIELDS):
        for x in range(nx):
            pad[f, x, SUB - 1 : SUB, :] = line
            pad[f, x, SUB + ny : SUB + ny + 1, :] = line
        for i in range(2):
            xpad[i, f, SUB - 1 : SUB, :] = line
            xpad[i, f, SUB + ny : SUB + ny + 1, :] = line
    for i, sx in enumerate((1, -1)):
        @pl.when(jnp.logical_not(has["gx", -sx]))
        def _(i=i):
            xpad[i, :, SUB : SUB + ny, :] = jnp.zeros((FIELDS, ny, LANE), jnp.float32)
    for i, sy in enumerate((1, -1)):
        @pl.when(jnp.logical_not(has["gy", -sy]))
        def _(i=i):
            yrecv[i] = jnp.zeros((FIELDS, nx, LANE), jnp.float32)
    for i, (sx, sy) in enumerate(corners):
        @pl.when(jnp.logical_not(jnp.logical_and(has["gx", -sx], has["gy", -sy])))
        def _(i=i):
            crecv[i] = jnp.zeros((FIELDS, 1, LANE), jnp.float32)
    for i, sz in sides:
        if not single:
            @pl.when(jnp.logical_not(has["gz", -sz]))
            def _(i=i):
                zrecv[i] = jnp.zeros(zrecv.shape[1:], jnp.float32)
        for n, sx in enumerate((1, -1)):
            @pl.when(jnp.logical_not(both((-sz, 0, -sx))))
            def _(i=i, n=n):
                xzrecv[i, n] = zero
        for n, sy in enumerate((1, -1)):
            @pl.when(jnp.logical_not(both((-sz, -sy, 0))))
            def _(i=i, n=n):
                yzrecv[i, n] = zero
        for n, (sx, sy) in enumerate(corners):
            @pl.when(jnp.logical_not(both((-sz, -sy, -sx))))
            def _(i=i, n=n):
                czrecv[i, n] = zero

    def count(a, index, extent):
        low = jnp.where(jnp.logical_and(me[a] == 0, index == 0), 0.0, 1.0)
        high = jnp.where(jnp.logical_and(me[a] == shape[a] - 1, index == extent - 1), 0.0, 1.0)
        return low + high
    cz = count("gz", lane, nz)
    for x in range(nx):
        cx = count("gx", jnp.full((SUB, LANE), x, jnp.int32), nx)
        for t in range(tiles):
            cy = count("gy", row + t * SUB, ny)
            den = W0 + W1 * (cx + cy + cz) + W2 * (cx * cy + cy * cz + cx * cz) + W3 * (cx * cy * cz)
            k = x * tiles + t
            invden[k] = 1.0 / den


    def turned(value, shift, axis=1):
        shift %= value.shape[axis]
        return pltpu.roll(value, shift, axis) if shift else value

    def place(packed, value, k, j):
        here = lane // 2 == k + j * chunks
        return jnp.where(here, turned(value, 2 * k + 1 + j * slots), packed)

    lines = pad.reshape(FIELDS, nx * (ny + 2 * SUB), nz)
    edges = []
    for g, fields in enumerate(groups):
        loads[g].wait()
        packed = zero
        for j, f in enumerate(fields):
            for i, y in enumerate((SUB + ny - 1, SUB)):
                ypack[i, f] = lines[f, pl.ds(y, nx, stride=ny + 2 * SUB), :]
            for i, (sx, sy) in enumerate(corners):
                x = nx - 1 if sx > 0 else 0
                y = SUB + ny - 1 if sy > 0 else SUB
                cpack[i, f] = pad[f, x, y : y + 1, :]
            for k in range(chunks):
                x, t = divmod(k, tiles)
                packed = place(packed, pad[f, x, SUB + t * SUB : 2 * SUB + t * SUB, :], k, j)
        zpack[g] = packed
        edges.append(packed)
    for n, x in enumerate((nx - 1, 0)):
        packed = zero
        for g in range(count_of):
            packed = jnp.where(x_of == g, turned(edges[g], (g - x) * wide_x), packed)
        xzpack[n] = packed
    for n, y in enumerate((SUB - 1, 0)):
        packed = zero
        for g in range(count_of):
            packed = jnp.where(row == g, jnp.broadcast_to(edges[g][y : y + 1, :], (SUB, LANE)), packed)
        yzpack[n] = packed
    pl.semaphore_wait(barrier, arrivals)

    def remote(src, dst, sends, recvs_, index, **moves):
        copy = pltpu.make_async_remote_copy(
            src_ref=src, dst_ref=dst, send_sem=sends.at[index], recv_sem=recvs_.at[index],
            device_id=at(**moves), device_id_type=MESH)
        there = both([moves.get(a, 0) for a in AXES])
        back = both([-moves.get(a, 0) for a in AXES])
        return there, back, copy

    starts = [sum(PARTS[:n]) for n in range(len(PARTS))]

    def moves_x(g):
        fields = pl.ds(starts[g], PARTS[g])
        return [
            remote(pad.at[fields, nx - 1 if sx > 0 else 0, SUB : SUB + ny, :],
                   xpad.at[i, fields, SUB : SUB + ny, :], send_sem, recv_sem, 6 + 2 * g + i, gx=sx)
            for i, sx in enumerate((1, -1))
        ]

    moves_c = [remote(cpack.at[i], crecv.at[i], send_sem, recv_sem, 2 + i, gx=sx, gy=sy)
               for i, (sx, sy) in enumerate(corners)]
    moves_y = [remote(ypack.at[i], yrecv.at[i], send_sem, recv_sem, i, gy=sy)
               for i, sy in enumerate((1, -1))]
    moves_z = []
    for i, sz in sides:
        first = 9 * i
        for n, (sx, sy) in enumerate(corners):
            moves_z.append(remote(yzpack.at[n % 2], czrecv.at[i, n], zsend_sem, zrecv_sem, first + 5 + n,
                                  gz=sz, gx=sx, gy=sy))
        for n, sx in enumerate((1, -1)):
            moves_z.append(remote(xzpack.at[n], xzrecv.at[i, n], zsend_sem, zrecv_sem, first + 1 + n,
                                  gz=sz, gx=sx))
        for n, sy in enumerate((1, -1)):
            moves_z.append(remote(yzpack.at[n], yzrecv.at[i, n], zsend_sem, zrecv_sem, first + 3 + n,
                                  gz=sz, gy=sy))
        moves_z.append(remote(zpack, zrecv.at[i], zsend_sem, zrecv_sem, first, gz=sz))

    lend = [
        pltpu.make_async_remote_copy(
            src_ref=src, dst_ref=dst, send_sem=lend_send.at[n], recv_sem=lend_recv.at[n],
            device_id={"gy": me["gy"] + 1 - 2 * lax.rem(me["gy"], 2)}, device_id_type=MESH)
        for n, (src, dst) in enumerate([
            (fields_ref.at[:, pl.ds(KEPT, nx - KEPT)], fields_more),
            (both_pq.at[:, pl.ds(0, FIELDS), pl.ds(KEPT * tiles, chunks - KEPT * tiles)],
             both_pq.at[:, pl.ds(0, FIELDS), pl.ds(lent, chunks - KEPT * tiles)])])
    ] if near else []

    def start(moves):
        for send, _, copy in moves:
            pl.when(send)(copy.start)

    def receive(moves):
        for _, expected, copy in moves:
            pl.when(expected)(copy.wait_recv)

    friends = sum(both(o).astype(jnp.int32) for o in plane)

    def tell(n):
        for o in plane:
            @pl.when(both(o))
            def _(o=o):
                pl.semaphore_signal(known.at[n], inc=1, device_id=at(gy=o[1], gx=o[2]),
                                    device_id_type=MESH)

    xs = [moves_x(g) for g in range(len(PARTS))]
    start(moves_z)
    start(moves_c)
    start(xs[0])
    start(moves_y)
    for move in xs[1:]:
        start(move)
    if near:
        tell(0)

    def along(s0, s1):
        up = jnp.where(lane == 0, 0.0, pltpu.roll(s1, 1, 1))
        down = jnp.where(lane == LANE - 1, 0.0, pltpu.roll(s1, LANE - 1, 1))
        return s0 + up + down

    for f in range(FIELDS):
        for t in range(tiles):
            y = SUB + t * SUB
            mids, sides = [None], [None]
            for x in range(nx):
                mids.append(pad[f, x, y : y + SUB, :])
                sides.append(pad[f, x, y - 1 : y - 1 + SUB, :] + pad[f, x, y + 1 : y + 1 + SUB, :])
            mids.append(None)
            sides.append(None)
            for x in range(nx):
                next_to = [v for v in (mids[x], mids[x + 2]) if v is not None]
                beyond = [v for v in (sides[x], sides[x + 2]) if v is not None]
                close = sides[x + 1] + sum(next_to[1:], next_to[0])
                far = sum(beyond[1:], beyond[0])
                s0 = W0 * mids[x + 1] + W1 * close + W2 * far
                s1 = W1 * mids[x + 1] + W2 * close + W3 * far
                mid[f, x * tiles + t] = along(s0, s1)

    def piece(ref, k):
        x, t = divmod(k, tiles)
        return ref[x, t * SUB : (t + 1) * SUB, :]

    for copy in small:
        copy.wait()
    for copy in lend[:1]:
        pl.when(distant)(copy.start)
    for n, ref in enumerate((span_ref, dens_ref, invden)):
        packed = zero
        for k in range(chunks):
            value = ref[k] if n == 2 else piece(ref, k)
            for j in range(LANE // slots):
                packed = place(packed, value, k, j)
        around[n, 0] = packed
        for i, y in enumerate((0, ny - 1)):
            for x in range(nx):
                k = x * tiles + y // SUB
                around[n, 1 + i, x : x + 1, :] = (
                    ref[k, y % SUB : y % SUB + 1, :] if n == 2 else ref[x, y : y + 1, :])
    for k in range(FIELDS):
        lam[k] = jnp.full((SUB, LANE), lam0_ref[k], jnp.float32)
    total = zero
    for k in range(chunks):
        s = piece(span_ref, k)
        square = s * s
        pp[FIELDS, k] = square * (1.001 + RAA)
        qq[FIELDS, k] = square * (0.001 + RAA)
        total += s * (1.002 + 2 * RAA)
    acc[ROWS - 1] = total
    weights = [lam[j] for j in range(FIELDS)]

    inside = jnp.logical_not(ends)
    core = range(tiles, chunks - tiles)
    faces = [k for k in range(chunks) if k not in core]

    def keep_of(k):
        keep = inside
        if k in faces:
            return keep
        if k % tiles == 0:
            keep = jnp.logical_and(keep, row != 0)
        if k % tiles == tiles - 1:
            keep = jnp.logical_and(keep, row != SUB - 1)
        return keep

    def grown(r, s):
        gp = jnp.maximum(r, 0.0)
        gm = jnp.maximum(-r, 0.0)
        square = s * s
        p = square * (1.001 * gp + 0.001 * gm + RAA)
        q = square * (0.001 * gp + 1.001 * gm + RAA)
        return p, q, s * (1.002 * (gp + gm) + 2 * RAA)

    def rows(f, j, packed, ks):
        total = zero
        for k in ks:
            x, t = divmod(k, tiles)
            value = mid[f, k]
            for i in range(2):
                if x == (0, nx - 1)[i]:
                    y = SUB + t * SUB
                    h = xpad[i, f, y : y + SUB, :]
                    pair = xpad[i, f, y - 1 : y - 1 + SUB, :] + xpad[i, f, y + 1 : y + 1 + SUB, :]
                    value += along(W1 * h + W2 * pair, W2 * h + W3 * pair)
            packed = place(packed, value, k, j)
            for i, y in enumerate((0, ny - 1)):
                if t == y // SUB:
                    if k in faces:
                        line = jnp.broadcast_to(ymid[i, f, x : x + 1, :], (SUB, LANE))
                        value += jnp.where(row == y % SUB, line, 0.0)
                    else:
                        ymid[i, f, x : x + 1, :] = value[y % SUB : y % SUB + 1, :]
            s = piece(span_ref, k)
            pp[f, k], qq[f, k], base = grown(value * invden[k], s)
            total += jnp.where(keep_of(k), base, 0.0)
        if f:
            acc[SUMS - 1 + f] = total + (zero if ks is core else acc[SUMS - 1 + f])
        return packed

    def respond(k, weights):
        big_p, big_q = pp[0, k], qq[0, k]
        for j in range(FIELDS):
            big_p += weights[j] * pp[j + 1, k]
            big_q += weights[j] * qq[j + 1, k]
        if k >= lent:
            s, d = piece(span_more, k - lent), piece(dens_more, k - lent)
        elif k >= chunks:
            s, d = around[0, k - chunks], around[1, k - chunks]
        else:
            s, d = piece(span_ref, k), piece(dens_ref, k)
        root_p = jnp.sqrt(big_p)
        root_q = jnp.sqrt(big_q)
        lower, upper = d - s, d + s
        moved = (root_p * lower + root_q * upper) / (root_p + root_q)
        low = jnp.maximum(0.0, d - MOVE * s)
        high = jnp.minimum(1.0, d + MOVE * s)
        return jnp.minimum(jnp.maximum(moved, low), high), big_p, big_q, lower, upper

    def terms(k, weights, keep=None):
        moved, big_p, big_q, lower, upper = respond(k, weights)
        ia = 1.0 / (upper - moved)
        ib = 1.0 / (moved - lower)
        ia2, ib2 = ia * ia, ib * ib
        inv = 1.0 / (2.0 * big_p * (ia2 * ia) + 2.0 * big_q * (ib2 * ib))
        if keep is not None:
            ia, ib, ia2, ib2 = [jnp.where(keep, v, 0.0) for v in (ia, ib, ia2, ib2)]
        grads, slopes, ratios = [], [], []
        for j in range(FIELDS):
            p, q = pp[j + 1, k], qq[j + 1, k]
            grads.append(p * ia + q * ib)
            a = p * ia2 - q * ib2
            slopes.append(a)
            ratios.append(a * inv)
        return grads, slopes, ratios

    def main_sums(weights, ks, masked, more):
        grads = [acc[j] if more else zero for j in range(FIELDS)]
        for n, k in enumerate(ks):
            extra, slopes, ratios = terms(k, weights, keep_of(k) if masked else None)
            for j in range(FIELDS):
                grads[j] += extra[j]
                slope[j, n] = slopes[j]
                scaled[j, n] = ratios[j]
        for j in range(FIELDS):
            acc[j] = grads[j]
        at_row = FIELDS
        for group in ((0, 1), (2, 3), (4, 5, 6, 7, 8)):
            keys = [(i, j) for i in group for j in range(i, FIELDS)]
            sums = {key: acc[at_row + n] if more else zero for n, key in enumerate(keys)}
            for n in range(len(ks)):
                right = {j: slope[j, n] for j in range(group[0], FIELDS)}
                for i in group:
                    left = scaled[i, n]
                    for j in range(i, FIELDS):
                        sums[i, j] += left * right[j]
            for key in keys:
                acc[at_row] = sums[key]
                at_row += 1

    def combined(ref, *index):
        last = 0 if single else 1
        low = pltpu.roll(ref[(0,) + index], 1, 1)
        high = pltpu.roll(ref[(last,) + index], LANE - 1, 1)
        if single:
            upper = me["gz"] == 1
            return jnp.where(odd, jnp.where(upper, low, 0.0), jnp.where(upper, 0.0, high))
        return jnp.where(odd, low, high)

    def outer_edges():
        last_x, last_t = wide_x * (nx - 1), 2 * (tiles - 1)
        yz = [combined(yzrecv, n) for n in range(2)]
        xz = [combined(xzrecv, n) for n in range(2)]
        cz_ = [combined(czrecv, n) for n in range(4)]

        def pick(value, g, shift):
            return turned(jnp.broadcast_to(value[g : g + 1, :], (SUB, LANE)), shift)

        def beside(c, first, final):
            down = pltpu.roll(c, 1, 0)
            up = pltpu.roll(c, SUB - 1, 0)
            before = jnp.where(row == 0, jnp.where(t_of == 0, first, turned(down, 2)), down)
            after = jnp.where(row == SUB - 1, jnp.where(t_of == tiles - 1, final, turned(up, LANE - 2)), up)
            return before + after

        out = []
        for g in range(count_of):
            c = combined(zrecv, g)
            s = beside(c, pick(yz[0], g, -last_t), pick(yz[1], g, last_t))
            c_low = turned(xz[0], -wide_x * g)
            c_high = turned(xz[1], last_x - wide_x * g)
            s_low = beside(c_low, pick(cz_[0], g, -last_x - last_t), pick(cz_[1], g, -last_x + last_t))
            s_high = beside(c_high, pick(cz_[2], g, last_x - last_t), pick(cz_[3], g, last_x + last_t))

            def pair(own, low, high):
                return (jnp.where(x_of == 0, low, turned(own, wide_x))
                        + jnp.where(x_of == nx - 1, high, turned(own, -wide_x)))
            out.append(W1 * c + W2 * (s + pair(c, c_low, c_high)) + W3 * pair(s, s_low, s_high))
        return out

    body_rows = jnp.logical_and(inside, jnp.logical_and(row != 0, row != nx - 1))

    def face_rows():
        drops = [[zero, zero] for _ in groups]
        bases = []
        for g, fields in enumerate(groups):
            for j, f in enumerate(fields):
                base = zero
                for i in range(2):
                    h = yrecv[i, f]
                    low = jnp.broadcast_to(crecv[i, f], (SUB, LANE))
                    high = jnp.broadcast_to(crecv[2 + i, f], (SUB, LANE))
                    pair = (jnp.where(row == 0, low, pltpu.roll(h, 1, 0))
                            + jnp.where(row == nx - 1, high, pltpu.roll(h, nx - 1, 0)))
                    extra = along(W1 * h + W2 * pair, W2 * h + W3 * pair)
                    s = around[0, 1 + i]
                    face = jnp.logical_or(row == 0, row == nx - 1)
                    value = jnp.where(face, 0.0, ymid[i, f]) + extra
                    p, q, more = grown(value * around[2, 1 + i], s)
                    pp[f, chunks + 1 + i] = p
                    qq[f, chunks + 1 + i] = q
                    base += jnp.where(body_rows, more, 0.0)
                    ymid[i, f, 0:1, :] = extra[:1]
                    ymid[i, f, nx - 1 : nx, :] = extra[nx - 1 :]
                    here = jnp.logical_and(row == x_of, lane // slots == j)
                    side = jnp.where(odd, jnp.broadcast_to(extra[:, :1], (SUB, LANE)),
                                     jnp.broadcast_to(extra[:, LANE - 1 :], (SUB, LANE)))
                    drops[g][i] = jnp.where(here, side, drops[g][i])
                bases.append(base)
        for i in range(2):
            s = around[0, 1 + i]
            pp[FIELDS, chunks + 1 + i] = s * s * (1.001 + RAA)
            qq[FIELDS, chunks + 1 + i] = s * s * (0.001 + RAA)
        extras = []
        for g in range(count_of):
            value = zero
            for i, y in enumerate((0, ny - 1)):
                full = jnp.broadcast_to(jnp.sum(drops[g][i], axis=0, keepdims=True), (SUB, LANE))
                here = jnp.logical_and(row == y % SUB, t_of == y // SUB)
                value += jnp.where(here, full, 0.0)
            extras.append(value)
        return extras, bases[1:]

    def edge_rows(extras):
        outer = outer_edges()
        s = around[0, 0]
        bases = []
        for g, fields in enumerate(groups):
            p, q, base = grown((inner[g] + extras[g] + outer[g]) * around[2, 0], s)
            for j, f in enumerate(fields):
                pp[f, chunks] = turned(p, -j * slots)
                qq[f, chunks] = turned(q, -j * slots)
                bases.append(turned(base, -j * slots))
        pp[FIELDS, chunks] = s * s * (1.001 + RAA)
        qq[FIELDS, chunks] = s * s * (0.001 + RAA)
        return bases[1:]

    def extra_sums(weights, ks, keep, bases):
        pieces = [terms(k, weights, keep) for k in ks]
        grads = [sum((p[0][j] for p in pieces[1:]), pieces[0][0][j]) for j in range(FIELDS)]
        squares = [sum((p[2][i] * p[1][j] for p in pieces[1:]), pieces[0][2][i] * pieces[0][1][j])
                   for i in range(FIELDS) for j in range(i, FIELDS)]
        for r, value in enumerate(grads + squares + list(bases)):
            acc[r] += value

    def between():
        for fields in groups:
            for f in fields:
                repair(f, range(KEPT * tiles, chunks))
            if near:
                of, at_k = pl.ds(fields[0], len(fields)), pl.ds(KEPT * tiles, chunks - KEPT * tiles)
                pl.when(distant)(pltpu.make_async_remote_copy(
                    src_ref=both_pq.at[:, of, at_k],
                    dst_ref=both_pq.at[:, of, pl.ds(lent, chunks - KEPT * tiles)],
                    send_sem=lend_send.at[1], recv_sem=lend_recv.at[1],
                    device_id={"gy": me["gy"] + 1 - 2 * lax.rem(me["gy"], 2)}, device_id_type=MESH).start)
        for f in range(FIELDS):
            repair(f, range(KEPT * tiles))
        for moves in [moves_c, moves_y] + xs + [moves_z]:
            for send, _, copy in moves:
                pl.when(send)(copy.wait_send)
        if near:
            @pl.when(jnp.logical_not(distant))
            def _():
                lend[0].wait_recv()
                for k in range(lent, both_pq.shape[2]):
                    s = piece(span_more, k - lent)
                    pp[FIELDS, k] = s * s * (1.001 + RAA)
                    qq[FIELDS, k] = s * s * (0.001 + RAA)
                lend[1].wait_recv()

    def repair(f, ks):
        for ref in (pp, qq):
            edge = ref[f, chunks]
            for k in ks:
                x, t = divmod(k, tiles)
                value = ref[f, k]
                for i, y in enumerate((0, ny - 1)):
                    if t == y // SUB and k in core:
                        line = jnp.broadcast_to(ref[f, chunks + 1 + i, x : x + 1, :], (SUB, LANE))
                        value = jnp.where(row == y % SUB, line, value)
                ref[f, k] = jnp.where(ends, turned(edge, -2 * k - 1), value)

    def flat(axes):
        index = 0
        for a in axes:
            index = index * shape[a] + me[a]
        return index

    def moved(a, d):
        size = shape[a]
        if size & (size - 1) or d < 1 or d > 3:
            return lax.rem(me[a] + d, size)
        if d == 1:
            return me[a] + 1 - 2 * lax.rem(me[a], 2)
        if d == 2:
            return me[a] + 2 - 4 * lax.rem(me[a] // 2, 2)
        return me[a] + 3 - 2 * lax.rem(me[a], 4)

    targets = []
    for axes in stages:
        to = {(a, d): moved(a, d) if d else me[a] for a in axes for d in range(shape[a])}
        far = sorted(offsets(axes, shape), reverse=True, key=lambda o: (
            sum(d // 2 if a == "gy" else d for a, d in zip(axes, o)), [-d for d in o]))
        targets.append([{a: to[a, d] for a, d in zip(axes, o)} for o in far])

    def exchange(it, count, meanwhile):
        packed = zero
        for g in range(count):
            values = [acc[r] if r < ROWS else zero for r in range(g * SUB, (g + 1) * SUB)]
            half = SUB // 2
            while half:
                upper = (row // half) % 2 == 1
                step = len(values) // 2
                values = [
                    jnp.where(upper, b, a) + pltpu.roll(jnp.where(upper, a, b), half, 0)
                    if half == SUB // 2 else
                    jnp.where(upper, b + turned(b, half, 0), a + turned(a, -half, 0))
                    for a, b in zip(values[:step], values[step:])
                ]
                half //= 2
            packed = jnp.where(lane == g * SUB + row, jnp.sum(values[0], axis=1, keepdims=True), packed)
        value = jnp.sum(packed, axis=0, keepdims=True)
        for n, axes in enumerate(stages):
            size = math.prod(shape[a] for a in axes)
            part[it, n] = value
            recvs[n][it, flat(axes)] = value
            for target in targets[n]:
                pltpu.make_async_remote_copy(
                    src_ref=part.at[it, n], dst_ref=recvs[n].at[it, flat(axes)],
                    send_sem=sum_send.at[n], recv_sem=sum_recv.at[it, n],
                    device_id=target, device_id_type=MESH).start()
            if n == 0:
                meanwhile()
            whole = recvs[n].at[it, pl.ds(0, size - 1)]
            pltpu.make_async_copy(whole, whole, sum_recv.at[it, n]).wait()
            values = [recvs[n][it, i] for i in range(size)]
            while len(values) > 1:
                values = [sum(values[i + 1 : i + 2], values[i]) for i in range(0, len(values), 2)]
            value = values[0]
        every = jnp.broadcast_to(value, (SUB, LANE))
        for g in range(count):
            one = jnp.sum(jnp.where(lane == g * SUB + row, every, 0.0), axis=1, keepdims=True)
            wide[g] = jnp.broadcast_to(one, (SUB, LANE))

    def solve(weights):
        def read(r):
            return jnp.broadcast_to(wide[r // SUB, r % SUB : r % SUB + 1, :], (SUB, LANE))
        b = [read(j) - (1.0 - viol_ref[j]) * read(SUMS + j) for j in range(FIELDS)]
        m = {}
        at_row = FIELDS
        for i in range(FIELDS):
            for j in range(i, FIELDS):
                m[i, j] = read(at_row)
                at_row += 1
        trace = m[0, 0]
        for i in range(1, FIELDS):
            trace += m[i, i]
        shift = REG * trace / FIELDS
        for i in range(FIELDS):
            m[i, i] += shift
        inverse = []
        for k in range(FIELDS):
            inverse.append(1.0 / m[k, k])
            for i in range(k + 1, FIELDS):
                factor = m[k, i] * inverse[k]
                for j in range(i, FIELDS):
                    m[i, j] -= factor * m[k, j]
                b[i] -= factor * b[k]
        delta = [None] * FIELDS
        for k in reversed(range(FIELDS)):
            v = b[k]
            for j in range(k + 1, FIELDS):
                v -= m[k, j] * delta[j]
            delta[k] = v * inverse[k]
        for k in range(FIELDS):
            lam[k] = jnp.maximum(weights[k] + delta[k], FLOOR * weights[k])

    def newton(it, carry):
        weights = [lam[j] for j in range(FIELDS)]
        if near:
            @pl.when(distant)
            def _():
                main_sums(weights, range(KEPT * tiles), False, False)

            @pl.when(jnp.logical_not(distant))
            def _():
                main_sums(weights, list(range(chunks)) + list(range(lent, both_pq.shape[2])), False, False)
        else:
            main_sums(weights, range(chunks), False, False)
        exchange(it, -(-SUMS // SUB), lambda: None)
        solve(weights)
        return carry

    inner = []
    for g, fields in enumerate(groups):
        packed = zero
        for j, f in enumerate(fields):
            packed = rows(f, j, packed, core)
        inner.append(packed)
    main_sums(weights, core, True, False)
    if near:
        pl.semaphore_wait(known.at[0], friends)
        tell(1)
    receive(moves_y)
    receive(moves_c)
    extras, bases = face_rows()
    extra_sums(weights, (chunks + 1, chunks + 2), body_rows, bases)
    for n, move in enumerate(xs):
        receive(move)
        if n == len(xs) - 1:
            receive(moves_z)
        for f in range(starts[n], starts[n] + PARTS[n]):
            g, j = divmod(f, GROUP)
            inner[g] = rows(f, j, inner[g], faces)
    main_sums(weights, faces, True, True)
    within = lane < slots
    bases = [jnp.where(within, v, 0.0) for v in edge_rows(extras)]
    extra_sums(weights, (chunks,), within, bases)
    if near:
        pl.semaphore_wait(known.at[1], friends)
    exchange(0, wide.shape[0], between)
    solve(weights)
    lax.fori_loop(1, ITERS, newton, 0)

    weights = [lam[j] for j in range(FIELDS)]
    for k in range(chunks):
        x, t = divmod(k, tiles)
        out_ref[x, t * SUB : (t + 1) * SUB, :] = respond(k, weights)[0]
    final = zero
    for j in range(FIELDS):
        final = jnp.where(lane == j, weights[j], final)
    lam_out[...] = final

    if near:
        @pl.when(distant)
        def _():
            for copy in lend:
                copy.wait_send()
    for n, axes in enumerate(stages):
        size = math.prod(shape[a] for a in axes)
        whole = recvs[n].at[:, pl.ds(0, size - 1)]
        pltpu.make_async_copy(whole, whole, sum_send.at[n]).wait()


def finish(field_ref, lam_ref, field_out, lam_out, row, sem):
    whole = pltpu.make_async_copy(field_ref, field_out, sem.at[0])
    whole.start()
    row[...] = lam_ref[0, :FIELDS]
    short = pltpu.make_async_copy(row, lam_out, sem.at[1])
    short.start()
    whole.wait()
    short.wait()


def shards(shape, density, spread, sensitivities, violation, multipliers_start):
    nx, ny, nz = density.shape
    chunks = nx * ny // SUB
    groups = len(steps())
    stages = plan(shape)
    corners = 9 if shape["gz"] == 2 else 18
    depth = corners // 9
    more = nx - KEPT if compact(shape) else 1
    every = chunks + 3 + (more * ny // SUB if compact(shape) else 0)
    f32 = jnp.float32
    vmem = pl.BlockSpec(memory_space=pltpu.VMEM)
    dma = pltpu.SemaphoreType.DMA
    hbm = pl.BlockSpec(memory_space=pltpu.HBM)
    field, lam = pl.pallas_call(
        functools.partial(body, shape, (nx, ny, nz)),
        out_shape=(
            pltpu.VMEM((nx, ny, nz), f32),
            pltpu.VMEM((SUB, LANE), f32),
        ),
        in_specs=[hbm] * 5,
        out_specs=(vmem, vmem),
        scratch_shapes=[
            pltpu.VMEM((2, nx, ny, nz), f32),
            pltpu.VMEM((2, more, ny, nz), f32),
            pltpu.SMEM((FIELDS,), f32),
            pltpu.SMEM((FIELDS,), f32),
            pltpu.VMEM((FIELDS, nx, ny + 2 * SUB, nz), f32),
            pltpu.VMEM((2, FIELDS, ny + 2 * SUB, nz), f32),
            pltpu.VMEM((2, FIELDS, nx, nz), f32),
            pltpu.VMEM((2, FIELDS, nx, nz), f32),
            pltpu.VMEM((4, FIELDS, 1, nz), f32),
            pltpu.VMEM((4, FIELDS, 1, nz), f32),
            pltpu.VMEM((2, FIELDS, nx, nz), f32),
            pltpu.VMEM((groups, SUB, LANE), f32),
            pltpu.VMEM((depth, groups, SUB, LANE), f32),
            pltpu.VMEM((2, SUB, LANE), f32),
            pltpu.VMEM((depth, 2, SUB, LANE), f32),
            pltpu.VMEM((2, SUB, LANE), f32),
            pltpu.VMEM((depth, 2, SUB, LANE), f32),
            pltpu.VMEM((depth, 4, SUB, LANE), f32),
            pltpu.VMEM((3, 3, SUB, LANE), f32),
            pltpu.VMEM((FIELDS, chunks, SUB, LANE), f32),
            pltpu.VMEM((chunks, SUB, LANE), f32),
            pltpu.VMEM((2, FIELDS + 1, every, SUB, LANE), f32),
            pltpu.VMEM((FIELDS, every, SUB, LANE), f32),
            pltpu.VMEM((FIELDS, every, SUB, LANE), f32),
            pltpu.VMEM((ROWS, SUB, LANE), f32),
            pltpu.VMEM((-(-ROWS // SUB), SUB, LANE), f32),
            pltpu.VMEM((FIELDS, SUB, LANE), f32),
            pltpu.VMEM((ITERS, len(stages), 1, LANE), f32),
        ] + [
            pltpu.VMEM((ITERS, math.prod(shape[a] for a in axes), 1, LANE), f32) for axes in stages
        ] + [
            dma((4 + groups,)), dma((6 + 2 * len(PARTS),)), dma((6 + 2 * len(PARTS),)), dma((corners,)), dma((corners,)), dma((2,)), dma((2,)),
            dma((len(stages),)), dma((ITERS, len(stages))), pltpu.SemaphoreType.REGULAR((2,)),
        ],
        compiler_params=pltpu.CompilerParams(
            collective_id=0, has_side_effects=True, vmem_limit_bytes=24 << 20),
        name="design_step",
    )(*[pltpu.with_memory_space_constraint(v, pltpu.HBM) for v in (density, spread, sensitivities, violation, multipliers_start)])
    return pl.pallas_call(
        finish,
        out_shape=(
            jax.ShapeDtypeStruct((nx, ny, nz), f32),
            jax.ShapeDtypeStruct((FIELDS,), f32),
        ),
        in_specs=[vmem, vmem],
        out_specs=(hbm, hbm),
        scratch_shapes=[pltpu.VMEM((FIELDS,), f32), dma((2,))],
        compiler_params=pltpu.CompilerParams(vmem_limit_bytes=1 << 20),
        name="finish",
    )(field, lam)


def solution(mesh):
    shape = {a: int(mesh.shape[a]) for a in AXES}
    return jax.shard_map(
        functools.partial(shards, shape),
        mesh=mesh,
        in_specs=(P("gx", "gy", "gz"), P("gx", "gy", "gz"), P(None, "gx", "gy", "gz"), P(), P()),
        out_specs=(P("gx", "gy", "gz"), P()),
        check_vma=False,
    )
```
